8 devices in a mesh: batch: 2 (over z, y), group: 4 (over x, core).
Axes of the slice: x: 2, y: 2, z: 1, core: 2. Of those that a mesh axis runs over, the one named last changes fastest.
Arguments:
- sort_keys: float32 [16384], P(('batch', 'group')), parts along dimension 0
- seg_ids: int32 [16384], P(('batch', 'group')), parts along dimension 0
- payload: bfloat16 [16384, 2048], P(('batch', 'group')), parts along dimension 0
Outputs:
- output: bfloat16 [16384, 2048], P(('batch', 'group')), parts along dimension 0
There are 2 independent parts. The reference program is written for one: setup_inputs(seed, part) draws one part's arguments, and reference() takes and returns one part's arrays. A program takes and returns all parts, laid end to end along the dimension named above; each array names one.
All inputs are finite; a program needn't handle non-finite values.
Results may differ from the reference program's by a relative error of at most 0.0066963.
Values are sent between devices in bfloat16 or wider.
A program may use at most 1 GiB of HBM per device.

```python
import jax
import jax.numpy as jnp
from jax import lax

GROUP = 4
ROWS_DEV = 2048
WIDTH = 2048
TOTAL = GROUP * ROWS_DEV
PAIR = ROWS_DEV // GROUP


def combine_runs(left_part, right_part):
    left_flag, left_rows = left_part
    right_flag, right_rows = right_part
    joined = jnp.where(right_flag[..., None], right_rows, left_rows + right_rows)
    return jnp.logical_or(left_flag, right_flag), joined


def draw_layout(base_key):
    phase_key, size_key, tie_key, place_key, cut_key, base_id_key = jax.random.split(base_key, 6)
    half_pair = PAIR // 2
    dev_phase = jax.random.permutation(phase_key, GROUP)
    bound_no = jnp.arange(1, GROUP, dtype=jnp.int32)
    bound_phase = (dev_phase[:, None] + bound_no[None, :]) % GROUP
    shift_size = jax.random.randint(size_key, (GROUP, GROUP - 1), 0, half_pair + 1)
    cut_shift = jnp.where(bound_phase < GROUP // 2, jnp.maximum(shift_size, 1), -shift_size)
    cut_shift = jnp.where(bound_phase == GROUP // 2, 0, cut_shift)
    full_dev = dev_phase == GROUP - 2
    cut_shift = cut_shift.at[:, 0].set(jnp.where(full_dev, -half_pair, cut_shift[:, 0]))
    cut_shift = cut_shift.at[:, 1].set(jnp.where(full_dev, half_pair, cut_shift[:, 1]))
    band_cuts = bound_no[None, :] * PAIR + cut_shift
    local_rank = jnp.arange(ROWS_DEV, dtype=jnp.int32)

    def band_search(cut_row):
        return jnp.searchsorted(cut_row, local_rank, side='right')

    band_of = jax.vmap(band_search)(band_cuts).astype(jnp.int32)
    prev_band = jnp.maximum(band_of - 1, 0)
    band_low = jnp.take_along_axis(band_cuts, prev_band, axis=1)
    band_phase = jnp.take_along_axis(bound_phase, prev_band, axis=1)
    lead_row = (band_of >= 1) & (local_rank[None, :] == band_low) & (band_phase == GROUP // 2)
    tie_break = jax.random.permutation(tie_key, TOTAL).reshape(GROUP, ROWS_DEV)
    rank_score = band_of * (TOTAL + 1) + jnp.where(lead_row, 0, tie_break + 1)
    score_order = jnp.argsort(rank_score.reshape(-1), stable=True)
    global_rank = jnp.argsort(score_order, stable=True).astype(jnp.int32).reshape(GROUP, ROWS_DEV)
    place_keys = jax.random.split(place_key, GROUP)

    def place_rows(row_key):
        return jax.random.permutation(row_key, ROWS_DEV)

    placement = jax.vmap(place_rows)(place_keys)
    rank_at = jnp.take_along_axis(global_rank, placement, axis=1).reshape(TOTAL)
    seg_cuts = jnp.sort(jax.random.randint(cut_key, (GROUP - 1,), 1, TOTAL))
    first_id = jax.random.randint(base_id_key, (), 0, 1000)
    seg_ids = (jnp.searchsorted(seg_cuts, rank_at, side='right') + first_id).astype(jnp.int32)
    return rank_at, seg_ids


def setup_inputs(seed: int = 0, part: int = 0) -> dict:
    base_key = jax.random.fold_in(jax.random.key(seed), part)
    layout_key, payload_key = jax.random.split(base_key, 2)
    rank_at, seg_ids = draw_layout(layout_key)
    centred = (2 * rank_at + 1 - TOTAL).astype(jnp.float32) / TOTAL
    sort_keys = centred * centred * centred
    noise = jax.random.normal(payload_key, (TOTAL, WIDTH), jnp.float32)
    payload = (noise * ROWS_DEV ** -0.5).astype(jnp.bfloat16)
    return {'sort_keys': sort_keys, 'seg_ids': seg_ids, 'payload': payload}


def reference(sort_keys, seg_ids, payload):
    row_pos = jnp.arange(sort_keys.shape[0], dtype=jnp.int32)
    _, seg_sorted, sort_order = lax.sort((sort_keys, seg_ids, row_pos), num_keys=1)
    run_rows = payload[sort_order].astype(jnp.float32)
    first_flag = jnp.ones((1,), dtype=jnp.bool_)
    run_start = jnp.concatenate([first_flag, seg_sorted[1:] != seg_sorted[:-1]])
    _, scanned = lax.associative_scan(combine_runs, (run_start, run_rows))
    _, back_order = lax.sort((sort_order, row_pos), num_keys=1)
    return scanned[back_order].astype(jnp.bfloat16)
```

```python
import jax
import jax.numpy as jnp
from jax import lax
from jax.experimental import pallas as pl
from jax.experimental.pallas import tpu as pltpu
from jax.sharding import PartitionSpec as P

MESH = pl.DeviceIdType.MESH
LANES = 128
COL_CHUNKS = 8
ROW_PIECES = 4


def kernel(keys_ref, segs_ref, x_ref, out_ref, land_ref, all_keys, all_segs,
           mask_ref, rows_buf, sums_buf, out_buf, key_send, key_recv, peer_send, peer_recv,
           mate_send, mate_recv, fwd_send, fwd_recv, load_sem, store_sem):
    rows, width = x_ref.shape
    col_w = width // COL_CHUNKS
    piece = rows // ROW_PIECES
    key_rows = rows // LANES
    batch = lax.axis_index('batch')
    me = lax.axis_index('group')
    mate = me + 1 - 2 * lax.rem(me, 2)
    peer = lax.rem(me + 2, 4)
    diag = 3 - me

    barrier = pltpu.get_barrier_semaphore()
    for other in (mate, peer, diag):
        pl.semaphore_signal(barrier, inc=1, device_id=(batch, other), device_id_type=MESH)
    pl.semaphore_wait(barrier, 3)

    def send(src, dst, ssem, rsem, dev):
        return pltpu.make_async_remote_copy(src, dst, ssem, rsem, device_id=(batch, dev),
                                            device_id_type=MESH)

    key_copies = []
    for q, dev in ((1, mate), (2, peer), (3, diag)):
        key_copies.append(send(keys_ref, all_keys.at[q], key_send.at[2 * q - 2],
                               key_recv.at[2 * q - 2], dev))
        key_copies.append(send(segs_ref, all_segs.at[q], key_send.at[2 * q - 1],
                               key_recv.at[2 * q - 1], dev))
    for copy in key_copies:
        copy.start()

    def cols(c):
        return pl.ds(c * col_w, col_w)

    peer_copies, mate_copies, fwd_copies = {}, {}, {}
    for c in range(COL_CHUNKS):
        for r in range(ROW_PIECES):
            part = (pl.ds(r * piece, piece), cols(c))
            n = c * ROW_PIECES + r
            peer_copies[c, r] = send(x_ref.at[part], land_ref.at[(1,) + part],
                                     peer_send.at[n], peer_recv.at[n], peer)
            fwd_copies[c, r] = send(land_ref.at[(1,) + part], land_ref.at[(2,) + part],
                                    fwd_send.at[n], fwd_recv.at[n], mate)
            peer_copies[c, r].start()
        mate_copies[c] = send(x_ref.at[:, cols(c)], land_ref.at[0, :, cols(c)],
                              mate_send.at[c], mate_recv.at[c], mate)
        mate_copies[c].start()

    all_keys[0] = keys_ref[...]
    all_segs[0] = segs_ref[...]
    for copy in key_copies:
        copy.wait()

    def low_block(b, carry):
        own_k = jnp.broadcast_to(keys_ref[pl.ds(b, 1), :], (LANES, LANES)).T
        own_s = jnp.broadcast_to(segs_ref[pl.ds(b, 1), :], (LANES, LANES)).T

        def scan_keys(t, low):
            for q in range(4):
                k = all_keys[q, pl.ds(t, 1), :]
                s = all_segs[q, pl.ds(t, 1), :]
                other = jnp.logical_and(k < own_k, s != own_s)
                low = jnp.maximum(low, jnp.where(other, k, -jnp.inf))
            return low

        low = lax.fori_loop(0, key_rows, scan_keys, jnp.full((LANES, LANES), -jnp.inf, jnp.float32))
        low = jnp.broadcast_to(jnp.max(low, axis=1, keepdims=True), (LANES, LANES))
        at = pl.ds(pl.multiple_of(b * LANES, LANES), LANES)

        def mask_keys(t, c):
            for q in range(4):
                k = all_keys[q, pl.ds(t, 1), :]
                inside = jnp.logical_and(k <= own_k, k > low)
                to = pl.ds(pl.multiple_of(q * rows + t * LANES, LANES), LANES)
                mask_ref[at, to] = jnp.where(inside, 1.0, 0.0).astype(jnp.bfloat16)
            return c

        lax.fori_loop(0, key_rows, mask_keys, 0)
        return carry

    lax.fori_loop(0, key_rows, low_block, 0)

    tile = 256
    stores = []

    def load(n, src, dst):
        copy = pltpu.make_async_copy(src, dst, load_sem.at[n])
        copy.start()
        return copy

    def flush(c):
        copy = pltpu.make_async_copy(out_buf.at[c % 2], out_ref.at[:, cols(c)], store_sem.at[c % 2])
        copy.start()
        stores.append(copy)

    last = COL_CHUNKS - 1
    for c in range(COL_CHUNKS):
        if c >= 2:
            stores[c - 2].wait()
        loads = [load(0, x_ref.at[:, cols(c)], rows_buf.at[pl.ds(0, rows), :])]
        mate_copies[c].wait_recv()
        loads.append(load(1, land_ref.at[0, :, cols(c)], rows_buf.at[pl.ds(rows, rows), :]))
        if c < last:
            for r in range(ROW_PIECES):
                peer_copies[c, r].wait_recv()
                fwd_copies[c, r].start()
            loads.append(load(2, land_ref.at[1, :, cols(c)], rows_buf.at[pl.ds(2 * rows, rows), :]))
            for r in range(ROW_PIECES):
                fwd_copies[c, r].wait_recv()
            loads.append(load(3, land_ref.at[2, :, cols(c)], rows_buf.at[pl.ds(3 * rows, rows), :]))
            for copy in loads:
                copy.wait()

            def whole(i, carry):
                at = pl.ds(pl.multiple_of(i * tile, tile), tile)
                out_buf[c % 2, at, :] = jnp.dot(
                    mask_ref[at, :], rows_buf[...],
                    preferred_element_type=jnp.float32).astype(jnp.bfloat16)
                return carry

            lax.fori_loop(0, rows // tile, whole, 0)
        else:
            for copy in loads:
                copy.wait()

            def near(i, carry):
                at = pl.ds(pl.multiple_of(i * tile, tile), tile)
                sums_buf[at, :] = jnp.dot(mask_ref[at, pl.ds(0, 2 * rows)],
                                          rows_buf[pl.ds(0, 2 * rows), :],
                                          preferred_element_type=jnp.float32)
                return carry

            lax.fori_loop(0, rows // tile, near, 0)
            for r in range(ROW_PIECES):
                part = (pl.ds(r * piece, piece), cols(c))
                from_peer = pl.ds(2 * rows + r * piece, piece)
                from_diag = pl.ds(3 * rows + r * piece, piece)
                peer_copies[c, r].wait_recv()
                fwd_copies[c, r].start()
                one = load(2, land_ref.at[(1,) + part], rows_buf.at[from_peer, :])
                fwd_copies[c, r].wait_recv()
                two = load(3, land_ref.at[(2,) + part], rows_buf.at[from_diag, :])
                one.wait()
                two.wait()

                def far(i, carry):
                    at = pl.ds(pl.multiple_of(i * tile, tile), tile)
                    more = jnp.dot(mask_ref[at, from_peer], rows_buf[from_peer, :],
                                   preferred_element_type=jnp.float32)
                    more += jnp.dot(mask_ref[at, from_diag], rows_buf[from_diag, :],
                                    preferred_element_type=jnp.float32)
                    more += sums_buf[at, :]
                    if r < ROW_PIECES - 1:
                        sums_buf[at, :] = more
                    else:
                        out_buf[c % 2, at, :] = more.astype(jnp.bfloat16)
                    return carry

                lax.fori_loop(0, rows // tile, far, 0)
        flush(c)
    for copy in stores[-2:]:
        copy.wait()
    for c in range(COL_CHUNKS):
        mate_copies[c].wait_send()
        for r in range(ROW_PIECES):
            peer_copies[c, r].wait_send()
            fwd_copies[c, r].wait_send()


def solution(mesh):
    def per_device(sort_keys, seg_ids, payload):
        rows, width = payload.shape
        col_w = width // COL_CHUNKS
        pieces = COL_CHUNKS * ROW_PIECES
        keys = sort_keys.reshape(rows // LANES, LANES)
        segs = seg_ids.reshape(rows // LANES, LANES)
        dma = pltpu.SemaphoreType.DMA
        out, _ = pl.pallas_call(
            kernel,
            out_shape=(jax.ShapeDtypeStruct((rows, width), jnp.bfloat16),
                       jax.ShapeDtypeStruct((3, rows, width), jnp.bfloat16)),
            in_specs=[pl.BlockSpec(memory_space=pltpu.VMEM)] * 2 + [pl.BlockSpec(memory_space=pl.ANY)],
            out_specs=(pl.BlockSpec(memory_space=pl.ANY),) * 2,
            scratch_shapes=[
                pltpu.VMEM((4, rows // LANES, LANES), jnp.float32),
                pltpu.VMEM((4, rows // LANES, LANES), jnp.int32),
                pltpu.VMEM((rows, 4 * rows), jnp.bfloat16),
                pltpu.VMEM((4 * rows, col_w), jnp.bfloat16),
                pltpu.VMEM((rows, col_w), jnp.float32),
                pltpu.VMEM((2, rows, col_w), jnp.bfloat16),
                dma((6,)), dma((6,)), dma((pieces,)), dma((pieces,)),
                dma((COL_CHUNKS,)), dma((COL_CHUNKS,)), dma((pieces,)), dma((pieces,)),
                dma((4,)), dma((2,)),
            ],
            compiler_params=pltpu.CompilerParams(collective_id=0, has_side_effects=True,
                                                 vmem_limit_bytes=60 * 1024 * 1024),
        )(keys, segs, payload)
        return out

    row_spec = P(('batch', 'group'))
    mat_spec = P(('batch', 'group'), None)
    return jax.shard_map(per_device, mesh=mesh, in_specs=(row_spec, row_spec, mat_spec),
                         out_specs=mat_spec, check_vma=False)
```

```python
import jax
import jax.numpy as jnp
from jax import lax
from jax.experimental import pallas as pl
from jax.experimental.pallas import tpu as pltpu
from jax.sharding import PartitionSpec as P

MESH = pl.DeviceIdType.MESH
LANES = 128
COL_CHUNKS = 8
ROW_PIECES = 4


def kernel(keys_ref, segs_ref, x_ref, out_ref, land_ref, all_keys, all_segs,
           mask_ref, rows_buf, tail_buf, sums_buf, key_send, key_recv, peer_send, peer_recv,
           mate_send, mate_recv, fwd_send, fwd_recv, load_sem):
    rows, width = x_ref.shape
    col_w = width // COL_CHUNKS
    piece = rows // ROW_PIECES
    key_rows = rows // LANES
    batch = lax.axis_index('batch')
    me = lax.axis_index('group')
    mate = me + 1 - 2 * lax.rem(me, 2)
    peer = lax.rem(me + 2, 4)
    diag = 3 - me

    barrier = pltpu.get_barrier_semaphore()
    for other in (mate, peer, diag):
        pl.semaphore_signal(barrier, inc=1, device_id=(batch, other), device_id_type=MESH)
    pl.semaphore_wait(barrier, 3)

    def send(src, dst, ssem, rsem, dev):
        return pltpu.make_async_remote_copy(src, dst, ssem, rsem, device_id=(batch, dev),
                                            device_id_type=MESH)

    key_copies = []
    for q, dev in ((1, mate), (2, peer), (3, diag)):
        key_copies.append(send(keys_ref, all_keys.at[q], key_send.at[2 * q - 2],
                               key_recv.at[2 * q - 2], dev))
        key_copies.append(send(segs_ref, all_segs.at[q], key_send.at[2 * q - 1],
                               key_recv.at[2 * q - 1], dev))
    for copy in key_copies:
        copy.start()

    def cols(c):
        return pl.ds(c * col_w, col_w)

    peer_copies, mate_copies, fwd_copies = {}, {}, {}
    for c in range(COL_CHUNKS):
        for r in range(ROW_PIECES):
            part = (pl.ds(r * piece, piece), cols(c))
            n = c * ROW_PIECES + r
            if c < COL_CHUNKS - 1:
                first, second = land_ref.at[(1,) + part], land_ref.at[(2,) + part]
            else:
                first, second = tail_buf.at[0, part[0], :], tail_buf.at[1, part[0], :]
            peer_copies[c, r] = send(x_ref.at[part], first, peer_send.at[n], peer_recv.at[n], peer)
            fwd_copies[c, r] = send(first, second, fwd_send.at[n], fwd_recv.at[n], mate)
            peer_copies[c, r].start()
        mate_copies[c] = send(x_ref.at[:, cols(c)], land_ref.at[0, :, cols(c)],
                              mate_send.at[c], mate_recv.at[c], mate)
        mate_copies[c].start()

    all_keys[0] = keys_ref[...]
    all_segs[0] = segs_ref[...]
    for copy in key_copies:
        copy.wait()

    def low_block(b, carry):
        own_k = jnp.broadcast_to(keys_ref[pl.ds(b, 1), :], (LANES, LANES)).T
        own_s = jnp.broadcast_to(segs_ref[pl.ds(b, 1), :], (LANES, LANES)).T

        def scan_keys(t, low):
            for q in range(4):
                k = all_keys[q, pl.ds(t, 1), :]
                s = all_segs[q, pl.ds(t, 1), :]
                other = jnp.logical_and(k < own_k, s != own_s)
                low = jnp.maximum(low, jnp.where(other, k, -jnp.inf))
            return low

        low = lax.fori_loop(0, key_rows, scan_keys, jnp.full((LANES, LANES), -jnp.inf, jnp.float32))
        low = jnp.broadcast_to(jnp.max(low, axis=1, keepdims=True), (LANES, LANES))
        at = pl.ds(pl.multiple_of(b * LANES, LANES), LANES)

        def mask_keys(t, c):
            for q in range(4):
                k = all_keys[q, pl.ds(t, 1), :]
                inside = jnp.logical_and(k <= own_k, k > low)
                to = pl.ds(pl.multiple_of(q * rows + t * LANES, LANES), LANES)
                mask_ref[at, to] = jnp.where(inside, 1.0, 0.0).astype(jnp.bfloat16)
            return c

        lax.fori_loop(0, key_rows, mask_keys, 0)
        return carry

    lax.fori_loop(0, key_rows, low_block, 0)

    tile = 1024

    def load(n, src, dst):
        copy = pltpu.make_async_copy(src, dst, load_sem.at[n])
        copy.start()
        return copy

    last = COL_CHUNKS - 1
    for c in range(last):
        loads = [load(0, x_ref.at[:, cols(c)], rows_buf.at[pl.ds(0, rows), :])]
        mate_copies[c].wait_recv()
        loads.append(load(1, land_ref.at[0, :, cols(c)], rows_buf.at[pl.ds(rows, rows), :]))
        for r in range(ROW_PIECES):
            peer_copies[c, r].wait_recv()
            fwd_copies[c, r].start()
        loads.append(load(2, land_ref.at[1, :, cols(c)], rows_buf.at[pl.ds(2 * rows, rows), :]))
        for r in range(ROW_PIECES):
            fwd_copies[c, r].wait_recv()
        loads.append(load(3, land_ref.at[2, :, cols(c)], rows_buf.at[pl.ds(3 * rows, rows), :]))
        for copy in loads:
            copy.wait()

        def whole(i, carry):
            at = pl.ds(pl.multiple_of(i * tile, tile), tile)
            out_ref[at, cols(c)] = jnp.dot(
                mask_ref[at, :], rows_buf[...],
                preferred_element_type=jnp.float32).astype(jnp.bfloat16)
            return carry

        lax.fori_loop(0, rows // tile, whole, 0)

    c = last
    loads = [load(0, x_ref.at[:, cols(c)], rows_buf.at[pl.ds(0, rows), :])]
    mate_copies[c].wait_recv()
    loads.append(load(1, land_ref.at[0, :, cols(c)], rows_buf.at[pl.ds(rows, rows), :]))
    for copy in loads:
        copy.wait()
    peer_copies[c, 0].wait_recv()
    fwd_copies[c, 0].start()

    def near(i, carry):
        at = pl.ds(pl.multiple_of(i * tile, tile), tile)
        sums_buf[at, :] = jnp.dot(mask_ref[at, pl.ds(0, 2 * rows)],
                                  rows_buf[pl.ds(0, 2 * rows), :],
                                  preferred_element_type=jnp.float32)
        return carry

    lax.fori_loop(0, rows // tile, near, 0)
    for r in range(ROW_PIECES):
        if r + 1 < ROW_PIECES:
            peer_copies[c, r + 1].wait_recv()
            fwd_copies[c, r + 1].start()
        fwd_copies[c, r].wait_recv()
        part = pl.ds(r * piece, piece)

        def far(i, carry):
            at = pl.ds(pl.multiple_of(i * tile, tile), tile)
            more = jnp.dot(mask_ref[at, pl.ds(2 * rows + r * piece, piece)], tail_buf[0, part, :],
                           preferred_element_type=jnp.float32)
            more += jnp.dot(mask_ref[at, pl.ds(3 * rows + r * piece, piece)], tail_buf[1, part, :],
                            preferred_element_type=jnp.float32)
            more += sums_buf[at, :]
            if r < ROW_PIECES - 1:
                sums_buf[at, :] = more
            else:
                out_ref[at, cols(c)] = more.astype(jnp.bfloat16)
            return carry

        lax.fori_loop(0, rows // tile, far, 0)
    for c in range(COL_CHUNKS):
        mate_copies[c].wait_send()
        for r in range(ROW_PIECES):
            peer_copies[c, r].wait_send()
            fwd_copies[c, r].wait_send()


def solution(mesh):
    def per_device(sort_keys, seg_ids, payload):
        rows, width = payload.shape
        col_w = width // COL_CHUNKS
        pieces = COL_CHUNKS * ROW_PIECES
        keys = sort_keys.reshape(rows // LANES, LANES)
        segs = seg_ids.reshape(rows // LANES, LANES)
        dma = pltpu.SemaphoreType.DMA
        out, _ = pl.pallas_call(
            kernel,
            out_shape=(pltpu.VMEM((rows, width), jnp.bfloat16),
                       jax.ShapeDtypeStruct((3, rows, width), jnp.bfloat16)),
            in_specs=[pl.BlockSpec(memory_space=pltpu.VMEM)] * 2 + [pl.BlockSpec(memory_space=pl.ANY)],
            out_specs=(pl.BlockSpec(memory_space=pltpu.VMEM), pl.BlockSpec(memory_space=pl.ANY)),
            scratch_shapes=[
                pltpu.VMEM((4, rows // LANES, LANES), jnp.float32),
                pltpu.VMEM((4, rows // LANES, LANES), jnp.int32),
                pltpu.VMEM((rows, 4 * rows), jnp.bfloat16),
                pltpu.VMEM((4 * rows, col_w), jnp.bfloat16),
                pltpu.VMEM((2, rows, col_w), jnp.bfloat16),
                pltpu.VMEM((rows, col_w), jnp.float32),
                dma((6,)), dma((6,)), dma((pieces,)), dma((pieces,)),
                dma((COL_CHUNKS,)), dma((COL_CHUNKS,)), dma((pieces,)), dma((pieces,)),
                dma((4,)),
            ],
            compiler_params=pltpu.CompilerParams(collective_id=0, has_side_effects=True,
                                                 vmem_limit_bytes=52 * 2**20),
        )(keys, segs, payload)
        return out

    row_spec = P(('batch', 'group'))
    mat_spec = P(('batch', 'group'), None)
    return jax.shard_map(per_device, mesh=mesh, in_specs=(row_spec, row_spec, mat_spec),
                         out_specs=mat_spec, check_vma=False)
```

```python
import jax
import jax.numpy as jnp
from jax import lax
from jax.experimental import pallas as pl
from jax.experimental.pallas import tpu as pltpu
from jax.sharding import PartitionSpec as P

MESH = pl.DeviceIdType.MESH
LANES = 128
COL_W = 256
RAW_CHUNKS = 2
BF16_MAX = 3.3895314e38
VMEM_LIMIT = int(55.4 * 2**20)
COL_CHUNKS = 8
ROW_PIECES = 4


def expand(ref, b, q=None):
    row = ref[pl.ds(b, 1), :] if q is None else ref[q, pl.ds(b, 1), :]
    return jnp.broadcast_to(row, (LANES, LANES)).T


def runs_kernel(keys_ref, segs_ref, x_ref, out_ref, flag_ref, land_mate, land_raw, land_one, land_sum,
                all_keys, all_segs, codes, slots, slot_keys, lows, col_keys, col_segs, col_out,
                col_slot, flags, mask_ref, pick_ref, rows_buf, mid_buf, low_buf, near_buf,
                one_buf, sum_buf, sum_in, sums_buf, small_send, small_recv, raw_send, raw_recv,
                rawf_send, rawf_recv, mate_send, mate_recv, run_send, run_recv, runf_send, runf_recv,
                load_sem, near_sem):
    rows, width = x_ref.shape
    key_rows = rows // LANES
    chunks = width // COL_W
    run_chunks = chunks - RAW_CHUNKS
    ones = rows // 4
    sums = land_sum.shape[1]
    sum_pad = 5 * LANES
    head = 2 * LANES
    tile = 512
    inf = jnp.inf
    batch = lax.axis_index('batch')
    me = lax.axis_index('group')
    core = lax.rem(me, 2)
    mate = me + 1 - 2 * core
    peer = lax.rem(me + 2, 4)
    diag = 3 - me

    barrier = pltpu.get_barrier_semaphore()
    for dev in ((batch, mate), (batch, peer), (batch, diag), (1 - batch, me)):
        pl.semaphore_signal(barrier, inc=1, device_id=dev, device_id_type=MESH)
    pl.semaphore_wait(barrier, 4)

    def send(src, dst, ssem, rsem, dev, group=None):
        return pltpu.make_async_remote_copy(src, dst, ssem, rsem,
                                            device_id=(batch if group is None else group, dev),
                                            device_id_type=MESH)

    def small(n, src, dst, dev, group=None):
        return send(src, dst, small_send.at[n], small_recv.at[n], dev, group)

    def cols(c):
        return pl.ds(c * COL_W, COL_W)

    key_copies = []
    for q, dev in ((1, mate), (2, peer), (3, diag)):
        key_copies.append(small(2 * q - 2, keys_ref, all_keys.at[q], dev))
        key_copies.append(small(2 * q - 1, segs_ref, all_segs.at[q], dev))
    for copy in key_copies:
        copy.start()
    raw, raw_fwd, near = [], [], []
    for c in range(RAW_CHUNKS):
        raw.append(send(x_ref.at[:, cols(c)], land_raw.at[0, :, cols(c)], raw_send.at[c],
                        raw_recv.at[c], peer))
        raw_fwd.append(send(land_raw.at[0, :, cols(c)], land_raw.at[1, :, cols(c)], rawf_send.at[c],
                            rawf_recv.at[c], mate))
        raw[c].start()
    for c in range(chunks):
        near.append(send(x_ref.at[:, cols(c)], land_mate.at[:, cols(c)], mate_send.at[c],
                         mate_recv.at[c], mate))
    for c in list(range(RAW_CHUNKS, chunks)) + list(range(RAW_CHUNKS)):
        near[c].start()

    all_keys[0] = keys_ref[...]
    all_segs[0] = segs_ref[...]
    for copy in key_copies:
        copy.wait()

    def code_block(b, carry):
        col_keys[...] = expand(keys_ref, b)
        col_segs[...] = expand(segs_ref, b)

        def half(h, c0):
            at = pl.ds(pl.multiple_of(h * 64, 64), 64)
            own_k = col_keys[at, :]
            own_s = col_segs[at, :]

            def scan(q):
                def step(t, c):
                    above, below, diff = c
                    for u in range(4):
                        k = all_keys[q, pl.ds(t * 4 + u, 1), :]
                        s = all_segs[q, pl.ds(t * 4 + u, 1), :]
                        higher = k > own_k
                        up = jnp.where(higher, k, inf)
                        above = jnp.minimum(above, up)
                        if q == 0:
                            below = jnp.maximum(below, jnp.where(k < own_k, k, -inf))
                        else:
                            below = jnp.maximum(below, jnp.where(higher, -inf, k))
                        diff = jnp.minimum(diff, jnp.where(s != own_s, up, inf))
                    return above, below, diff
                return step

            top = jnp.full((64, LANES), inf, jnp.float32)
            above, below, diff = top, -top, top
            for q in (2, 3):
                above, below, diff = lax.fori_loop(0, key_rows // 4, scan(q), (above, below, diff))
            far_above = jnp.min(above, axis=1, keepdims=True)
            far_below = jnp.max(below, axis=1, keepdims=True)
            above, below = top, -top
            for q in (0, 1):
                above, below, diff = lax.fori_loop(0, key_rows // 4, scan(q), (above, below, diff))
            near_above = jnp.min(above, axis=1, keepdims=True)
            near_below = jnp.max(below, axis=1, keepdims=True)
            diff_above = jnp.min(diff, axis=1, keepdims=True)
            code = jnp.where(near_below <= far_below, 1.0, 2.0)
            code = jnp.where(far_above < near_above, code, 3.0)
            code = jnp.where(far_above < diff_above, code, 0.0)
            col_out[at, :] = jnp.broadcast_to(code, (64, LANES))
            return c0

        lax.fori_loop(0, 2, half, 0)
        codes[0, pl.ds(b, 1), :] = col_out[...].T[0:1, :]
        return carry

    lax.fori_loop(0, key_rows, code_block, 0)
    code_copy = small(6, codes.at[0], codes.at[1], mate)
    code_copy.start()
    code_copy.wait()

    single = jnp.where(codes[0:2] == 1.0, 1.0, 0.0)
    longer = jnp.where(codes[0:2] == 2.0, 1.0, 0.0)

    def total(v):
        v = jnp.sum(v, axis=0)
        v = jnp.sum(v, axis=0, keepdims=True)
        return jnp.sum(v, axis=1, keepdims=True)

    n_single, n_longer = total(single), total(longer)
    spill = n_longer + jnp.maximum(n_single - 2.0 * ones, 0.0)
    full = jnp.where(spill > 2.0 * sums, 1.0, 0.0)
    flags[0] = jnp.broadcast_to(full, (8, LANES))
    codes[2:4] = single + 4096.0 * longer

    def slot_block(b, carry):
        col_keys[...] = expand(keys_ref, b)
        own_k = col_keys[...]

        def step(t, acc):
            for q in range(2):
                for u in range(4):
                    k = all_keys[q, pl.ds(t * 4 + u, 1), :]
                    acc = acc + jnp.where(k < own_k, codes[2 + q, pl.ds(t * 4 + u, 1), :], 0.0)
            return acc

        acc = lax.fori_loop(0, key_rows // 4, step, jnp.zeros((LANES, LANES), jnp.float32))
        acc = jnp.broadcast_to(jnp.sum(acc, axis=1, keepdims=True), (LANES, LANES)).T[0:1, :]
        code = codes[0, pl.ds(b, 1), :]
        before_longer = jnp.floor(acc * (1.0 / 4096.0))
        before_single = acc - 4096.0 * before_longer
        over = 2048.0 + n_longer + before_single - 2.0 * ones
        slot = jnp.where(before_single < 2.0 * ones, before_single, over)
        slot = jnp.where(code == 1.0, slot, 2048.0 + before_longer)
        slots[0, pl.ds(b, 1), :] = jnp.where(code == 0.0, -1.0, slot)
        return carry

    lax.fori_loop(0, key_rows, slot_block, 0)
    slot_copy = small(7, slots.at[0], slots.at[1], mate)
    slot_copy.start()
    flag_copy = small(8, flags.at[0], flags.at[1], peer)
    flag_copy.start()
    col_slot[...] = jnp.full(col_slot.shape, -inf, jnp.float32)

    def near_loads(c, buf, sem):
        return (pltpu.make_async_copy(x_ref.at[:, cols(c)], buf.at[pl.ds(0, rows), :], sem.at[0]),
                pltpu.make_async_copy(land_mate.at[:, cols(c)], buf.at[pl.ds(rows, rows), :], sem.at[1]))

    first_near = near_loads(RAW_CHUNKS, near_buf, near_sem)
    first_near[0].start()
    near[RAW_CHUNKS].wait_recv()
    first_near[1].start()
    slot_copy.wait()

    block = 32

    def pick_block(b, carry):
        base = jnp.where(b < ones // block, core * ones, 2048 + core * sums - ones) + b * block
        want = (lax.broadcasted_iota(jnp.int32, (block, LANES), 0) + base).astype(jnp.float32)
        at = pl.ds(pl.multiple_of(b * block, block), block)

        def step(t, top):
            for q in range(2):
                hit = slots[q, pl.ds(t, 1), :] == want
                to = pl.ds(pl.multiple_of(q * rows + t * LANES, LANES), LANES)
                pick_ref[at, to] = jnp.where(hit, 1.0, 0.0).astype(jnp.bfloat16)
                top = jnp.maximum(top, jnp.where(hit, all_keys[q, pl.ds(t, 1), :], -inf))
            return top

        top = jnp.full((block, LANES), -inf, jnp.float32)
        top = lax.fori_loop(0, key_rows, step, top)
        col_slot[at, :] = jnp.broadcast_to(jnp.max(top, axis=1, keepdims=True), (block, LANES))
        return carry

    lax.fori_loop(0, (ones + sums) // block, pick_block, 0)
    for copy in first_near:
        copy.wait()

    run, run_fwd = {}, {}
    parts = ((0, 0, ones), (1, 0, head), (2, head, sums - head))
    for e in range(run_chunks):
        for kind, lo, n in parts:
            at = pl.ds(lo, n)
            buf, land = (one_buf, land_one) if kind == 0 else (sum_buf, land_sum)
            i = 3 * e + kind
            run[e, kind] = send(buf.at[e % 2, at, :], land.at[0, at, cols(e)], run_send.at[i],
                                run_recv.at[i], peer)
            run_fwd[e, kind] = send(land.at[0, at, cols(e)], land.at[1, at, cols(e)],
                                    runf_send.at[i], runf_recv.at[i], mate)

    def reduce_runs(e, loaded=False):
        if not loaded:
            near[RAW_CHUNKS + e].wait_recv()
            copies = near_loads(RAW_CHUNKS + e, near_buf, near_sem)
            for copy in copies:
                copy.start()
            for copy in copies:
                copy.wait()
        if e >= 2:
            for kind in range(3):
                run[e - 2, kind].wait_send()
        one_buf[e % 2] = jnp.dot(pick_ref[pl.ds(0, ones), :], near_buf[...],
                                 preferred_element_type=jnp.float32).astype(jnp.bfloat16)
        sum_buf[e % 2] = jnp.dot(pick_ref[pl.ds(ones, sums), :], near_buf[...],
                                 preferred_element_type=jnp.float32)
        for kind in range(3):
            run[e, kind].start()

    reduce_runs(0, loaded=True)

    for t in range((ones + sum_pad) // LANES):
        slot_keys[0, pl.ds(t, 1), :] = col_slot[pl.ds(t * LANES, LANES), :].T[0:1, :]
    raw[0].wait_recv()
    raw_fwd[0].start()
    slot_key_copies = (small(9, slot_keys.at[0], slot_keys.at[1], peer),
                       small(10, slot_keys.at[0], slot_keys.at[2], diag))
    for copy in slot_key_copies:
        copy.start()
    reduce_runs(1)

    flag_copy.wait()
    flags[2] = jnp.maximum(flags[0], flags[1])
    flag_all = small(11, flags.at[2], flags.at[3], me, 1 - batch)
    flag_all.start()

    def write_mask(b, tiles):
        own_k = col_keys[...]
        low = col_out[...]
        at = pl.ds(pl.multiple_of(b * LANES, LANES), LANES)
        for k, column in tiles:
            inside = jnp.logical_and(k <= own_k, k > low)
            to = pl.ds(pl.multiple_of(column, LANES), LANES)
            mask_ref[at, to] = jnp.where(inside, 1.0, 0.0).astype(jnp.bfloat16)

    def low_block(b, carry):
        col_keys[...] = expand(keys_ref, b)
        col_segs[...] = expand(segs_ref, b)
        own_k = col_keys[...]
        own_s = col_segs[...]

        def scan(t, low):
            for q in range(4):
                for u in range(2):
                    k = all_keys[q, pl.ds(t * 2 + u, 1), :]
                    s = all_segs[q, pl.ds(t * 2 + u, 1), :]
                    other = jnp.logical_and(k < own_k, s != own_s)
                    low = jnp.maximum(low, jnp.where(other, k, -inf))
            return low

        low = lax.fori_loop(0, key_rows // 2, scan, jnp.full((LANES, LANES), -inf, jnp.float32))
        low = jnp.broadcast_to(jnp.max(low, axis=1, keepdims=True), (LANES, LANES))
        col_out[...] = low
        lows[pl.ds(b, 1), :] = low.T[0:1, :]

        def fill(t, c):
            write_mask(b, [(all_keys[q, pl.ds(t, 1), :], q * rows + t * LANES) for q in range(4)])
            return c

        lax.fori_loop(0, key_rows, fill, 0)
        return carry

    lax.fori_loop(0, key_rows, low_block, 0)
    for c in range(1, RAW_CHUNKS):
        raw[c].wait_recv()
        raw_fwd[c].start()
    reduce_runs(2)

    def load(n, src, dst):
        copy = pltpu.make_async_copy(src, dst, load_sem.at[n])
        copy.start()
        return copy

    def finish(copies):
        for copy in copies:
            copy.wait()

    def tiles_loop(body):
        def step(i, carry):
            body(pl.ds(pl.multiple_of(i * tile, tile), tile))
            return carry
        lax.fori_loop(0, rows // tile, step, 0)

    def dot(at, start, size, buf, offset):
        return jnp.dot(mask_ref[at, pl.ds(start, size)], buf[pl.ds(offset, size), :],
                       preferred_element_type=jnp.float32)

    for c in range(RAW_CHUNKS):
        near[c].wait_recv()
        raw_fwd[c].wait_recv()
        finish([load(0, x_ref.at[:, cols(c)], rows_buf.at[pl.ds(0, rows), :]),
                load(1, land_mate.at[:, cols(c)], rows_buf.at[pl.ds(rows, rows), :]),
                load(2, land_raw.at[0, :, cols(c)], rows_buf.at[pl.ds(2 * rows, rows), :]),
                load(3, land_raw.at[1, :, cols(c)], rows_buf.at[pl.ds(3 * rows, rows), :])])

        def whole(at):
            out_ref[at, cols(c)] = dot(at, 0, 4 * rows, rows_buf, 0).astype(jnp.bfloat16)

        tiles_loop(whole)

    reduce_runs(3)

    ones_at = 2 * rows
    sums_at = ones_at + 2 * ones
    run_cols = 2 * sum_pad
    for copy in slot_key_copies:
        copy.wait()

    def slot_mask(b, carry):
        col_keys[...] = expand(keys_ref, b)
        col_out[...] = expand(lows, b)
        for s in range(2):
            def fill_one(t, c):
                write_mask(b, [(slot_keys[1 + s, pl.ds(t, 1), :], ones_at + s * ones + t * LANES)])
                return c

            def fill_sum(t, c):
                write_mask(b, [(slot_keys[1 + s, pl.ds(ones // LANES + t, 1), :],
                                sums_at + s * sum_pad + t * LANES)])
                return c

            lax.fori_loop(0, ones // LANES, fill_one, 0)
            lax.fori_loop(0, sum_pad // LANES, fill_sum, 0)
        return carry

    lax.fori_loop(0, key_rows, slot_mask, 0)
    for s in range(2):
        pad = pl.ds(s * sum_pad + sums, sum_pad - sums)
        nothing = jnp.zeros((sum_pad - sums, COL_W), jnp.bfloat16)
        rows_buf[pl.ds(sums_at + s * sum_pad + sums, sum_pad - sums), :] = nothing
        mid_buf[pad, :] = nothing
        low_buf[pad, :] = nothing

    def split(lo, n):
        for s in range(2):
            def step(i, carry):
                at = pl.multiple_of(lo + i * 32, 32)
                v = sum_in[s, pl.ds(at, 32), :]
                high = jnp.clip(v, -BF16_MAX, BF16_MAX).astype(jnp.bfloat16)
                rest = v - high.astype(jnp.float32)
                mid = rest.astype(jnp.bfloat16)
                low = (rest - mid.astype(jnp.float32)).astype(jnp.bfloat16)
                rows_buf[pl.ds(pl.multiple_of(sums_at + s * sum_pad + at, 32), 32), :] = high
                mid_buf[pl.ds(pl.multiple_of(s * sum_pad + at, 32), 32), :] = mid
                low_buf[pl.ds(pl.multiple_of(s * sum_pad + at, 32), 32), :] = low
                return carry
            lax.fori_loop(0, n // 32, step, 0)

    def run_load(e, kind, n):
        _, lo, size = parts[kind]
        out = []
        for s in range(2):
            if kind == 0:
                dst = rows_buf.at[pl.ds(ones_at + s * ones, ones), :]
                out.append(load(n + s, land_one.at[s, :, cols(e)], dst))
            else:
                at = pl.ds(lo, size)
                out.append(load(n + s, land_sum.at[s, at, cols(e)], sum_in.at[s, at, :]))
        return out

    def forward(e, kind):
        run[e, kind].wait_recv()
        run_fwd[e, kind].start()

    last = run_chunks - 1
    for kind in range(3):
        forward(0, kind)
    for e in range(last):
        c = RAW_CHUNKS + e
        copies = [load(0, x_ref.at[:, cols(c)], rows_buf.at[pl.ds(0, rows), :]),
                  load(1, land_mate.at[:, cols(c)], rows_buf.at[pl.ds(rows, rows), :])]
        if e > 0:
            for kind in range(3):
                forward(e, kind)
        for kind in range(3):
            run_fwd[e, kind].wait_recv()
            copies += run_load(e, kind, 2 + 2 * kind)
        finish(copies)
        split(0, sums)

        def whole_runs(at):
            acc = dot(at, 0, sums_at + run_cols, rows_buf, 0)
            acc += dot(at, sums_at, run_cols, mid_buf, 0)
            acc += dot(at, sums_at, run_cols, low_buf, 0)
            out_ref[at, cols(c)] = acc.astype(jnp.bfloat16)

        tiles_loop(whole_runs)
        if e + 4 < run_chunks:
            reduce_runs(e + 4)

    c = chunks - 1
    finish([load(0, x_ref.at[:, cols(c)], rows_buf.at[pl.ds(0, rows), :]),
            load(1, land_mate.at[:, cols(c)], rows_buf.at[pl.ds(rows, rows), :])])

    def near_rows(at):
        sums_buf[at, :] = dot(at, 0, 2 * rows, rows_buf, 0)

    tiles_loop(near_rows)
    forward(last, 0)
    forward(last, 1)
    run_fwd[last, 0].wait_recv()
    run_fwd[last, 1].wait_recv()
    finish(run_load(last, 0, 2) + run_load(last, 1, 4))
    split(0, head)

    def first_runs(at):
        acc = sums_buf[at, :] + dot(at, ones_at, 2 * ones, rows_buf, ones_at)
        for s in range(2):
            col = sums_at + s * sum_pad
            acc += dot(at, col, head, rows_buf, col)
            acc += dot(at, col, head, mid_buf, s * sum_pad)
            acc += dot(at, col, head, low_buf, s * sum_pad)
        sums_buf[at, :] = acc

    tiles_loop(first_runs)
    forward(last, 2)
    run_fwd[last, 2].wait_recv()
    finish(run_load(last, 2, 2))
    split(head, sums - head)

    def last_runs(at):
        acc = sums_buf[at, :]
        for s in range(2):
            col = sums_at + s * sum_pad + head
            acc += dot(at, col, sum_pad - head, rows_buf, col)
            acc += dot(at, col, sum_pad - head, mid_buf, s * sum_pad + head)
            acc += dot(at, col, sum_pad - head, low_buf, s * sum_pad + head)
        out_ref[at, cols(c)] = acc.astype(jnp.bfloat16)

    tiles_loop(last_runs)
    flag_all.wait()
    flag_ref[...] = jnp.maximum(flags[2], flags[3])
    for copy in raw + raw_fwd + near:
        copy.wait_send()
    for e in range(run_chunks):
        for kind in range(3):
            if e >= run_chunks - 2:
                run[e, kind].wait_send()
            run_fwd[e, kind].wait_send()


def rows_kernel(keys_ref, segs_ref, x_ref, out_ref, land_ref, all_keys, all_segs,
           mask_ref, rows_buf, sums_buf, out_buf, key_send, key_recv, peer_send, peer_recv,
           mate_send, mate_recv, fwd_send, fwd_recv, load_sem, store_sem):
    rows, width = x_ref.shape
    col_w = width // COL_CHUNKS
    piece = rows // ROW_PIECES
    key_rows = rows // LANES
    batch = lax.axis_index('batch')
    me = lax.axis_index('group')
    mate = me + 1 - 2 * lax.rem(me, 2)
    peer = lax.rem(me + 2, 4)
    diag = 3 - me

    barrier = pltpu.get_barrier_semaphore()
    for other in (mate, peer, diag):
        pl.semaphore_signal(barrier, inc=1, device_id=(batch, other), device_id_type=MESH)
    pl.semaphore_wait(barrier, 3)

    def send(src, dst, ssem, rsem, dev):
        return pltpu.make_async_remote_copy(src, dst, ssem, rsem, device_id=(batch, dev),
                                            device_id_type=MESH)

    key_copies = []
    for q, dev in ((1, mate), (2, peer), (3, diag)):
        key_copies.append(send(keys_ref, all_keys.at[q], key_send.at[2 * q - 2],
                               key_recv.at[2 * q - 2], dev))
        key_copies.append(send(segs_ref, all_segs.at[q], key_send.at[2 * q - 1],
                               key_recv.at[2 * q - 1], dev))
    for copy in key_copies:
        copy.start()

    def cols(c):
        return pl.ds(c * col_w, col_w)

    peer_copies, mate_copies, fwd_copies = {}, {}, {}
    for c in range(COL_CHUNKS):
        for r in range(ROW_PIECES):
            part = (pl.ds(r * piece, piece), cols(c))
            n = c * ROW_PIECES + r
            peer_copies[c, r] = send(x_ref.at[part], land_ref.at[(1,) + part],
                                     peer_send.at[n], peer_recv.at[n], peer)
            fwd_copies[c, r] = send(land_ref.at[(1,) + part], land_ref.at[(2,) + part],
                                    fwd_send.at[n], fwd_recv.at[n], mate)
            peer_copies[c, r].start()
        mate_copies[c] = send(x_ref.at[:, cols(c)], land_ref.at[0, :, cols(c)],
                              mate_send.at[c], mate_recv.at[c], mate)
        mate_copies[c].start()

    all_keys[0] = keys_ref[...]
    all_segs[0] = segs_ref[...]
    for copy in key_copies:
        copy.wait()

    def low_block(b, carry):
        own_k = jnp.broadcast_to(keys_ref[pl.ds(b, 1), :], (LANES, LANES)).T
        own_s = jnp.broadcast_to(segs_ref[pl.ds(b, 1), :], (LANES, LANES)).T

        def scan_keys(t, low):
            for q in range(4):
                k = all_keys[q, pl.ds(t, 1), :]
                s = all_segs[q, pl.ds(t, 1), :]
                other = jnp.logical_and(k < own_k, s != own_s)
                low = jnp.maximum(low, jnp.where(other, k, -jnp.inf))
            return low

        low = lax.fori_loop(0, key_rows, scan_keys, jnp.full((LANES, LANES), -jnp.inf, jnp.float32))
        low = jnp.broadcast_to(jnp.max(low, axis=1, keepdims=True), (LANES, LANES))
        at = pl.ds(pl.multiple_of(b * LANES, LANES), LANES)

        def mask_keys(t, c):
            for q in range(4):
                k = all_keys[q, pl.ds(t, 1), :]
                inside = jnp.logical_and(k <= own_k, k > low)
                to = pl.ds(pl.multiple_of(q * rows + t * LANES, LANES), LANES)
                mask_ref[at, to] = jnp.where(inside, 1.0, 0.0).astype(jnp.bfloat16)
            return c

        lax.fori_loop(0, key_rows, mask_keys, 0)
        return carry

    lax.fori_loop(0, key_rows, low_block, 0)

    tile = 256
    stores = []

    def load(n, src, dst):
        copy = pltpu.make_async_copy(src, dst, load_sem.at[n])
        copy.start()
        return copy

    def flush(c):
        copy = pltpu.make_async_copy(out_buf.at[c % 2], out_ref.at[:, cols(c)], store_sem.at[c % 2])
        copy.start()
        stores.append(copy)

    last = COL_CHUNKS - 1
    for c in range(COL_CHUNKS):
        if c >= 2:
            stores[c - 2].wait()
        loads = [load(0, x_ref.at[:, cols(c)], rows_buf.at[pl.ds(0, rows), :])]
        mate_copies[c].wait_recv()
        loads.append(load(1, land_ref.at[0, :, cols(c)], rows_buf.at[pl.ds(rows, rows), :]))
        if c < last:
            for r in range(ROW_PIECES):
                peer_copies[c, r].wait_recv()
                fwd_copies[c, r].start()
            loads.append(load(2, land_ref.at[1, :, cols(c)], rows_buf.at[pl.ds(2 * rows, rows), :]))
            for r in range(ROW_PIECES):
                fwd_copies[c, r].wait_recv()
            loads.append(load(3, land_ref.at[2, :, cols(c)], rows_buf.at[pl.ds(3 * rows, rows), :]))
            for copy in loads:
                copy.wait()

            def whole(i, carry):
                at = pl.ds(pl.multiple_of(i * tile, tile), tile)
                out_buf[c % 2, at, :] = jnp.dot(
                    mask_ref[at, :], rows_buf[...],
                    preferred_element_type=jnp.float32).astype(jnp.bfloat16)
                return carry

            lax.fori_loop(0, rows // tile, whole, 0)
        else:
            for copy in loads:
                copy.wait()

            def near(i, carry):
                at = pl.ds(pl.multiple_of(i * tile, tile), tile)
                sums_buf[at, :] = jnp.dot(mask_ref[at, pl.ds(0, 2 * rows)],
                                          rows_buf[pl.ds(0, 2 * rows), :],
                                          preferred_element_type=jnp.float32)
                return carry

            lax.fori_loop(0, rows // tile, near, 0)
            for r in range(ROW_PIECES):
                part = (pl.ds(r * piece, piece), cols(c))
                from_peer = pl.ds(2 * rows + r * piece, piece)
                from_diag = pl.ds(3 * rows + r * piece, piece)
                peer_copies[c, r].wait_recv()
                fwd_copies[c, r].start()
                one = load(2, land_ref.at[(1,) + part], rows_buf.at[from_peer, :])
                fwd_copies[c, r].wait_recv()
                two = load(3, land_ref.at[(2,) + part], rows_buf.at[from_diag, :])
                one.wait()
                two.wait()

                def far(i, carry):
                    at = pl.ds(pl.multiple_of(i * tile, tile), tile)
                    more = jnp.dot(mask_ref[at, from_peer], rows_buf[from_peer, :],
                                   preferred_element_type=jnp.float32)
                    more += jnp.dot(mask_ref[at, from_diag], rows_buf[from_diag, :],
                                    preferred_element_type=jnp.float32)
                    more += sums_buf[at, :]
                    if r < ROW_PIECES - 1:
                        sums_buf[at, :] = more
                    else:
                        out_buf[c % 2, at, :] = more.astype(jnp.bfloat16)
                    return carry

                lax.fori_loop(0, rows // tile, far, 0)
        flush(c)
    for copy in stores[-2:]:
        copy.wait()
    for c in range(COL_CHUNKS):
        mate_copies[c].wait_send()
        for r in range(ROW_PIECES):
            peer_copies[c, r].wait_send()
            fwd_copies[c, r].wait_send()


def solution(mesh):
    dma = pltpu.SemaphoreType.DMA
    any_spec = pl.BlockSpec(memory_space=pl.ANY)
    vmem_spec = pl.BlockSpec(memory_space=pltpu.VMEM)
    f32, bf16 = jnp.float32, jnp.bfloat16

    def raw_exchange(keys, segs, payload):
        rows, width = payload.shape
        col_w = width // COL_CHUNKS
        pieces = COL_CHUNKS * ROW_PIECES
        out, _ = pl.pallas_call(
            rows_kernel,
            out_shape=(jax.ShapeDtypeStruct((rows, width), bf16),
                       jax.ShapeDtypeStruct((3, rows, width), bf16)),
            in_specs=[vmem_spec, vmem_spec, any_spec],
            out_specs=(any_spec, any_spec),
            scratch_shapes=[
                pltpu.VMEM((4, rows // LANES, LANES), f32),
                pltpu.VMEM((4, rows // LANES, LANES), jnp.int32),
                pltpu.VMEM((rows, 4 * rows), bf16),
                pltpu.VMEM((4 * rows, col_w), bf16),
                pltpu.VMEM((rows, col_w), f32),
                pltpu.VMEM((2, rows, col_w), bf16),
                dma((6,)), dma((6,)), dma((pieces,)), dma((pieces,)),
                dma((COL_CHUNKS,)), dma((COL_CHUNKS,)), dma((pieces,)), dma((pieces,)),
                dma((4,)), dma((2,)),
            ],
            compiler_params=pltpu.CompilerParams(collective_id=1, has_side_effects=True,
                                                 vmem_limit_bytes=52 * 2**20),
        )(keys, segs, payload)
        return out

    def run_exchange(keys, segs, payload):
        rows, width = payload.shape
        ones, sums, sum_pad = rows // 4, rows * 17 // 64, 5 * LANES
        run_chunks = width // COL_W - RAW_CHUNKS
        run_w = run_chunks * COL_W
        shape = jax.ShapeDtypeStruct
        key_shape = (rows // LANES, LANES)
        outs = pl.pallas_call(
            runs_kernel,
            out_shape=(pltpu.VMEM((rows, width), bf16), shape((8, LANES), f32),
                       shape((rows, width), bf16), shape((2, rows, RAW_CHUNKS * COL_W), bf16),
                       shape((2, ones, run_w), bf16), shape((2, sums, run_w), f32)),
            in_specs=[vmem_spec, vmem_spec, any_spec],
            out_specs=(vmem_spec, vmem_spec, any_spec, any_spec, any_spec, any_spec),
            scratch_shapes=[
                pltpu.VMEM((4,) + key_shape, f32), pltpu.VMEM((4,) + key_shape, jnp.int32),
                pltpu.VMEM((4,) + key_shape, f32), pltpu.VMEM((2,) + key_shape, f32),
                pltpu.VMEM((3,) + key_shape, f32), pltpu.VMEM(key_shape, f32),
                pltpu.VMEM((LANES, LANES), f32), pltpu.VMEM((LANES, LANES), jnp.int32),
                pltpu.VMEM((LANES, LANES), f32), pltpu.VMEM((ones + sum_pad, LANES), f32),
                pltpu.VMEM((4, 8, LANES), f32),
                pltpu.VMEM((rows, 4 * rows), bf16), pltpu.VMEM((ones + sums, 2 * rows), bf16),
                pltpu.VMEM((4 * rows, COL_W), bf16), pltpu.VMEM((2 * sum_pad, COL_W), bf16),
                pltpu.VMEM((2 * sum_pad, COL_W), bf16), pltpu.VMEM((2 * rows, COL_W), bf16),
                pltpu.VMEM((2, ones, COL_W), bf16), pltpu.VMEM((2, sums, COL_W), f32),
                pltpu.VMEM((2, sums, COL_W), f32), pltpu.VMEM((rows, COL_W), f32),
                dma((12,)), dma((12,)), dma((RAW_CHUNKS,)), dma((RAW_CHUNKS,)),
                dma((RAW_CHUNKS,)), dma((RAW_CHUNKS,)), dma((width // COL_W,)), dma((width // COL_W,)),
                dma((3 * run_chunks,)), dma((3 * run_chunks,)), dma((3 * run_chunks,)),
                dma((3 * run_chunks,)), dma((8,)), dma((2,)),
            ],
            compiler_params=pltpu.CompilerParams(collective_id=0, has_side_effects=True,
                                                 vmem_limit_bytes=VMEM_LIMIT),
        )(keys, segs, payload)
        return outs[0], outs[1]

    def per_device(sort_keys, seg_ids, payload):
        rows = payload.shape[0]
        keys = sort_keys.reshape(rows // LANES, LANES)
        segs = seg_ids.reshape(rows // LANES, LANES)
        out, full = run_exchange(keys, segs, payload)
        return lax.cond(full[0, 0] > 0.0, raw_exchange, lambda k, s, p: out, keys, segs, payload)

    row_spec = P(('batch', 'group'))
    mat_spec = P(('batch', 'group'), None)
    return jax.shard_map(per_device, mesh=mesh, in_specs=(row_spec, row_spec, mat_spec),
                         out_specs=mat_spec, check_vma=False)
```

```python
import jax
import jax.numpy as jnp
from jax import lax
from jax.experimental import pallas as pl
from jax.experimental.pallas import tpu as pltpu
from jax.sharding import PartitionSpec as P

MESH = pl.DeviceIdType.MESH
LANES = 128
COL_W = 256
LOG_N = 13
BF16_MAX = 3.3895314e38
VMEM_LIMIT = 58400000
f32, bf16 = jnp.float32, jnp.bfloat16


def expand(ref, b, q=None):
    row = ref[pl.ds(b, 1), :] if q is None else ref[q, pl.ds(b, 1), :]
    return jnp.broadcast_to(row, (LANES, LANES)).T


def sort_index():
    sub = lax.broadcasted_iota(jnp.int32, (8, LANES), 0)
    lane = lax.broadcasted_iota(jnp.int32, (8, LANES), 1)
    return sub, lane


def bitonic(arrays):
    sub, lane = sort_index()
    arrays = [list(a) for a in arrays]

    def bit(k, v):
        if k < 3:
            return bool(v >> k & 1)
        if k < 6:
            return (sub >> (k - 3) & 1) == 1
        return (lane >> (k - 6) & 1) == 1

    for size in range(1, LOG_N + 1):
        for j in reversed(range(size)):
            if j < 3:
                for v in range(8):
                    if v >> j & 1:
                        continue
                    w = v | 1 << j
                    swap = arrays[0][v] > arrays[0][w]
                    if size < LOG_N:
                        down = bit(size, v)
                        if isinstance(down, bool):
                            swap = arrays[0][v] < arrays[0][w] if down else swap
                        else:
                            swap = jnp.logical_xor(swap, down)
                    for a in arrays:
                        a[v], a[w] = jnp.where(swap, a[w], a[v]), jnp.where(swap, a[v], a[w])
                continue
            axis, d, n = (0, 1 << (j - 3), 8) if j < 6 else (1, 1 << (j - 6), LANES)
            upper = bit(j, 0)
            for v in range(8):
                other = [jnp.where(upper, pltpu.roll(a[v], d, axis), pltpu.roll(a[v], n - d, axis))
                         for a in arrays]
                keep_max = upper
                if size < LOG_N:
                    down = bit(size, v)
                    if isinstance(down, bool):
                        keep_max = jnp.logical_not(upper) if down else upper
                    else:
                        keep_max = jnp.logical_xor(upper, down)
                take = jnp.logical_xor(other[0] < arrays[0][v], keep_max)
                for a, o in zip(arrays, other):
                    a[v] = jnp.where(take, o, a[v])
    return arrays


def shifted(values, step, fill):
    sub, lane = sort_index()
    if step == 1:
        edge, first = pltpu.roll(values[7], 1, 0), sub == 0
        edge = jnp.where(first, pltpu.roll(edge, 1, 1), edge)
        edge = jnp.where(jnp.logical_and(first, lane == 0), fill, edge)
        return [edge] + values[:7]
    edge, last = pltpu.roll(values[0], 7, 0), sub == 7
    edge = jnp.where(last, pltpu.roll(edge, LANES - 1, 1), edge)
    edge = jnp.where(jnp.logical_and(last, lane == LANES - 1), fill, edge)
    return values[1:] + [edge]


def running(values, op, start, back=False):
    sub, lane = sort_index()
    seq = values[::-1] if back else values
    inc = [seq[0]]
    for x in seq[1:]:
        inc.append(op(inc[-1], x))

    def moved(x, d, axis):
        n = 8 if axis == 0 else LANES
        at = sub if axis == 0 else lane
        if back:
            return jnp.where(at < n - d, pltpu.roll(x, n - d, axis), start)
        return jnp.where(at >= d, pltpu.roll(x, d, axis), start)

    t = inc[-1]
    for d in (1, 2, 4):
        t = op(t, moved(t, d, 0))
    row = t[0:1, :] if back else t[7:8, :]
    u = jnp.broadcast_to(row, (8, LANES))
    for d in (1, 2, 4, 8, 16, 32, 64):
        u = op(u, moved(u, d, 1))
    base = op(moved(u, 1, 1), moved(t, 1, 0))
    out = [op(base, x) for x in inc]
    return out[::-1] if back else out


def cols(c):
    return pl.ds(pl.multiple_of(c * COL_W, COL_W), COL_W)


def block(i, size):
    return pl.ds(pl.multiple_of(i * size, size), size)


def loop(n, body, first=0):
    def step(i, carry):
        body(i)
        return carry
    lax.fori_loop(first, n, step, 0)


def write_mask(mask_ref, at, own_k, low, k, column):
    inside = jnp.logical_and(k <= own_k, k > low)
    to = pl.ds(pl.multiple_of(column, LANES), LANES)
    mask_ref[at, to] = jnp.where(inside, 1.0, 0.0).astype(bf16)


def row_masks(keys_ref, lows, all_keys, mask_ref):
    key_rows = keys_ref.shape[0]
    unroll = 4

    def mask_block(b):
        own_k, low = expand(keys_ref, b), expand(lows, b)

        def fill(t):
            for q in range(all_keys.shape[0]):
                for u in range(unroll):
                    row = t * unroll + u
                    write_mask(mask_ref, block(b, LANES), own_k, low, all_keys[q, pl.ds(row, 1), :],
                               (q * key_rows + row) * LANES)

        loop(key_rows // unroll, fill)

    loop(key_rows, mask_block)


def neighbours():
    batch, me = lax.axis_index('batch'), lax.axis_index('group')
    core = lax.rem(me, 2)
    return batch, me, core, me + 1 - 2 * core, lax.rem(me + 2, 4), 3 - me


def greet(devices):
    barrier = pltpu.get_barrier_semaphore()
    for dev in devices:
        pl.semaphore_signal(barrier, inc=1, device_id=dev, device_id_type=MESH)
    pl.semaphore_wait(barrier, len(devices))


def local(src, dst, sem):
    return pltpu.make_async_copy(src, dst, sem)


def remote(src, dst, ssem, rsem, dev):
    return pltpu.make_async_remote_copy(src, dst, ssem, rsem, device_id=dev, device_id_type=MESH)


def runs_kernel(keys_ref, segs_ref, x_ref, out_ref, flag_ref, lows, all_keys, land_mate, land_raw,
                land_one, land_sum, all_segs, slots, slot_keys, col_slot, flags, mask_ref, pick_ref,
                rows_buf, mid_buf, low_buf, near_buf, one_buf, sum_buf, sum_in, acc_buf, small_send,
                small_recv, raw_send, raw_recv, mate_send, mate_recv, run_send, run_recv, fwd_send,
                fwd_recv, load_sem, near_sem):
    rows, width = x_ref.shape
    key_rows = rows // LANES
    chunks = width // COL_W
    run_chunks = chunks - 1
    ones, sums = land_one.shape[1], land_sum.shape[1]
    main = ones
    tail = sums - main
    ones_at = 2 * rows
    sums_at = ones_at + 2 * ones
    tail_at = sums_at + 2 * main
    run_cols = 2 * main + LANES
    tile = 512
    inf = jnp.inf
    batch, me, core, mate, peer, diag = neighbours()
    mate, peer, diag = (batch, mate), (batch, peer), (batch, diag)
    greet((mate, peer, diag, (1 - batch, me)))

    def small(n, src, dst, dev):
        return remote(src, dst, small_send.at[n], small_recv.at[n], dev)

    key_copies = []
    for q, dev in enumerate((mate, peer, diag)):
        key_copies.append(small(2 * q, keys_ref, all_keys.at[q + 1], dev))
        key_copies.append(small(2 * q + 1, segs_ref, all_segs.at[q + 1], dev))
    for copy in key_copies:
        copy.start()

    raw = remote(x_ref.at[:, cols(0)], land_raw.at[0], raw_send.at[0], raw_recv.at[0], peer)
    raw_fwd = remote(land_raw.at[0], land_raw.at[1], raw_send.at[1], raw_recv.at[1], mate)
    raw.start()

    def near(c):
        return remote(x_ref.at[:, cols(c)], land_mate.at[:, cols(c)], mate_send.at[c],
                      mate_recv.at[c], mate)

    loop(chunks, lambda c: near(c).start(), 1)
    near(0).start()
    all_keys[0] = keys_ref[...]
    all_segs[0] = segs_ref[...]
    for copy in key_copies:
        copy.wait()

    sub, lane = sort_index()
    key_list = [all_keys[v // 2, pl.ds(v % 2 * 8, 8), :] for v in range(8)]
    seg_list = [all_segs[v // 2, pl.ds(v % 2 * 8, 8), :] for v in range(8)]
    place = [(lane * 64 + sub * 8 + v).astype(f32) for v in range(8)]
    key_list, place_list, seg_list = bitonic([key_list, place, seg_list])

    zero, one = jnp.zeros((8, LANES), f32), jnp.ones((8, LANES), f32)
    both = jnp.logical_and

    def flag(c):
        return jnp.where(c, one, zero)

    first_seg = shifted(seg_list, 1, -1)
    before_key = shifted(key_list, 1, -inf)
    starts = [flag(x != y) for x, y in zip(seg_list, first_seg)]
    low_list = running([jnp.where(x > 0, k, -inf) for x, k in zip(starts, before_key)],
                       jnp.maximum, -inf)
    mine = [flag(p - 8.0 * jnp.floor(p * 0.125) < 4.0) for p in place_list]
    mine_before, mine_after = shifted(mine, 1, 0.0), shifted(mine, -1, 0.0)
    starts_after = shifted(starts, -1, 1.0)
    leader = [flag(both(both(m > 0, x == 0), y == 0))
              for m, x, y in zip(mine, mine_after, starts_after)]
    goes_on = [both(x > 0, y == 0) for x, y in zip(mine_after, starts_after)]
    begins = [jnp.logical_or(x == 0, y > 0) for x, y in zip(mine_before, starts)]
    weight = [jnp.where(x > 0, jnp.where(y, 1.0, 4096.0), 0.0) for x, y in zip(leader, begins)]
    counted = [x - y for x, y in zip(running(weight, jnp.add, 0.0), weight)]
    stop = [jnp.where(x > 0, 2.0 * p, jnp.where(both(m > 0, jnp.logical_not(g)), 2.0 * p + 1.0, 32768.0))
            for x, p, m, g in zip(leader, place, mine, goes_on)]
    stop = running(stop, jnp.minimum, 32768.0, back=True)
    needed = [both(m > 0, x - 2.0 * jnp.floor(x * 0.5) == 0.0) for m, x in zip(mine, stop)]

    def total(values):
        v = values[0]
        for x in values[1:]:
            v = v + x
        return jnp.sum(jnp.sum(v, axis=0, keepdims=True), axis=1, keepdims=True)

    n_single = total([flag(w == 1.0) for w in weight])
    n_longer = total([flag(w == 4096.0) for w in weight])
    spill = n_longer + jnp.maximum(n_single - 2.0 * ones, 0.0)
    flags[0] = jnp.broadcast_to(jnp.where(spill > 2.0 * sums, 1.0, 0.0), (8, LANES))

    float32_slots = float(rows)
    slot_list = []
    for w, c, m in zip(weight, counted, needed):
        before_longer = jnp.floor(c * (1.0 / 4096.0))
        before_single = c - 4096.0 * before_longer
        over = float32_slots + n_longer + before_single - 2.0 * ones
        slot = jnp.where(before_single < 2.0 * ones, before_single, over)
        slot = jnp.where(w == 1.0, slot, float32_slots + before_longer)
        slot_list.append(jnp.where(m, slot, -1.0))
    _, low_list, slot_list = bitonic([place_list, low_list, slot_list])
    for v in range(2):
        lows[pl.ds(v * 8, 8), :] = low_list[v]
    for v in range(4):
        slots[v // 2, pl.ds(v % 2 * 8, 8), :] = slot_list[v]
    flag_copy = small(6, flags.at[0], flags.at[1], peer)
    flag_copy.start()

    def near_loads(c, buf, sem):
        return (local(x_ref.at[:, cols(c)], buf.at[pl.ds(0, rows), :], sem.at[0]),
                local(land_mate.at[:, cols(c)], buf.at[pl.ds(rows, rows), :], sem.at[1]))

    def start_near(c, buf, sem):
        for copy in near_loads(c, buf, sem):
            copy.start()

    def wait_near(c, buf, sem):
        for copy in near_loads(c, buf, sem):
            copy.wait()

    near(1).wait_recv()
    start_near(1, near_buf, near_sem)

    size, unroll = 32, 4
    col_slot[...] = jnp.full(col_slot.shape, -inf, f32)

    def pick_block(b):
        base = jnp.where(b < ones // size, core * ones, rows + core * sums - ones) + b * size
        want = (lax.broadcasted_iota(jnp.int32, (size, LANES), 0) + base).astype(f32)

        def step(t, top):
            for q in range(2):
                for u in range(unroll):
                    row = t * unroll + u
                    hit = slots[q, pl.ds(row, 1), :] == want
                    pick_ref[block(b, size), block(q * key_rows + row, LANES)] = jnp.where(
                        hit, 1.0, 0.0).astype(bf16)
                    top = jnp.maximum(top, jnp.where(hit, all_keys[q, pl.ds(row, 1), :], -inf))
            return top

        top = lax.fori_loop(0, key_rows // unroll, step, jnp.full((size, LANES), -inf, f32))
        col_slot[block(b, size), :] = jnp.broadcast_to(jnp.max(top, axis=1, keepdims=True),
                                                       (size, LANES))

    loop((ones + sums) // size, pick_block)

    for t in range(col_slot.shape[0] // LANES):
        slot_keys[0, pl.ds(t, 1), :] = col_slot[pl.ds(t * LANES, LANES), :].T[0:1, :]
    slot_key_copies = (small(7, slot_keys.at[0], slot_keys.at[1], peer),
                       small(8, slot_keys.at[0], slot_keys.at[2], diag))
    for copy in slot_key_copies:
        copy.start()

    parts = ((0, ones), (0, main // 2), (main // 2, main // 2), (main, tail))

    def run(e, kind):
        at = pl.ds(*parts[kind])
        buf, land = (sum_buf, land_sum) if kind else (one_buf, land_one)
        return remote(buf.at[lax.rem(e, 2), at, :], land.at[0, at, cols(e)], run_send.at[kind, e],
                      run_recv.at[kind, e], peer)

    def fwd(e, kind):
        at = pl.ds(*parts[kind])
        land = land_sum if kind else land_one
        return remote(land.at[0, at, cols(e)], land.at[1, at, cols(e)], fwd_send.at[kind, e],
                      fwd_recv.at[kind, e], mate)

    kinds = range(len(parts))

    def reduce_runs(e):
        wait_near(e + 1, near_buf, near_sem)
        slot = lax.rem(e, 2)
        one_buf[slot] = jnp.dot(pick_ref[pl.ds(0, ones), :], near_buf[...],
                                preferred_element_type=f32).astype(bf16)
        sum_buf[slot] = jnp.dot(pick_ref[pl.ds(ones, sums), :], near_buf[...],
                                preferred_element_type=f32)
        for kind in kinds:
            run(e, kind).start()

    def next_near(e):
        near(e + 1).wait_recv()
        start_near(e + 1, near_buf, near_sem)

    def reduce_first(e):
        reduce_runs(e)
        next_near(e + 1)

    loop(2, reduce_first)

    near(0).wait_recv()
    start_near(0, rows_buf, load_sem)
    row_masks(keys_ref, lows, all_keys, mask_ref)
    raw.wait_recv()
    raw_fwd.start()

    def tiles_loop(body):
        loop(rows // tile, lambda i: body(block(i, tile)))

    def dot(at, start, n, buf, offset):
        return jnp.dot(mask_ref[at, pl.ds(start, n)], buf[pl.ds(offset, n), :],
                       preferred_element_type=f32)

    def raw_load(s):
        return local(land_raw.at[s], rows_buf.at[pl.ds((2 + s) * rows, rows), :], load_sem.at[2 + s])

    raw_load(0).start()
    raw_fwd.wait_recv()
    raw_load(1).start()
    wait_near(0, rows_buf, load_sem)
    raw_load(0).wait()
    raw_load(1).wait()

    def whole(at):
        out_ref[at, cols(0)] = dot(at, 0, mask_ref.shape[1], rows_buf, 0).astype(bf16)

    tiles_loop(whole)
    start_near(1, rows_buf, load_sem)

    for copy in slot_key_copies:
        copy.wait()

    def slot_mask(b):
        own_k, low = expand(keys_ref, b), expand(lows, b)
        for s in range(2):
            for t in range((ones + main) // LANES):
                column = t * LANES + s * ones + (ones_at if t < ones // LANES else sums_at - ones)
                write_mask(mask_ref, block(b, LANES), own_k, low, slot_keys[1 + s, pl.ds(t, 1), :],
                           column)
        t = (ones + main) // LANES
        ends = [slot_keys[1 + s, pl.ds(t, 1), :] for s in range(2)]
        ends = jnp.where(lax.broadcasted_iota(jnp.int32, ends[0].shape, 1) < tail, ends[0],
                         pltpu.roll(jnp.broadcast_to(ends[1], (8, LANES)), tail, 1)[0:1, :])
        write_mask(mask_ref, block(b, LANES), own_k, low, ends, tail_at)

    loop(key_rows, slot_mask)
    pad = LANES - 2 * tail
    for buf, end in ((rows_buf, tail_at + LANES), (mid_buf, run_cols), (low_buf, run_cols)):
        buf[pl.ds(end - pad, pad), :] = jnp.zeros((pad, COL_W), bf16)

    def split(kind, s):
        lo, n = parts[kind]
        offset = (2 * main + s * tail - lo) if lo == main else s * main

        def step(i):
            at = lo + i * size
            v = sum_in[s, block(lo // size + i, size), :]
            high = jnp.clip(v, -BF16_MAX, BF16_MAX).astype(bf16)
            rest = v - high.astype(f32)
            mid = rest.astype(bf16)
            to = pl.multiple_of(at + offset, size)
            rows_buf[pl.ds(sums_at + to, size), :] = high
            mid_buf[pl.ds(to, size), :] = mid
            low_buf[pl.ds(to, size), :] = (rest - mid.astype(f32)).astype(bf16)

        loop(n // size, step)

    def run_load(e, kind, s):
        at = pl.ds(*parts[kind])
        if kind:
            src, dst = land_sum.at[s, at, cols(e)], sum_in.at[s, at, :]
        else:
            src, dst = land_one.at[s, :, cols(e)], rows_buf.at[pl.ds(ones_at + s * ones, ones), :]
        return local(src, dst, load_sem.at[2 + 2 * kind + s])

    def receive(e, kind):
        run(e, kind).wait_recv()
        fwd(e, kind).start()
        run_load(e, kind, 0).start()

    def arrive(e, kind):
        fwd(e, kind).wait_recv()
        run_load(e, kind, 1).start()

    def take(e, kind):
        for s in range(2):
            run_load(e, kind, s).wait()
            if kind:
                split(kind, s)

    def add_chunk(e):
        for kind in kinds:
            arrive(e, kind)
        wait_near(e + 1, rows_buf, load_sem)
        for kind in kinds:
            take(e, kind)

        def whole_runs(at):
            acc = dot(at, 0, tail_at + LANES, rows_buf, 0)
            acc += dot(at, sums_at, run_cols, mid_buf, 0)
            acc += dot(at, sums_at, run_cols, low_buf, 0)
            out_ref[at, cols(e + 1)] = acc.astype(bf16)

        tiles_loop(whole_runs)
        start_near(e + 2, rows_buf, load_sem)

    def steady(e):
        for kind in kinds:
            receive(e, kind)
        for kind in kinds:
            run(e, kind).wait_send()
        reduce_runs(e + 2)

        @pl.when(e + 3 < run_chunks)
        def _():
            next_near(e + 3)

        add_chunk(e)

    loop(run_chunks - 2, steady)
    flag_copy.wait()
    flags[2] = jnp.maximum(flags[0], flags[1])
    flag_all = small(9, flags.at[2], flags.at[3], (1 - batch, me))
    flag_all.start()

    last = run_chunks - 1
    for kind in kinds:
        receive(last - 1, kind)
    add_chunk(last - 1)

    wait_near(chunks - 1, rows_buf, load_sem)

    def near_rows(at):
        acc_buf[at, :] = dot(at, 0, 2 * rows, rows_buf, 0)

    tiles_loop(near_rows)
    receive(last, 0)
    receive(last, 1)
    for kind in range(2):
        arrive(last, kind)
        take(last, kind)

    def add_sums(acc, at, lo, n):
        for s in range(2):
            place = s * main + lo
            acc += dot(at, sums_at + place, n, rows_buf, sums_at + place)
            acc += dot(at, sums_at + place, n, mid_buf, place)
            acc += dot(at, sums_at + place, n, low_buf, place)
        return acc

    def first_runs(at):
        acc = acc_buf[at, :] + dot(at, ones_at, 2 * ones, rows_buf, ones_at)
        acc_buf[at, :] = add_sums(acc, at, *parts[1])

    tiles_loop(first_runs)
    receive(last, 2)
    receive(last, 3)
    arrive(last, 2)
    take(last, 2)
    arrive(last, 3)

    def second_runs(at):
        acc_buf[at, :] = add_sums(acc_buf[at, :], at, *parts[2])

    tiles_loop(second_runs)
    take(last, 3)

    def last_runs(at):
        acc = acc_buf[at, :] + dot(at, tail_at, LANES, rows_buf, tail_at)
        acc += dot(at, tail_at, LANES, mid_buf, 2 * main)
        acc += dot(at, tail_at, LANES, low_buf, 2 * main)
        out_ref[at, cols(chunks - 1)] = acc.astype(bf16)

    tiles_loop(last_runs)
    flag_all.wait()
    flag_ref[...] = jnp.maximum(flags[2], flags[3])
    raw.wait_send()
    raw_fwd.wait_send()
    loop(chunks, lambda c: near(c).wait_send())
    for kind in kinds:
        loop(run_chunks, lambda e: fwd(e, kind).wait_send())
        loop(run_chunks, lambda e: run(e, kind).wait_send(), run_chunks - 2)


def rows_kernel(keys_ref, x_ref, lows, all_keys, out_ref, land_ref, mask_ref, rows_buf, out_buf,
                send_sem, recv_sem, load_sem):
    rows, width = x_ref.shape
    chunks = width // COL_W
    tile = COL_W
    batch, _, _, mate, peer, diag = neighbours()
    mate, peer, diag = (batch, mate), (batch, peer), (batch, diag)
    greet((mate, peer, diag))

    def copy(kind, c):
        if kind < 2:
            src, dst, dev = x_ref.at[:, cols(c)], land_ref.at[kind, :, cols(c)], (mate, peer)[kind]
        else:
            src, dst, dev = land_ref.at[1, :, cols(c)], land_ref.at[2, :, cols(c)], mate
        return remote(src, dst, send_sem.at[kind, c], recv_sem.at[kind, c], dev)

    loop(chunks, lambda c: copy(1, c).start())
    loop(chunks, lambda c: copy(0, c).start())
    row_masks(keys_ref, lows, all_keys, mask_ref)

    def chunk(c):
        copy(1, c).wait_recv()
        copy(2, c).start()
        copy(0, c).wait_recv()
        copy(2, c).wait_recv()
        loads = [local(x_ref.at[:, cols(c)], rows_buf.at[pl.ds(0, rows), :], load_sem.at[0])]
        for q in range(3):
            loads.append(local(land_ref.at[q, :, cols(c)], rows_buf.at[pl.ds((q + 1) * rows, rows), :],
                               load_sem.at[q + 1]))
        for load in loads:
            load.start()
        for load in loads:
            load.wait()

        def whole(i):
            out_buf[block(i, tile), :] = jnp.dot(mask_ref[block(i, tile), :], rows_buf[...],
                                                 preferred_element_type=f32).astype(bf16)

        loop(rows // tile, whole)
        store = local(out_buf, out_ref.at[:, cols(c)], load_sem.at[0])
        store.start()
        store.wait()

    loop(chunks, chunk)
    for kind in range(3):
        loop(chunks, lambda c: copy(kind, c).wait_send())


def solution(mesh):
    dma = pltpu.SemaphoreType.DMA
    any_spec = pl.BlockSpec(memory_space=pl.ANY)
    vmem_spec = pl.BlockSpec(memory_space=pltpu.VMEM)
    shape, vmem = jax.ShapeDtypeStruct, pltpu.VMEM

    def raw_exchange(keys, payload, lows, all_keys):
        rows, width = payload.shape
        chunks = width // COL_W
        out, _ = pl.pallas_call(
            rows_kernel,
            out_shape=(shape((rows, width), bf16), shape((3, rows, width), bf16)),
            in_specs=[vmem_spec, any_spec, vmem_spec, vmem_spec],
            out_specs=(any_spec, any_spec),
            scratch_shapes=[
                vmem((rows, 4 * rows), bf16), vmem((4 * rows, COL_W), bf16), vmem((rows, COL_W), bf16),
                dma((3, chunks)), dma((3, chunks)), dma((4,)),
            ],
            compiler_params=pltpu.CompilerParams(collective_id=1, has_side_effects=True,
                                                 vmem_limit_bytes=VMEM_LIMIT),
        )(keys, payload, lows, all_keys)
        return out

    def run_exchange(keys, segs, payload):
        rows, width = payload.shape
        ones, sums = rows // 4, rows * 17 // 64
        chunks = width // COL_W
        run_w = width - COL_W
        slot_rows = 2 * ones + LANES
        sum_rows = 2 * ones + LANES
        key_shape = keys.shape
        small, kinds = 10, 4
        return pl.pallas_call(
            runs_kernel,
            out_shape=(vmem((rows, width), bf16), vmem((8, LANES), f32), vmem(key_shape, f32),
                       vmem((4,) + key_shape, f32), shape((rows, width), bf16),
                       shape((2, rows, COL_W), bf16), shape((2, ones, run_w), bf16),
                       shape((2, sums, run_w), f32)),
            in_specs=[vmem_spec, vmem_spec, any_spec],
            out_specs=(vmem_spec,) * 4 + (any_spec,) * 4,
            scratch_shapes=[
                vmem((4,) + key_shape, jnp.int32), vmem((2,) + key_shape, f32),
                vmem((3,) + key_shape, f32), vmem((slot_rows, LANES), f32), vmem((4, 8, LANES), f32),
                vmem((rows, 4 * rows), bf16), vmem((ones + sums, 2 * rows), bf16),
                vmem((4 * rows, COL_W), bf16), vmem((sum_rows, COL_W), bf16),
                vmem((sum_rows, COL_W), bf16), vmem((2 * rows, COL_W), bf16),
                vmem((2, ones, COL_W), bf16), vmem((2, sums, COL_W), f32),
                vmem((2, sums, COL_W), f32), vmem((rows, COL_W), f32),
                dma((small,)), dma((small,)), dma((2,)), dma((2,)), dma((chunks,)), dma((chunks,)),
                dma((kinds, chunks)), dma((kinds, chunks)), dma((kinds, chunks)), dma((kinds, chunks)),
                dma((small,)), dma((2,)),
            ],
            compiler_params=pltpu.CompilerParams(collective_id=0, has_side_effects=True,
                                                 vmem_limit_bytes=VMEM_LIMIT),
        )(keys, segs, payload)[:4]

    def per_device(sort_keys, seg_ids, payload):
        key_shape = (payload.shape[0] // LANES, LANES)
        keys = sort_keys.reshape(key_shape)
        out, full, lows, all_keys = run_exchange(keys, seg_ids.reshape(key_shape), payload)
        return lax.cond(full[0, 0] > 0.0, raw_exchange, lambda *_: out, keys, payload, lows, all_keys)

    row_spec = P(('batch', 'group'))
    mat_spec = P(('batch', 'group'), None)
    return jax.shard_map(per_device, mesh=mesh, in_specs=(row_spec, row_spec, mat_spec),
                         out_specs=mat_spec, check_vma=False)
```

```python
import jax
import jax.numpy as jnp
from jax import lax
from jax.experimental import pallas as pl
from jax.experimental.pallas import tpu as pltpu
from jax.sharding import PartitionSpec as P

MESH = pl.DeviceIdType.MESH
LANES = 128
COL_W = 256
LOG_N = 13
BF16_MAX = 3.3895314e38
VMEM_LIMIT = 58400000
f32, bf16 = jnp.float32, jnp.bfloat16


def expand(ref, b, q=None):
    row = ref[pl.ds(b, 1), :] if q is None else ref[q, pl.ds(b, 1), :]
    return jnp.broadcast_to(row, (LANES, LANES)).T


def sort_index():
    sub = lax.broadcasted_iota(jnp.int32, (8, LANES), 0)
    lane = lax.broadcasted_iota(jnp.int32, (8, LANES), 1)
    return sub, lane


def bitonic(arrays):
    sub, lane = sort_index()
    arrays = [list(a) for a in arrays]

    def bit(k, v):
        if k < 3:
            return bool(v >> k & 1)
        if k < 6:
            return (sub >> (k - 3) & 1) == 1
        return (lane >> (k - 6) & 1) == 1

    for size in range(1, LOG_N + 1):
        for j in reversed(range(size)):
            if j < 3:
                for v in range(8):
                    if v >> j & 1:
                        continue
                    w = v | 1 << j
                    swap = arrays[0][v] > arrays[0][w]
                    if size < LOG_N:
                        down = bit(size, v)
                        if isinstance(down, bool):
                            swap = arrays[0][v] < arrays[0][w] if down else swap
                        else:
                            swap = jnp.logical_xor(swap, down)
                    for a in arrays:
                        a[v], a[w] = jnp.where(swap, a[w], a[v]), jnp.where(swap, a[v], a[w])
                continue
            axis, d, n = (0, 1 << (j - 3), 8) if j < 6 else (1, 1 << (j - 6), LANES)
            upper = bit(j, 0)
            for v in range(8):
                other = [jnp.where(upper, pltpu.roll(a[v], d, axis), pltpu.roll(a[v], n - d, axis))
                         for a in arrays]
                keep_max = upper
                if size < LOG_N:
                    down = bit(size, v)
                    if isinstance(down, bool):
                        keep_max = jnp.logical_not(upper) if down else upper
                    else:
                        keep_max = jnp.logical_xor(upper, down)
                take = jnp.logical_xor(other[0] < arrays[0][v], keep_max)
                for a, o in zip(arrays, other):
                    a[v] = jnp.where(take, o, a[v])
    return arrays


def shifted(values, step, fill):
    sub, lane = sort_index()
    if step == 1:
        edge, first = pltpu.roll(values[7], 1, 0), sub == 0
        edge = jnp.where(first, pltpu.roll(edge, 1, 1), edge)
        edge = jnp.where(jnp.logical_and(first, lane == 0), fill, edge)
        return [edge] + values[:7]
    edge, last = pltpu.roll(values[0], 7, 0), sub == 7
    edge = jnp.where(last, pltpu.roll(edge, LANES - 1, 1), edge)
    edge = jnp.where(jnp.logical_and(last, lane == LANES - 1), fill, edge)
    return values[1:] + [edge]


def running(values, op, start, back=False):
    sub, lane = sort_index()
    seq = values[::-1] if back else values
    inc = [seq[0]]
    for x in seq[1:]:
        inc.append(op(inc[-1], x))

    def moved(x, d, axis):
        n = 8 if axis == 0 else LANES
        at = sub if axis == 0 else lane
        if back:
            return jnp.where(at < n - d, pltpu.roll(x, n - d, axis), start)
        return jnp.where(at >= d, pltpu.roll(x, d, axis), start)

    t = inc[-1]
    for d in (1, 2, 4):
        t = op(t, moved(t, d, 0))
    row = t[0:1, :] if back else t[7:8, :]
    u = jnp.broadcast_to(row, (8, LANES))
    for d in (1, 2, 4, 8, 16, 32, 64):
        u = op(u, moved(u, d, 1))
    base = op(moved(u, 1, 1), moved(t, 1, 0))
    out = [op(base, x) for x in inc]
    return out[::-1] if back else out


def cols(c):
    return pl.ds(pl.multiple_of(c * COL_W, COL_W), COL_W)


def block(i, size):
    return pl.ds(pl.multiple_of(i * size, size), size)


def loop(n, body, first=0):
    def step(i, carry):
        body(i)
        return carry
    lax.fori_loop(first, n, step, 0)


def write_mask(mask_ref, at, own_k, low, k, column):
    inside = jnp.logical_and(k <= own_k, k > low)
    to = pl.ds(pl.multiple_of(column, LANES), LANES)
    mask_ref[at, to] = jnp.where(inside, 1.0, 0.0).astype(bf16)


def row_masks(keys_ref, lows, all_keys, mask_ref):
    key_rows = keys_ref.shape[0]
    unroll = 4

    def mask_block(b):
        own_k, low = expand(keys_ref, b), expand(lows, b)

        def fill(t):
            for q in range(all_keys.shape[0]):
                for u in range(unroll):
                    row = t * unroll + u
                    write_mask(mask_ref, block(b, LANES), own_k, low, all_keys[q, pl.ds(row, 1), :],
                               (q * key_rows + row) * LANES)

        loop(key_rows // unroll, fill)

    loop(key_rows, mask_block)


def neighbours():
    batch, me = lax.axis_index('batch'), lax.axis_index('group')
    core = lax.rem(me, 2)
    return batch, me, core, me + 1 - 2 * core, lax.rem(me + 2, 4), 3 - me


def greet(devices):
    barrier = pltpu.get_barrier_semaphore()
    for dev in devices:
        pl.semaphore_signal(barrier, inc=1, device_id=dev, device_id_type=MESH)
    pl.semaphore_wait(barrier, len(devices))


def local(src, dst, sem):
    return pltpu.make_async_copy(src, dst, sem)


def remote(src, dst, ssem, rsem, dev):
    return pltpu.make_async_remote_copy(src, dst, ssem, rsem, device_id=dev, device_id_type=MESH)


def runs_kernel(keys_ref, segs_ref, x_ref, out_ref, flag_ref, lows, all_keys, land_mate, land_raw,
                land_one, land_sum, all_segs, slots, slot_keys, col_slot, flags, mask_ref, pick_ref,
                rows_buf, mid_buf, low_buf, near_buf, one_buf, sum_buf, sum_in, acc_buf, small_send,
                small_recv, raw_send, raw_recv, mate_send, mate_recv, run_send, run_recv, fwd_send,
                fwd_recv, load_sem, near_sem):
    rows, width = x_ref.shape
    key_rows = rows // LANES
    chunks = width // COL_W
    run_chunks = chunks - 1
    ones, sums = land_one.shape[1], land_sum.shape[1]
    main = ones
    tail = sums - main
    ones_at = 2 * rows
    sums_at = ones_at + 2 * ones
    tail_at = sums_at + 2 * main
    run_cols = 2 * main + LANES
    tile = 512
    inf = jnp.inf
    batch, me, core, mate, peer, diag = neighbours()
    mate, peer, diag = (batch, mate), (batch, peer), (batch, diag)
    greet((mate, peer, diag, (1 - batch, me)))

    def small(n, src, dst, dev):
        return remote(src, dst, small_send.at[n], small_recv.at[n], dev)

    key_copies = []
    for q, dev in enumerate((mate, peer, diag)):
        key_copies.append(small(2 * q, keys_ref, all_keys.at[q + 1], dev))
        key_copies.append(small(2 * q + 1, segs_ref, all_segs.at[q + 1], dev))
    for copy in key_copies:
        copy.start()

    raw = remote(x_ref.at[:, cols(0)], land_raw.at[0], raw_send.at[0], raw_recv.at[0], peer)
    raw_fwd = remote(land_raw.at[0], land_raw.at[1], raw_send.at[1], raw_recv.at[1], mate)
    raw.start()

    def near(c):
        return remote(x_ref.at[:, cols(c)], land_mate.at[:, cols(c)], mate_send.at[c],
                      mate_recv.at[c], mate)

    loop(chunks, lambda c: near(c).start(), 1)
    near(0).start()
    all_keys[0] = keys_ref[...]
    all_segs[0] = segs_ref[...]
    for copy in key_copies:
        copy.wait()

    sub, lane = sort_index()
    key_list = [all_keys[v // 2, pl.ds(v % 2 * 8, 8), :] for v in range(8)]
    seg_list = [all_segs[v // 2, pl.ds(v % 2 * 8, 8), :] for v in range(8)]
    place = [(lane * 64 + sub * 8 + v).astype(f32) for v in range(8)]
    key_list, place_list, seg_list = bitonic([key_list, place, seg_list])

    zero, one = jnp.zeros((8, LANES), f32), jnp.ones((8, LANES), f32)
    both = jnp.logical_and

    def flag(c):
        return jnp.where(c, one, zero)

    first_seg = shifted(seg_list, 1, -1)
    before_key = shifted(key_list, 1, -inf)
    starts = [flag(x != y) for x, y in zip(seg_list, first_seg)]
    low_list = running([jnp.where(x > 0, k, -inf) for x, k in zip(starts, before_key)],
                       jnp.maximum, -inf)
    mine = [flag(p - 8.0 * jnp.floor(p * 0.125) < 4.0) for p in place_list]
    mine_before, mine_after = shifted(mine, 1, 0.0), shifted(mine, -1, 0.0)
    starts_after = shifted(starts, -1, 1.0)
    leader = [flag(both(both(m > 0, x == 0), y == 0))
              for m, x, y in zip(mine, mine_after, starts_after)]
    goes_on = [both(x > 0, y == 0) for x, y in zip(mine_after, starts_after)]
    begins = [jnp.logical_or(x == 0, y > 0) for x, y in zip(mine_before, starts)]
    weight = [jnp.where(x > 0, jnp.where(y, 1.0, 4096.0), 0.0) for x, y in zip(leader, begins)]
    counted = [x - y for x, y in zip(running(weight, jnp.add, 0.0), weight)]
    stop = [jnp.where(x > 0, 2.0 * p, jnp.where(both(m > 0, jnp.logical_not(g)), 2.0 * p + 1.0, 32768.0))
            for x, p, m, g in zip(leader, place, mine, goes_on)]
    stop = running(stop, jnp.minimum, 32768.0, back=True)
    needed = [both(m > 0, x - 2.0 * jnp.floor(x * 0.5) == 0.0) for m, x in zip(mine, stop)]

    def total(values):
        v = values[0]
        for x in values[1:]:
            v = v + x
        return jnp.sum(jnp.sum(v, axis=0, keepdims=True), axis=1, keepdims=True)

    n_single = total([flag(w == 1.0) for w in weight])
    n_longer = total([flag(w == 4096.0) for w in weight])
    spill = n_longer + jnp.maximum(n_single - 2.0 * ones, 0.0)
    flags[0] = jnp.broadcast_to(jnp.where(spill > 2.0 * sums, 1.0, 0.0), (8, LANES))

    float32_slots = float(rows)
    slot_list = []
    for w, c, m in zip(weight, counted, needed):
        before_longer = jnp.floor(c * (1.0 / 4096.0))
        before_single = c - 4096.0 * before_longer
        over = float32_slots + n_longer + before_single - 2.0 * ones
        slot = jnp.where(before_single < 2.0 * ones, before_single, over)
        slot = jnp.where(w == 1.0, slot, float32_slots + before_longer)
        slot_list.append(jnp.where(m, slot, -1.0))
    _, low_list, slot_list = bitonic([place_list, low_list, slot_list])
    for v in range(2):
        lows[pl.ds(v * 8, 8), :] = low_list[v]
    for v in range(4):
        slots[v // 2, pl.ds(v % 2 * 8, 8), :] = slot_list[v]
    flag_copy = small(6, flags.at[0], flags.at[1], peer)
    flag_copy.start()

    def near_loads(c, buf, sem):
        return (local(x_ref.at[:, cols(c)], buf.at[pl.ds(0, rows), :], sem.at[0]),
                local(land_mate.at[:, cols(c)], buf.at[pl.ds(rows, rows), :], sem.at[1]))

    def start_near(c, buf, sem):
        for copy in near_loads(c, buf, sem):
            copy.start()

    def wait_near(c, buf, sem):
        for copy in near_loads(c, buf, sem):
            copy.wait()

    near(1).wait_recv()
    start_near(1, near_buf, near_sem)

    size, unroll = 16, 4
    col_slot[...] = jnp.full(col_slot.shape, -inf, f32)

    def pick_block(b):
        base = jnp.where(b < ones // size, core * ones, rows + core * sums - ones) + b * size
        want = (lax.broadcasted_iota(jnp.int32, (size, LANES), 0) + base).astype(f32)

        def step(t, top):
            for q in range(2):
                for u in range(unroll):
                    row = t * unroll + u
                    hit = slots[q, pl.ds(row, 1), :] == want
                    pick_ref[block(b, size), block(q * key_rows + row, LANES)] = jnp.where(
                        hit, 1.0, 0.0).astype(bf16)
                    top = jnp.maximum(top, jnp.where(hit, all_keys[q, pl.ds(row, 1), :], -inf))
            return top

        top = lax.fori_loop(0, key_rows // unroll, step, jnp.full((size, LANES), -inf, f32))
        col_slot[block(b, size), :] = jnp.broadcast_to(jnp.max(top, axis=1, keepdims=True),
                                                       (size, LANES))

    loop((ones + sums) // size, pick_block)

    for t in range(col_slot.shape[0] // LANES):
        slot_keys[0, pl.ds(t, 1), :] = col_slot[pl.ds(t * LANES, LANES), :].T[0:1, :]
    slot_key_copies = (small(7, slot_keys.at[0], slot_keys.at[1], peer),
                       small(8, slot_keys.at[0], slot_keys.at[2], diag))
    for copy in slot_key_copies:
        copy.start()

    parts = ((0, ones), (0, main // 2), (main // 2, main // 2), (main, tail))

    def run(e, kind):
        at = pl.ds(*parts[kind])
        buf, land = (sum_buf, land_sum) if kind else (one_buf, land_one)
        return remote(buf.at[lax.rem(e, 2), at, :], land.at[0, at, cols(e)], run_send.at[kind, e],
                      run_recv.at[kind, e], peer)

    def fwd(e, kind):
        at = pl.ds(*parts[kind])
        land = land_sum if kind else land_one
        return remote(land.at[0, at, cols(e)], land.at[1, at, cols(e)], fwd_send.at[kind, e],
                      fwd_recv.at[kind, e], mate)

    kinds = range(len(parts))

    def reduce_runs(e):
        wait_near(e + 1, near_buf, near_sem)
        slot = lax.rem(e, 2)
        one_buf[slot] = jnp.dot(pick_ref[pl.ds(0, ones), :], near_buf[...],
                                preferred_element_type=f32).astype(bf16)
        sum_buf[slot] = jnp.dot(pick_ref[pl.ds(ones, sums), :], near_buf[...],
                                preferred_element_type=f32)
        for kind in kinds:
            run(e, kind).start()

    def next_near(e):
        near(e + 1).wait_recv()
        start_near(e + 1, near_buf, near_sem)

    def reduce_first(e):
        reduce_runs(e)
        next_near(e + 1)

    loop(2, reduce_first)

    near(0).wait_recv()
    start_near(0, rows_buf, load_sem)
    row_masks(keys_ref, lows, all_keys, mask_ref)
    raw.wait_recv()
    raw_fwd.start()

    def tiles_loop(body):
        loop(rows // tile, lambda i: body(block(i, tile)))

    def dot(at, start, n, buf, offset):
        return jnp.dot(mask_ref[at, pl.ds(start, n)], buf[pl.ds(offset, n), :],
                       preferred_element_type=f32)

    def raw_load(s):
        return local(land_raw.at[s], rows_buf.at[pl.ds((2 + s) * rows, rows), :], load_sem.at[2 + s])

    raw_load(0).start()
    raw_fwd.wait_recv()
    raw_load(1).start()
    wait_near(0, rows_buf, load_sem)
    raw_load(0).wait()
    raw_load(1).wait()

    def whole(at):
        out_ref[at, cols(0)] = dot(at, 0, mask_ref.shape[1], rows_buf, 0).astype(bf16)

    tiles_loop(whole)
    start_near(1, rows_buf, load_sem)

    for copy in slot_key_copies:
        copy.wait()

    def slot_mask(b):
        own_k, low = expand(keys_ref, b), expand(lows, b)
        for s in range(2):
            for t in range((ones + main) // LANES):
                column = t * LANES + s * ones + (ones_at if t < ones // LANES else sums_at - ones)
                write_mask(mask_ref, block(b, LANES), own_k, low, slot_keys[1 + s, pl.ds(t, 1), :],
                           column)
        t = (ones + main) // LANES
        ends = [slot_keys[1 + s, pl.ds(t, 1), :] for s in range(2)]
        ends = jnp.where(lax.broadcasted_iota(jnp.int32, ends[0].shape, 1) < tail, ends[0],
                         pltpu.roll(jnp.broadcast_to(ends[1], (8, LANES)), tail, 1)[0:1, :])
        write_mask(mask_ref, block(b, LANES), own_k, low, ends, tail_at)

    loop(key_rows, slot_mask)
    pad = LANES - 2 * tail
    for buf, end in ((rows_buf, tail_at + LANES), (mid_buf, run_cols), (low_buf, run_cols)):
        buf[pl.ds(end - pad, pad), :] = jnp.zeros((pad, COL_W), bf16)

    def split(kind, s):
        lo, n = parts[kind]
        offset = (2 * main + s * tail - lo) if lo == main else s * main

        def step(i):
            at = lo + i * size
            v = sum_in[s, block(lo // size + i, size), :]
            high = jnp.clip(v, -BF16_MAX, BF16_MAX).astype(bf16)
            rest = v - high.astype(f32)
            mid = rest.astype(bf16)
            to = pl.multiple_of(at + offset, size)
            rows_buf[pl.ds(sums_at + to, size), :] = high
            mid_buf[pl.ds(to, size), :] = mid
            low_buf[pl.ds(to, size), :] = (rest - mid.astype(f32)).astype(bf16)

        loop(n // size, step)

    def run_load(e, kind, s):
        at = pl.ds(*parts[kind])
        if kind:
            src, dst = land_sum.at[s, at, cols(e)], sum_in.at[s, at, :]
        else:
            src, dst = land_one.at[s, :, cols(e)], rows_buf.at[pl.ds(ones_at + s * ones, ones), :]
        return local(src, dst, load_sem.at[2 + 2 * kind + s])

    def receive(e, kind):
        run(e, kind).wait_recv()
        fwd(e, kind).start()
        run_load(e, kind, 0).start()

    def arrive(e, kind):
        fwd(e, kind).wait_recv()
        run_load(e, kind, 1).start()

    def take(e, kind):
        for s in range(2):
            run_load(e, kind, s).wait()
            if kind:
                split(kind, s)

    def arrived(e):
        for kind in kinds:
            arrive(e, kind)
        wait_near(e + 1, rows_buf, load_sem)
        for kind in kinds:
            take(e, kind)

    def add_tile(e):
        def whole_runs(i):
            at = block(i, tile)
            acc = dot(at, 0, tail_at + LANES, rows_buf, 0)
            acc += dot(at, sums_at, run_cols, mid_buf, 0)
            acc += dot(at, sums_at, run_cols, low_buf, 0)
            out_ref[at, cols(e + 1)] = acc.astype(bf16)

        return whole_runs

    def steady(e):
        for kind in kinds:
            receive(e, kind)
        for kind in kinds:
            run(e, kind).wait_send()
        reduce_runs(e + 2)

        @pl.when(e + 3 < run_chunks)
        def _():
            next_near(e + 3)

        arrived(e)
        loop(rows // tile, add_tile(e))
        start_near(e + 2, rows_buf, load_sem)

    loop(run_chunks - 2, steady)
    flag_copy.wait()
    flags[2] = jnp.maximum(flags[0], flags[1])
    flag_all = small(9, flags.at[2], flags.at[3], (1 - batch, me))
    flag_all.start()

    last = run_chunks - 1

    def near_rows(at):
        acc_buf[at, :] = dot(at, 0, 2 * rows, near_buf, 0)

    tiles_loop(near_rows)
    for kind in kinds:
        receive(last - 1, kind)
    arrived(last - 1)
    half = rows // tile // 2
    loop(half, add_tile(last - 1))
    run(last, 0).wait_recv()
    fwd(last, 0).start()
    loop(2 * half, add_tile(last - 1), half)
    run_load(last, 0, 0).start()
    receive(last, 1)
    arrive(last, 0)
    take(last, 0)

    def add_sums(acc, at, lo, n):
        for s in range(2):
            place = s * main + lo
            acc += dot(at, sums_at + place, n, rows_buf, sums_at + place)
            acc += dot(at, sums_at + place, n, mid_buf, place)
            acc += dot(at, sums_at + place, n, low_buf, place)
        return acc

    def single_rows(at):
        acc_buf[at, :] += dot(at, ones_at, 2 * ones, rows_buf, ones_at)

    def first_runs(at):
        acc_buf[at, :] = add_sums(acc_buf[at, :], at, *parts[1])

    def second_runs(at):
        acc_buf[at, :] = add_sums(acc_buf[at, :], at, *parts[2])

    tiles_loop(single_rows)
    arrive(last, 1)
    take(last, 1)
    receive(last, 2)
    tiles_loop(first_runs)
    receive(last, 3)
    arrive(last, 2)
    take(last, 2)
    arrive(last, 3)
    tiles_loop(second_runs)
    take(last, 3)

    def last_runs(at):
        acc = acc_buf[at, :] + dot(at, tail_at, LANES, rows_buf, tail_at)
        acc += dot(at, tail_at, LANES, mid_buf, 2 * main)
        acc += dot(at, tail_at, LANES, low_buf, 2 * main)
        out_ref[at, cols(chunks - 1)] = acc.astype(bf16)

    tiles_loop(last_runs)
    flag_all.wait()
    flag_ref[...] = jnp.maximum(flags[2], flags[3])
    raw.wait_send()
    raw_fwd.wait_send()
    loop(chunks, lambda c: near(c).wait_send())
    for kind in kinds:
        loop(run_chunks, lambda e: fwd(e, kind).wait_send())
        loop(run_chunks, lambda e: run(e, kind).wait_send(), run_chunks - 2)


def rows_kernel(keys_ref, x_ref, lows, all_keys, out_ref, land_ref, mask_ref, rows_buf, out_buf,
                send_sem, recv_sem, load_sem):
    rows, width = x_ref.shape
    chunks = width // COL_W
    tile = COL_W
    batch, _, _, mate, peer, diag = neighbours()
    mate, peer, diag = (batch, mate), (batch, peer), (batch, diag)
    greet((mate, peer, diag))

    def copy(kind, c):
        if kind < 2:
            src, dst, dev = x_ref.at[:, cols(c)], land_ref.at[kind, :, cols(c)], (mate, peer)[kind]
        else:
            src, dst, dev = land_ref.at[1, :, cols(c)], land_ref.at[2, :, cols(c)], mate
        return remote(src, dst, send_sem.at[kind, c], recv_sem.at[kind, c], dev)

    loop(chunks, lambda c: copy(1, c).start())
    loop(chunks, lambda c: copy(0, c).start())
    row_masks(keys_ref, lows, all_keys, mask_ref)

    def chunk(c):
        copy(1, c).wait_recv()
        copy(2, c).start()
        copy(0, c).wait_recv()
        copy(2, c).wait_recv()
        loads = [local(x_ref.at[:, cols(c)], rows_buf.at[pl.ds(0, rows), :], load_sem.at[0])]
        for q in range(3):
            loads.append(local(land_ref.at[q, :, cols(c)], rows_buf.at[pl.ds((q + 1) * rows, rows), :],
                               load_sem.at[q + 1]))
        for load in loads:
            load.start()
        for load in loads:
            load.wait()

        def whole(i):
            out_buf[block(i, tile), :] = jnp.dot(mask_ref[block(i, tile), :], rows_buf[...],
                                                 preferred_element_type=f32).astype(bf16)

        loop(rows // tile, whole)
        store = local(out_buf, out_ref.at[:, cols(c)], load_sem.at[0])
        store.start()
        store.wait()

    loop(chunks, chunk)
    for kind in range(3):
        loop(chunks, lambda c: copy(kind, c).wait_send())


def solution(mesh):
    dma = pltpu.SemaphoreType.DMA
    any_spec = pl.BlockSpec(memory_space=pl.ANY)
    vmem_spec = pl.BlockSpec(memory_space=pltpu.VMEM)
    shape, vmem = jax.ShapeDtypeStruct, pltpu.VMEM

    def raw_exchange(keys, payload, lows, all_keys):
        rows, width = payload.shape
        chunks = width // COL_W
        out, _ = pl.pallas_call(
            rows_kernel,
            out_shape=(shape((rows, width), bf16), shape((3, rows, width), bf16)),
            in_specs=[vmem_spec, any_spec, vmem_spec, vmem_spec],
            out_specs=(any_spec, any_spec),
            scratch_shapes=[
                vmem((rows, 4 * rows), bf16), vmem((4 * rows, COL_W), bf16), vmem((rows, COL_W), bf16),
                dma((3, chunks)), dma((3, chunks)), dma((4,)),
            ],
            compiler_params=pltpu.CompilerParams(collective_id=1, has_side_effects=True,
                                                 vmem_limit_bytes=VMEM_LIMIT),
        )(keys, payload, lows, all_keys)
        return out

    def run_exchange(keys, segs, payload):
        rows, width = payload.shape
        ones, sums = rows // 4, rows * 33 // 128
        chunks = width // COL_W
        run_w = width - COL_W
        slot_rows = 2 * ones + LANES
        sum_rows = 2 * ones + LANES
        key_shape = keys.shape
        small, kinds = 10, 4
        return pl.pallas_call(
            runs_kernel,
            out_shape=(vmem((rows, width), bf16), vmem((8, LANES), f32), vmem(key_shape, f32),
                       vmem((4,) + key_shape, f32), shape((rows, width), bf16),
                       shape((2, rows, COL_W), bf16), shape((2, ones, run_w), bf16),
                       shape((2, sums, run_w), f32)),
            in_specs=[vmem_spec, vmem_spec, any_spec],
            out_specs=(vmem_spec,) * 4 + (any_spec,) * 4,
            scratch_shapes=[
                vmem((4,) + key_shape, jnp.int32), vmem((2,) + key_shape, f32),
                vmem((3,) + key_shape, f32), vmem((slot_rows, LANES), f32), vmem((4, 8, LANES), f32),
                vmem((rows, 4 * rows), bf16), vmem((ones + sums, 2 * rows), bf16),
                vmem((4 * rows, COL_W), bf16), vmem((sum_rows, COL_W), bf16),
                vmem((sum_rows, COL_W), bf16), vmem((2 * rows, COL_W), bf16),
                vmem((2, ones, COL_W), bf16), vmem((2, sums, COL_W), f32),
                vmem((2, sums, COL_W), f32), vmem((rows, COL_W), f32),
                dma((small,)), dma((small,)), dma((2,)), dma((2,)), dma((chunks,)), dma((chunks,)),
                dma((kinds, chunks)), dma((kinds, chunks)), dma((kinds, chunks)), dma((kinds, chunks)),
                dma((small,)), dma((2,)),
            ],
            compiler_params=pltpu.CompilerParams(collective_id=0, has_side_effects=True,
                                                 vmem_limit_bytes=VMEM_LIMIT),
        )(keys, segs, payload)[:4]

    def per_device(sort_keys, seg_ids, payload):
        key_shape = (payload.shape[0] // LANES, LANES)
        keys = sort_keys.reshape(key_shape)
        out, full, lows, all_keys = run_exchange(keys, seg_ids.reshape(key_shape), payload)
        return lax.cond(full[0, 0] > 0.0, raw_exchange, lambda *_: out, keys, payload, lows, all_keys)

    row_spec = P(('batch', 'group'))
    mat_spec = P(('batch', 'group'), None)
    return jax.shard_map(per_device, mesh=mesh, in_specs=(row_spec, row_spec, mat_spec),
                         out_specs=mat_spec, check_vma=False)
```

```python
import jax
import jax.numpy as jnp
from jax import lax
from jax.experimental import pallas as pl
from jax.experimental.pallas import tpu as pltpu
from jax.sharding import PartitionSpec as P

MESH = pl.DeviceIdType.MESH
LANES = 128
COL_W = 256
LOG_N = 13
BF16_MAX = 3.3895314e38
VMEM_LIMIT = 58400000
f32, bf16 = jnp.float32, jnp.bfloat16


def expand(ref, b, q=None):
    row = ref[pl.ds(b, 1), :] if q is None else ref[q, pl.ds(b, 1), :]
    return jnp.broadcast_to(row, (LANES, LANES)).T


def sort_index():
    sub = lax.broadcasted_iota(jnp.int32, (8, LANES), 0)
    lane = lax.broadcasted_iota(jnp.int32, (8, LANES), 1)
    return sub, lane


def bitonic(arrays):
    sub, lane = sort_index()
    arrays = [list(a) for a in arrays]

    def bit(k, v):
        if k < 3:
            return bool(v >> k & 1)
        if k < 6:
            return (sub >> (k - 3) & 1) == 1
        return (lane >> (k - 6) & 1) == 1

    for size in range(1, LOG_N + 1):
        for j in reversed(range(size)):
            if j < 3:
                for v in range(8):
                    if v >> j & 1:
                        continue
                    w = v | 1 << j
                    swap = arrays[0][v] > arrays[0][w]
                    if size < LOG_N:
                        down = bit(size, v)
                        if isinstance(down, bool):
                            swap = arrays[0][v] < arrays[0][w] if down else swap
                        else:
                            swap = jnp.logical_xor(swap, down)
                    for a in arrays:
                        a[v], a[w] = jnp.where(swap, a[w], a[v]), jnp.where(swap, a[v], a[w])
                continue
            axis, d, n = (0, 1 << (j - 3), 8) if j < 6 else (1, 1 << (j - 6), LANES)
            upper = bit(j, 0)
            for v in range(8):
                other = [jnp.where(upper, pltpu.roll(a[v], d, axis), pltpu.roll(a[v], n - d, axis))
                         for a in arrays]
                keep_max = upper
                if size < LOG_N:
                    down = bit(size, v)
                    if isinstance(down, bool):
                        keep_max = jnp.logical_not(upper) if down else upper
                    else:
                        keep_max = jnp.logical_xor(upper, down)
                take = jnp.logical_xor(other[0] < arrays[0][v], keep_max)
                for a, o in zip(arrays, other):
                    a[v] = jnp.where(take, o, a[v])
    return arrays


def shifted(values, step, fill):
    sub, lane = sort_index()
    if step == 1:
        edge, first = pltpu.roll(values[7], 1, 0), sub == 0
        edge = jnp.where(first, pltpu.roll(edge, 1, 1), edge)
        edge = jnp.where(jnp.logical_and(first, lane == 0), fill, edge)
        return [edge] + values[:7]
    edge, last = pltpu.roll(values[0], 7, 0), sub == 7
    edge = jnp.where(last, pltpu.roll(edge, LANES - 1, 1), edge)
    edge = jnp.where(jnp.logical_and(last, lane == LANES - 1), fill, edge)
    return values[1:] + [edge]


def running(values, op, start, back=False):
    sub, lane = sort_index()
    seq = values[::-1] if back else values
    inc = [seq[0]]
    for x in seq[1:]:
        inc.append(op(inc[-1], x))

    def moved(x, d, axis):
        n = 8 if axis == 0 else LANES
        at = sub if axis == 0 else lane
        if back:
            return jnp.where(at < n - d, pltpu.roll(x, n - d, axis), start)
        return jnp.where(at >= d, pltpu.roll(x, d, axis), start)

    t = inc[-1]
    for d in (1, 2, 4):
        t = op(t, moved(t, d, 0))
    row = t[0:1, :] if back else t[7:8, :]
    u = jnp.broadcast_to(row, (8, LANES))
    for d in (1, 2, 4, 8, 16, 32, 64):
        u = op(u, moved(u, d, 1))
    base = op(moved(u, 1, 1), moved(t, 1, 0))
    out = [op(base, x) for x in inc]
    return out[::-1] if back else out


def cols(c):
    return pl.ds(pl.multiple_of(c * COL_W, COL_W), COL_W)


def block(i, size):
    return pl.ds(pl.multiple_of(i * size, size), size)


def loop(n, body, first=0):
    def step(i, carry):
        body(i)
        return carry
    lax.fori_loop(first, n, step, 0)


def write_mask(mask_ref, at, own_k, low, k, column):
    inside = jnp.logical_and(k <= own_k, k > low)
    to = pl.ds(pl.multiple_of(column, LANES), LANES)
    mask_ref[at, to] = jnp.where(inside, 1.0, 0.0).astype(bf16)


def row_masks(keys_ref, lows, all_keys, places, between=None):
    key_rows = keys_ref.shape[0]
    unroll = 4

    def mask_block(b):
        own_k, low = expand(keys_ref, b), expand(lows, b)

        def fill(t):
            for q, (ref, first) in enumerate(places):
                for u in range(unroll):
                    row = t * unroll + u
                    write_mask(ref, block(b, LANES), own_k, low, all_keys[q, pl.ds(row, 1), :],
                               row * LANES + first)

        loop(key_rows // unroll, fill)

    if between is None:
        loop(key_rows, mask_block)
    else:
        loop(key_rows // 2, mask_block)
        between()
        loop(key_rows, mask_block, key_rows // 2)


def neighbours():
    batch, me = lax.axis_index('batch'), lax.axis_index('group')
    core = lax.rem(me, 2)
    return batch, me, core, me + 1 - 2 * core, lax.rem(me + 2, 4), 3 - me


def greet(devices):
    barrier = pltpu.get_barrier_semaphore()
    for dev in devices:
        pl.semaphore_signal(barrier, inc=1, device_id=dev, device_id_type=MESH)
    pl.semaphore_wait(barrier, len(devices))


def local(src, dst, sem):
    return pltpu.make_async_copy(src, dst, sem)


def remote(src, dst, ssem, rsem, dev):
    return pltpu.make_async_remote_copy(src, dst, ssem, rsem, device_id=dev, device_id_type=MESH)


def runs_kernel(keys_ref, segs_ref, x_ref, out_ref, flag_ref, lows, all_keys, land_mate, land_raw,
                land_one, land_sum, all_segs, slots, slot_keys, col_slot, flags, mask_ref, pick_ref,
                rows_buf, mid_buf, low_buf, near_buf, one_buf, sum_buf, sum_in, acc_buf, small_send,
                small_recv, raw_send, raw_recv, mate_send, mate_recv, run_send, run_recv, fwd_send,
                fwd_recv, load_sem, near_sem):
    rows, width = x_ref.shape
    key_rows = rows // LANES
    chunks = width // COL_W
    run_chunks = chunks - 1
    ones, sums = land_one.shape[1], land_sum.shape[1]
    main = ones
    tail = sums - main
    ones_at = 2 * rows
    sums_at = ones_at + 2 * ones
    tail_at = sums_at + 2 * main
    run_cols = 2 * main + LANES
    tile = 1024
    inf = jnp.inf
    batch, me, core, mate, peer, diag = neighbours()
    mate, peer, diag = (batch, mate), (batch, peer), (batch, diag)
    greet((mate, peer, diag, (1 - batch, me)))

    def small(n, src, dst, dev):
        return remote(src, dst, small_send.at[n], small_recv.at[n], dev)

    key_copies = []
    for q, dev in enumerate((mate, peer, diag)):
        key_copies.append(small(2 * q, keys_ref, all_keys.at[q + 1], dev))
        key_copies.append(small(2 * q + 1, segs_ref, all_segs.at[q + 1], dev))
    for copy in key_copies:
        copy.start()

    raw = remote(x_ref.at[:, cols(0)], land_raw.at[0], raw_send.at[0], raw_recv.at[0], peer)
    raw_fwd = remote(land_raw.at[0], land_raw.at[1], raw_send.at[1], raw_recv.at[1], mate)
    raw.start()

    def near(c):
        return remote(x_ref.at[:, cols(c)], land_mate.at[:, cols(c)], mate_send.at[c],
                      mate_recv.at[c], mate)

    loop(chunks, lambda c: near(c).start(), 1)
    near(0).start()
    all_keys[0] = keys_ref[...]
    all_segs[0] = segs_ref[...]
    for copy in key_copies:
        copy.wait()

    sub, lane = sort_index()
    key_list = [all_keys[v // 2, pl.ds(v % 2 * 8, 8), :] for v in range(8)]
    seg_list = [all_segs[v // 2, pl.ds(v % 2 * 8, 8), :] for v in range(8)]
    place = [(lane * 64 + sub * 8 + v).astype(f32) for v in range(8)]
    key_list, place_list, seg_list = bitonic([key_list, place, seg_list])

    zero, one = jnp.zeros((8, LANES), f32), jnp.ones((8, LANES), f32)
    both = jnp.logical_and

    def flag(c):
        return jnp.where(c, one, zero)

    first_seg = shifted(seg_list, 1, -1)
    before_key = shifted(key_list, 1, -inf)
    starts = [flag(x != y) for x, y in zip(seg_list, first_seg)]
    low_list = running([jnp.where(x > 0, k, -inf) for x, k in zip(starts, before_key)],
                       jnp.maximum, -inf)
    mine = [flag(p - 8.0 * jnp.floor(p * 0.125) < 4.0) for p in place_list]
    mine_before, mine_after = shifted(mine, 1, 0.0), shifted(mine, -1, 0.0)
    starts_after = shifted(starts, -1, 1.0)
    leader = [flag(both(both(m > 0, x == 0), y == 0))
              for m, x, y in zip(mine, mine_after, starts_after)]
    goes_on = [both(x > 0, y == 0) for x, y in zip(mine_after, starts_after)]
    begins = [jnp.logical_or(x == 0, y > 0) for x, y in zip(mine_before, starts)]
    weight = [jnp.where(x > 0, jnp.where(y, 1.0, 4096.0), 0.0) for x, y in zip(leader, begins)]
    counted = [x - y for x, y in zip(running(weight, jnp.add, 0.0), weight)]
    stop = [jnp.where(x > 0, 2.0 * p, jnp.where(both(m > 0, jnp.logical_not(g)), 2.0 * p + 1.0, 32768.0))
            for x, p, m, g in zip(leader, place, mine, goes_on)]
    stop = running(stop, jnp.minimum, 32768.0, back=True)
    needed = [both(m > 0, x - 2.0 * jnp.floor(x * 0.5) == 0.0) for m, x in zip(mine, stop)]

    def total(values):
        v = values[0]
        for x in values[1:]:
            v = v + x
        return jnp.sum(jnp.sum(v, axis=0, keepdims=True), axis=1, keepdims=True)

    n_single = total([flag(w == 1.0) for w in weight])
    n_longer = total([flag(w == 4096.0) for w in weight])
    spill = n_longer + jnp.maximum(n_single - 2.0 * ones, 0.0)
    flags[0] = jnp.broadcast_to(jnp.where(spill > 2.0 * sums, 1.0, 0.0), (8, LANES))

    float32_slots = float(rows)
    slot_list = []
    for w, c, m in zip(weight, counted, needed):
        before_longer = jnp.floor(c * (1.0 / 4096.0))
        before_single = c - 4096.0 * before_longer
        over = float32_slots + n_longer + before_single - 2.0 * ones
        slot = jnp.where(before_single < 2.0 * ones, before_single, over)
        slot = jnp.where(w == 1.0, slot, float32_slots + before_longer)
        slot_list.append(jnp.where(m, slot, -1.0))
    _, low_list, slot_list = bitonic([place_list, low_list, slot_list])
    for v in range(2):
        lows[pl.ds(v * 8, 8), :] = low_list[v]
    for v in range(4):
        slots[v // 2, pl.ds(v % 2 * 8, 8), :] = slot_list[v]
    flag_copy = small(6, flags.at[0], flags.at[1], peer)
    flag_copy.start()

    def near_loads(c, buf, sem):
        return (local(x_ref.at[:, cols(c)], buf.at[pl.ds(0, rows), :], sem.at[0]),
                local(land_mate.at[:, cols(c)], buf.at[pl.ds(rows, rows), :], sem.at[1]))

    def start_near(c, buf, sem):
        for copy in near_loads(c, buf, sem):
            copy.start()

    def wait_near(c, buf, sem):
        for copy in near_loads(c, buf, sem):
            copy.wait()

    near(1).wait_recv()
    start_near(1, near_buf, near_sem)

    size, unroll = 64, 4
    col_slot[...] = jnp.full(col_slot.shape, -inf, f32)

    def pick_block(b):
        base = jnp.where(b < ones // size, core * ones, rows + core * sums - ones) + b * size
        want = (lax.broadcasted_iota(jnp.int32, (size, LANES), 0) + base).astype(f32)

        def step(t, top):
            for q in range(2):
                for u in range(unroll):
                    row = t * unroll + u
                    hit = slots[q, pl.ds(row, 1), :] == want
                    pick_ref[block(b, size), block(q * key_rows + row, LANES)] = jnp.where(
                        hit, 1.0, 0.0).astype(bf16)
                    top = jnp.maximum(top, jnp.where(hit, all_keys[q, pl.ds(row, 1), :], -inf))
            return top

        top = lax.fori_loop(0, key_rows // unroll, step, jnp.full((size, LANES), -inf, f32))
        col_slot[block(b, size), :] = jnp.broadcast_to(jnp.max(top, axis=1, keepdims=True),
                                                       (size, LANES))

    loop(pick_ref.shape[0] // size, pick_block)

    for t in range(col_slot.shape[0] // LANES):
        slot_keys[0, pl.ds(t, 1), :] = col_slot[pl.ds(t * LANES, LANES), :].T[0:1, :]
    slot_key_copies = (small(7, slot_keys.at[0], slot_keys.at[1], peer),
                       small(8, slot_keys.at[0], slot_keys.at[2], diag))
    for copy in slot_key_copies:
        copy.start()

    parts = ((0, ones), (0, main // 2), (main // 2, main // 2), (main, tail))

    def run(e, kind):
        at = pl.ds(*parts[kind])
        buf, land = (sum_buf, land_sum) if kind else (one_buf, land_one)
        return remote(buf.at[lax.rem(e, 2), at, :], land.at[0, at, cols(e)], run_send.at[kind, e],
                      run_recv.at[kind, e], peer)

    def fwd(e, kind):
        at = pl.ds(*parts[kind])
        land = land_sum if kind else land_one
        return remote(land.at[0, at, cols(e)], land.at[1, at, cols(e)], fwd_send.at[kind, e],
                      fwd_recv.at[kind, e], mate)

    kinds = range(len(parts))

    def reduce_runs(e):
        wait_near(e + 1, near_buf, near_sem)
        slot = lax.rem(e, 2)
        one_buf[slot] = jnp.dot(pick_ref[pl.ds(0, ones), :], near_buf[...],
                                preferred_element_type=f32).astype(bf16)
        sum_buf[slot] = jnp.dot(pick_ref[pl.ds(ones, sums), :], near_buf[...],
                                preferred_element_type=f32)
        for kind in kinds:
            run(e, kind).start()

    def next_near(e):
        near(e + 1).wait_recv()
        start_near(e + 1, near_buf, near_sem)

    def reduce_first(e):
        reduce_runs(e)
        next_near(e + 1)

    loop(2, reduce_first)

    near(0).wait_recv()
    start_near(0, rows_buf, load_sem)

    def forward_raw():
        raw.wait_recv()
        raw_fwd.start()

    places = [(mask_ref, 0), (mask_ref, rows), (mask_ref, 2 * rows), (out_ref, 0)]
    row_masks(keys_ref, lows, all_keys, places, forward_raw)

    def tiles_loop(body):
        loop(rows // tile, lambda i: body(block(i, tile)))

    def dot(at, start, n, buf, offset):
        return jnp.dot(mask_ref[at, pl.ds(start, n)], buf[pl.ds(offset, n), :],
                       preferred_element_type=f32)

    def raw_load(s):
        return local(land_raw.at[s], rows_buf.at[pl.ds((2 + s) * rows, rows), :], load_sem.at[2 + s])

    raw_load(0).start()
    raw_fwd.wait_recv()
    raw_load(1).start()
    wait_near(0, rows_buf, load_sem)
    raw_load(0).wait()
    raw_load(1).wait()

    def whole(at):
        acc = dot(at, 0, 3 * rows, rows_buf, 0)
        acc += jnp.dot(out_ref[at, :], rows_buf[pl.ds(3 * rows, rows), :], preferred_element_type=f32)
        out_ref[at, cols(0)] = acc.astype(bf16)

    tiles_loop(whole)
    start_near(1, rows_buf, load_sem)

    for copy in slot_key_copies:
        copy.wait()

    def slot_mask(b):
        own_k, low = expand(keys_ref, b), expand(lows, b)
        for s in range(2):
            for t in range((ones + main) // LANES):
                column = t * LANES + s * ones + (ones_at if t < ones // LANES else sums_at - ones)
                write_mask(mask_ref, block(b, LANES), own_k, low, slot_keys[1 + s, pl.ds(t, 1), :],
                           column)
        t = (ones + main) // LANES
        ends = [slot_keys[1 + s, pl.ds(t, 1), :] for s in range(2)]
        end_lane = lax.broadcasted_iota(jnp.int32, ends[0].shape, 1)
        ends = jnp.where(end_lane < tail, ends[0],
                         pltpu.roll(jnp.broadcast_to(ends[1], (8, LANES)), tail, 1)[0:1, :])
        ends = jnp.where(end_lane < 2 * tail, ends, -inf)
        write_mask(mask_ref, block(b, LANES), own_k, low, ends, tail_at)

    loop(key_rows, slot_mask)
    pad = LANES - 2 * tail
    for buf, end in ((rows_buf, tail_at + LANES), (mid_buf, run_cols), (low_buf, run_cols)):
        buf[pl.ds(end - pad, pad), :] = jnp.zeros((pad, COL_W), bf16)

    size = tail

    def split(kind, s):
        lo, n = parts[kind]
        offset = (2 * main + s * tail - lo) if lo == main else s * main

        def step(i):
            at = lo + i * size
            v = sum_in[s, block(lo // size + i, size), :]
            high = jnp.clip(v, -BF16_MAX, BF16_MAX).astype(bf16)
            rest = v - high.astype(f32)
            mid = rest.astype(bf16)
            to = pl.multiple_of(at + offset, size)
            rows_buf[pl.ds(sums_at + to, size), :] = high
            mid_buf[pl.ds(to, size), :] = mid
            low_buf[pl.ds(to, size), :] = (rest - mid.astype(f32)).astype(bf16)

        loop(n // size, step)

    def run_load(e, kind, s):
        at = pl.ds(*parts[kind])
        if kind:
            src, dst = land_sum.at[s, at, cols(e)], sum_in.at[s, at, :]
        else:
            src, dst = land_one.at[s, :, cols(e)], rows_buf.at[pl.ds(ones_at + s * ones, ones), :]
        return local(src, dst, load_sem.at[2 + 2 * kind + s])

    def receive(e, kind):
        run(e, kind).wait_recv()
        fwd(e, kind).start()
        run_load(e, kind, 0).start()

    def arrive(e, kind):
        fwd(e, kind).wait_recv()
        run_load(e, kind, 1).start()

    def take(e, kind):
        for s in range(2):
            run_load(e, kind, s).wait()
            if kind:
                split(kind, s)

    def arrived(e):
        for kind in kinds:
            arrive(e, kind)
        wait_near(e + 1, rows_buf, load_sem)
        for kind in kinds:
            take(e, kind)

    def add_tile(e):
        def whole_runs(i):
            at = block(i, tile)
            acc = dot(at, 0, tail_at + LANES, rows_buf, 0)
            acc += dot(at, sums_at, run_cols, mid_buf, 0)
            acc += dot(at, sums_at, run_cols, low_buf, 0)
            out_ref[at, cols(e + 1)] = acc.astype(bf16)

        return whole_runs

    flag_copy.wait()
    flags[2] = jnp.maximum(flags[0], flags[1])
    flag_all = small(9, flags.at[2], flags.at[3], (1 - batch, me))
    flag_all.start()

    last = run_chunks - 1

    def near_rows(at):
        acc_buf[at, :] = dot(at, 0, 2 * rows, near_buf, 0)

    def steady(e):
        @pl.when(e == last - 1)
        def _():
            tiles_loop(near_rows)

        for kind in kinds:
            receive(e, kind)

        @pl.when(e < last - 1)
        def _():
            for kind in kinds:
                run(e, kind).wait_send()
            reduce_runs(e + 2)

        @pl.when(e < last - 2)
        def _():
            next_near(e + 3)

        arrived(e)
        add_chunk = add_tile(e)

        def step(i):
            add_chunk(i)

            @pl.when(jnp.logical_and(e == last - 1, i == 0))
            def _():
                run(last, 0).wait_recv()
                fwd(last, 0).start()

        loop(rows // tile, step)

        @pl.when(e < last - 1)
        def _():
            start_near(e + 2, rows_buf, load_sem)

    loop(last, steady)
    run_load(last, 0, 0).start()
    receive(last, 1)
    arrive(last, 0)
    take(last, 0)

    def add_sums(acc, at, lo, n):
        for s in range(2):
            place = s * main + lo
            acc += dot(at, sums_at + place, n, rows_buf, sums_at + place)
            acc += dot(at, sums_at + place, n, mid_buf, place)
            acc += dot(at, sums_at + place, n, low_buf, place)
        return acc

    def single_rows(at):
        acc_buf[at, :] += dot(at, ones_at, 2 * ones, rows_buf, ones_at)

    def first_runs(at):
        acc_buf[at, :] = add_sums(acc_buf[at, :], at, *parts[1])

    def second_runs(at):
        acc_buf[at, :] = add_sums(acc_buf[at, :], at, *parts[2])

    tiles_loop(single_rows)
    arrive(last, 1)
    take(last, 1)
    receive(last, 2)
    tiles_loop(first_runs)
    receive(last, 3)
    arrive(last, 2)
    take(last, 2)
    arrive(last, 3)
    tiles_loop(second_runs)
    take(last, 3)

    def last_runs(at):
        acc = acc_buf[at, :] + dot(at, tail_at, LANES, rows_buf, tail_at)
        acc += dot(at, tail_at, LANES, mid_buf, 2 * main)
        acc += dot(at, tail_at, LANES, low_buf, 2 * main)
        out_ref[at, cols(chunks - 1)] = acc.astype(bf16)

    tiles_loop(last_runs)
    flag_all.wait()
    flag_ref[...] = jnp.maximum(flags[2], flags[3])
    raw.wait_send()
    raw_fwd.wait_send()
    loop(chunks, lambda c: near(c).wait_send())
    for kind in kinds:
        loop(run_chunks, lambda e: fwd(e, kind).wait_send())
        loop(run_chunks, lambda e: run(e, kind).wait_send(), run_chunks - 2)


def rows_kernel(keys_ref, x_ref, lows, all_keys, out_ref, land_ref, mask_ref, rows_buf, out_buf,
                send_sem, recv_sem, load_sem):
    rows, width = x_ref.shape
    chunks = width // COL_W
    tile = COL_W
    batch, _, _, mate, peer, diag = neighbours()
    mate, peer, diag = (batch, mate), (batch, peer), (batch, diag)
    greet((mate, peer, diag))

    def copy(kind, c):
        if kind < 2:
            src, dst, dev = x_ref.at[:, cols(c)], land_ref.at[kind, :, cols(c)], (mate, peer)[kind]
        else:
            src, dst, dev = land_ref.at[1, :, cols(c)], land_ref.at[2, :, cols(c)], mate
        return remote(src, dst, send_sem.at[kind, c], recv_sem.at[kind, c], dev)

    loop(chunks, lambda c: copy(1, c).start())
    loop(chunks, lambda c: copy(0, c).start())
    row_masks(keys_ref, lows, all_keys, [(mask_ref, q * rows) for q in range(4)])

    def chunk(c):
        copy(1, c).wait_recv()
        copy(2, c).start()
        copy(0, c).wait_recv()
        copy(2, c).wait_recv()
        loads = [local(x_ref.at[:, cols(c)], rows_buf.at[pl.ds(0, rows), :], load_sem.at[0])]
        for q in range(3):
            loads.append(local(land_ref.at[q, :, cols(c)], rows_buf.at[pl.ds((q + 1) * rows, rows), :],
                               load_sem.at[q + 1]))
        for load in loads:
            load.start()
        for load in loads:
            load.wait()

        def whole(i):
            out_buf[block(i, tile), :] = jnp.dot(mask_ref[block(i, tile), :], rows_buf[...],
                                                 preferred_element_type=f32).astype(bf16)

        loop(rows // tile, whole)
        store = local(out_buf, out_ref.at[:, cols(c)], load_sem.at[0])
        store.start()
        store.wait()

    loop(chunks, chunk)
    for kind in range(3):
        loop(chunks, lambda c: copy(kind, c).wait_send())


def solution(mesh):
    dma = pltpu.SemaphoreType.DMA
    any_spec = pl.BlockSpec(memory_space=pl.ANY)
    vmem_spec = pl.BlockSpec(memory_space=pltpu.VMEM)
    shape, vmem = jax.ShapeDtypeStruct, pltpu.VMEM

    def raw_exchange(keys, payload, lows, all_keys):
        rows, width = payload.shape
        chunks = width // COL_W
        out, _ = pl.pallas_call(
            rows_kernel,
            out_shape=(shape((rows, width), bf16), shape((3, rows, width), bf16)),
            in_specs=[vmem_spec, any_spec, vmem_spec, vmem_spec],
            out_specs=(any_spec, any_spec),
            scratch_shapes=[
                vmem((rows, 4 * rows), bf16), vmem((4 * rows, COL_W), bf16), vmem((rows, COL_W), bf16),
                dma((3, chunks)), dma((3, chunks)), dma((4,)),
            ],
            compiler_params=pltpu.CompilerParams(collective_id=1, has_side_effects=True,
                                                 vmem_limit_bytes=VMEM_LIMIT),
        )(keys, payload, lows, all_keys)
        return out

    def run_exchange(keys, segs, payload):
        rows, width = payload.shape
        ones, sums = rows // 4, rows * 33 // 128
        chunks = width // COL_W
        run_w = width - COL_W
        slot_rows = 2 * ones + LANES
        sum_rows = 2 * ones + LANES
        key_shape = keys.shape
        small, kinds = 10, 4
        return pl.pallas_call(
            runs_kernel,
            out_shape=(vmem((rows, width), bf16), vmem((8, LANES), f32), vmem(key_shape, f32),
                       vmem((4,) + key_shape, f32), shape((rows, width), bf16),
                       shape((2, rows, COL_W), bf16), shape((2, ones, run_w), bf16),
                       shape((2, sums, run_w), f32)),
            in_specs=[vmem_spec, vmem_spec, any_spec],
            out_specs=(vmem_spec,) * 4 + (any_spec,) * 4,
            scratch_shapes=[
                vmem((4,) + key_shape, jnp.int32), vmem((2,) + key_shape, f32),
                vmem((3,) + key_shape, f32), vmem((slot_rows, LANES), f32), vmem((4, 8, LANES), f32),
                vmem((rows, 3 * rows + LANES), bf16), vmem((2 * ones + COL_W // 4, 2 * rows), bf16),
                vmem((4 * rows, COL_W), bf16), vmem((sum_rows, COL_W), bf16),
                vmem((sum_rows, COL_W), bf16), vmem((2 * rows, COL_W), bf16),
                vmem((2, ones, COL_W), bf16), vmem((2, sums, COL_W), f32),
                vmem((2, sums, COL_W), f32), vmem((rows, COL_W), f32),
                dma((small,)), dma((small,)), dma((2,)), dma((2,)), dma((chunks,)), dma((chunks,)),
                dma((kinds, chunks)), dma((kinds, chunks)), dma((kinds, chunks)), dma((kinds, chunks)),
                dma((small,)), dma((2,)),
            ],
            compiler_params=pltpu.CompilerParams(collective_id=0, has_side_effects=True,
                                                 vmem_limit_bytes=VMEM_LIMIT),
        )(keys, segs, payload)[:4]

    def per_device(sort_keys, seg_ids, payload):
        key_shape = (payload.shape[0] // LANES, LANES)
        keys = sort_keys.reshape(key_shape)
        out, full, lows, all_keys = run_exchange(keys, seg_ids.reshape(key_shape), payload)
        return lax.cond(full[0, 0] > 0.0, raw_exchange, lambda *_: out, keys, payload, lows, all_keys)

    row_spec = P(('batch', 'group'))
    mat_spec = P(('batch', 'group'), None)
    return jax.shard_map(per_device, mesh=mesh, in_specs=(row_spec, row_spec, mat_spec),
                         out_specs=mat_spec, check_vma=False)
```

```python
import jax
import jax.numpy as jnp
from jax import lax
from jax.experimental import pallas as pl
from jax.experimental.pallas import tpu as pltpu
from jax.sharding import PartitionSpec as P

MESH = pl.DeviceIdType.MESH
LANES = 128
COL_W = 256
LOG_N = 13
BF16_MAX = 3.3895314e38
VMEM_LIMIT = 58400000
f32, bf16 = jnp.float32, jnp.bfloat16


def expand(ref, b, q=None):
    row = ref[pl.ds(b, 1), :] if q is None else ref[q, pl.ds(b, 1), :]
    return jnp.broadcast_to(row, (LANES, LANES)).T


def sort_index():
    sub = lax.broadcasted_iota(jnp.int32, (8, LANES), 0)
    lane = lax.broadcasted_iota(jnp.int32, (8, LANES), 1)
    return sub, lane


def bitonic(arrays):
    sub, lane = sort_index()
    arrays = [list(a) for a in arrays]

    def bit(k, v):
        if k < 3:
            return bool(v >> k & 1)
        if k < 6:
            return (sub >> (k - 3) & 1) == 1
        return (lane >> (k - 6) & 1) == 1

    for size in range(1, LOG_N + 1):
        for j in reversed(range(size)):
            if j < 3:
                for v in range(8):
                    if v >> j & 1:
                        continue
                    w = v | 1 << j
                    swap = arrays[0][v] > arrays[0][w]
                    if size < LOG_N:
                        down = bit(size, v)
                        if isinstance(down, bool):
                            swap = arrays[0][v] < arrays[0][w] if down else swap
                        else:
                            swap = jnp.logical_xor(swap, down)
                    for a in arrays:
                        a[v], a[w] = jnp.where(swap, a[w], a[v]), jnp.where(swap, a[v], a[w])
                continue
            axis, d, n = (0, 1 << (j - 3), 8) if j < 6 else (1, 1 << (j - 6), LANES)
            upper = bit(j, 0)
            for v in range(8):
                other = [jnp.where(upper, pltpu.roll(a[v], d, axis), pltpu.roll(a[v], n - d, axis))
                         for a in arrays]
                keep_max = upper
                if size < LOG_N:
                    down = bit(size, v)
                    if isinstance(down, bool):
                        keep_max = jnp.logical_not(upper) if down else upper
                    else:
                        keep_max = jnp.logical_xor(upper, down)
                take = jnp.logical_xor(other[0] < arrays[0][v], keep_max)
                for a, o in zip(arrays, other):
                    a[v] = jnp.where(take, o, a[v])
    return arrays


def shifted(values, step, fill):
    sub, lane = sort_index()
    if step == 1:
        edge, first = pltpu.roll(values[7], 1, 0), sub == 0
        edge = jnp.where(first, pltpu.roll(edge, 1, 1), edge)
        edge = jnp.where(jnp.logical_and(first, lane == 0), fill, edge)
        return [edge] + values[:7]
    edge, last = pltpu.roll(values[0], 7, 0), sub == 7
    edge = jnp.where(last, pltpu.roll(edge, LANES - 1, 1), edge)
    edge = jnp.where(jnp.logical_and(last, lane == LANES - 1), fill, edge)
    return values[1:] + [edge]


def running(values, op, start, back=False):
    sub, lane = sort_index()
    seq = values[::-1] if back else values
    inc = [seq[0]]
    for x in seq[1:]:
        inc.append(op(inc[-1], x))

    def moved(x, d, axis):
        n = 8 if axis == 0 else LANES
        at = sub if axis == 0 else lane
        if back:
            return jnp.where(at < n - d, pltpu.roll(x, n - d, axis), start)
        return jnp.where(at >= d, pltpu.roll(x, d, axis), start)

    t = inc[-1]
    for d in (1, 2, 4):
        t = op(t, moved(t, d, 0))
    row = t[0:1, :] if back else t[7:8, :]
    u = jnp.broadcast_to(row, (8, LANES))
    for d in (1, 2, 4, 8, 16, 32, 64):
        u = op(u, moved(u, d, 1))
    base = op(moved(u, 1, 1), moved(t, 1, 0))
    out = [op(base, x) for x in inc]
    return out[::-1] if back else out


def cols(c):
    return pl.ds(pl.multiple_of(c * COL_W, COL_W), COL_W)


def block(i, size):
    return pl.ds(pl.multiple_of(i * size, size), size)


def loop(n, body, first=0):
    def step(i, carry):
        body(i)
        return carry
    lax.fori_loop(first, n, step, 0)


def write_mask(mask_ref, at, own_k, low, k, column):
    inside = jnp.logical_and(k <= own_k, k > low)
    to = pl.ds(pl.multiple_of(column, LANES), LANES)
    mask_ref[at, to] = jnp.where(inside, 1.0, 0.0).astype(bf16)


def row_masks(keys_ref, lows, all_keys, places, between=None):
    key_rows = keys_ref.shape[0]
    unroll = 4

    def mask_block(b):
        own_k, low = expand(keys_ref, b), expand(lows, b)

        def fill(t):
            for q, (ref, first) in enumerate(places):
                for u in range(unroll):
                    row = t * unroll + u
                    write_mask(ref, block(b, LANES), own_k, low, all_keys[q, pl.ds(row, 1), :],
                               row * LANES + first)

        loop(key_rows // unroll, fill)

    if between is None:
        loop(key_rows, mask_block)
    else:
        loop(key_rows // 2, mask_block)
        between()
        loop(key_rows, mask_block, key_rows // 2)


def neighbours():
    batch, me = lax.axis_index('batch'), lax.axis_index('group')
    core = lax.rem(me, 2)
    return batch, me, core, me + 1 - 2 * core, lax.rem(me + 2, 4), 3 - me


def greet(devices):
    barrier = pltpu.get_barrier_semaphore()
    for dev in devices:
        pl.semaphore_signal(barrier, inc=1, device_id=dev, device_id_type=MESH)
    pl.semaphore_wait(barrier, len(devices))


def local(src, dst, sem):
    return pltpu.make_async_copy(src, dst, sem)


def remote(src, dst, ssem, rsem, dev):
    return pltpu.make_async_remote_copy(src, dst, ssem, rsem, device_id=dev, device_id_type=MESH)


def runs_kernel(keys_ref, segs_ref, x_ref, out_ref, flag_ref, lows, all_keys, land_mate, land_raw,
                land_one, land_sum, all_segs, slots, slot_keys, col_slot, flags, mask_ref, pick_ref,
                rows_buf, mid_buf, low_buf, near_buf, last_buf, one_buf, sum_buf, sum_in, acc_buf, small_send,
                small_recv, raw_send, raw_recv, mate_send, mate_recv, run_send, run_recv, fwd_send,
                fwd_recv, load_sem, near_sem, last_sem):
    rows, width = x_ref.shape
    key_rows = rows // LANES
    chunks = width // COL_W
    run_chunks = chunks - 1
    ones, sums = land_one.shape[1], land_sum.shape[1]
    main = ones
    tail = sums - main
    ones_at = 2 * rows
    sums_at = ones_at + 2 * ones
    end_tile = 4
    tile_of = ((0, 1, 5, 7), (2, 3, 6, 8))
    tail_at = sums_at + end_tile * LANES
    run_cols = 2 * main + LANES
    tile = 1024
    inf = jnp.inf
    batch, me, core, mate, peer, diag = neighbours()
    mate, peer, diag = (batch, mate), (batch, peer), (batch, diag)
    greet((mate, peer, diag, (1 - batch, me)))

    def small(n, src, dst, dev):
        return remote(src, dst, small_send.at[n], small_recv.at[n], dev)

    key_copies = []
    for q, dev in enumerate((mate, peer, diag)):
        key_copies.append(small(2 * q, keys_ref, all_keys.at[q + 1], dev))
        key_copies.append(small(2 * q + 1, segs_ref, all_segs.at[q + 1], dev))
    for copy in key_copies:
        copy.start()

    raw = remote(x_ref.at[:, cols(0)], land_raw.at[0], raw_send.at[0], raw_recv.at[0], peer)
    raw_fwd = remote(land_raw.at[0], land_raw.at[1], raw_send.at[1], raw_recv.at[1], mate)
    raw.start()

    def near(c):
        return remote(x_ref.at[:, cols(c)], land_mate.at[:, cols(c)], mate_send.at[c],
                      mate_recv.at[c], mate)

    loop(chunks, lambda c: near(c).start(), 1)
    near(0).start()
    all_keys[0] = keys_ref[...]
    all_segs[0] = segs_ref[...]
    for copy in key_copies:
        copy.wait()

    sub, lane = sort_index()
    key_list = [all_keys[v // 2, pl.ds(v % 2 * 8, 8), :] for v in range(8)]
    seg_list = [all_segs[v // 2, pl.ds(v % 2 * 8, 8), :] for v in range(8)]
    place = [(lane * 64 + sub * 8 + v).astype(f32) for v in range(8)]
    key_list, place_list, seg_list = bitonic([key_list, place, seg_list])

    zero, one = jnp.zeros((8, LANES), f32), jnp.ones((8, LANES), f32)
    both = jnp.logical_and

    def flag(c):
        return jnp.where(c, one, zero)

    first_seg = shifted(seg_list, 1, -1)
    before_key = shifted(key_list, 1, -inf)
    starts = [flag(x != y) for x, y in zip(seg_list, first_seg)]
    low_list = running([jnp.where(x > 0, k, -inf) for x, k in zip(starts, before_key)],
                       jnp.maximum, -inf)
    mine = [flag(p - 8.0 * jnp.floor(p * 0.125) < 4.0) for p in place_list]
    mine_before, mine_after = shifted(mine, 1, 0.0), shifted(mine, -1, 0.0)
    starts_after = shifted(starts, -1, 1.0)
    leader = [flag(both(both(m > 0, x == 0), y == 0))
              for m, x, y in zip(mine, mine_after, starts_after)]
    goes_on = [both(x > 0, y == 0) for x, y in zip(mine_after, starts_after)]
    begins = [jnp.logical_or(x == 0, y > 0) for x, y in zip(mine_before, starts)]
    weight = [jnp.where(x > 0, jnp.where(y, 1.0, 4096.0), 0.0) for x, y in zip(leader, begins)]
    counted = [x - y for x, y in zip(running(weight, jnp.add, 0.0), weight)]
    stop = [jnp.where(x > 0, 2.0 * p, jnp.where(both(m > 0, jnp.logical_not(g)), 2.0 * p + 1.0, 32768.0))
            for x, p, m, g in zip(leader, place, mine, goes_on)]
    stop = running(stop, jnp.minimum, 32768.0, back=True)
    needed = [both(m > 0, x - 2.0 * jnp.floor(x * 0.5) == 0.0) for m, x in zip(mine, stop)]

    def total(values):
        v = values[0]
        for x in values[1:]:
            v = v + x
        return jnp.sum(jnp.sum(v, axis=0, keepdims=True), axis=1, keepdims=True)

    n_single = total([flag(w == 1.0) for w in weight])
    n_longer = total([flag(w == 4096.0) for w in weight])
    spill = n_longer + jnp.maximum(n_single - 2.0 * ones, 0.0)
    flags[0] = jnp.broadcast_to(jnp.where(spill > 2.0 * sums, 1.0, 0.0), (8, LANES))

    float32_slots = float(rows)
    slot_list = []
    for w, c, m in zip(weight, counted, needed):
        before_longer = jnp.floor(c * (1.0 / 4096.0))
        before_single = c - 4096.0 * before_longer
        over = float32_slots + n_longer + before_single - 2.0 * ones
        slot = jnp.where(before_single < 2.0 * ones, before_single, over)
        slot = jnp.where(w == 1.0, slot, float32_slots + before_longer)
        slot_list.append(jnp.where(m, slot, -1.0))
    _, low_list, slot_list = bitonic([place_list, low_list, slot_list])
    for v in range(2):
        lows[pl.ds(v * 8, 8), :] = low_list[v]
    for v in range(4):
        slots[v // 2, pl.ds(v % 2 * 8, 8), :] = slot_list[v]
    flag_copy = small(6, flags.at[0], flags.at[1], peer)
    flag_copy.start()

    def near_loads(c, buf, sem):
        return (local(x_ref.at[:, cols(c)], buf.at[pl.ds(0, rows), :], sem.at[0]),
                local(land_mate.at[:, cols(c)], buf.at[pl.ds(rows, rows), :], sem.at[1]))

    def start_near(c, buf, sem):
        for copy in near_loads(c, buf, sem):
            copy.start()

    def wait_near(c, buf, sem):
        for copy in near_loads(c, buf, sem):
            copy.wait()

    near(1).wait_recv()
    start_near(1, near_buf, near_sem)

    size, unroll = 64, 4
    col_slot[...] = jnp.full(col_slot.shape, -inf, f32)

    def pick_block(b):
        base = jnp.where(b < ones // size, core * ones, rows + core * sums - ones) + b * size
        want = (lax.broadcasted_iota(jnp.int32, (size, LANES), 0) + base).astype(f32)

        def step(t, top):
            for q in range(2):
                for u in range(unroll):
                    row = t * unroll + u
                    hit = slots[q, pl.ds(row, 1), :] == want
                    pick_ref[block(b, size), block(q * key_rows + row, LANES)] = jnp.where(
                        hit, 1.0, 0.0).astype(bf16)
                    top = jnp.maximum(top, jnp.where(hit, all_keys[q, pl.ds(row, 1), :], -inf))
            return top

        top = lax.fori_loop(0, key_rows // unroll, step, jnp.full((size, LANES), -inf, f32))
        col_slot[block(b, size), :] = jnp.broadcast_to(jnp.max(top, axis=1, keepdims=True),
                                                       (size, LANES))

    loop(pick_ref.shape[0] // size, pick_block)

    for t in range(col_slot.shape[0] // LANES):
        slot_keys[0, pl.ds(t, 1), :] = col_slot[pl.ds(t * LANES, LANES), :].T[0:1, :]
    slot_key_copies = (small(7, slot_keys.at[0], slot_keys.at[1], peer),
                       small(8, slot_keys.at[0], slot_keys.at[2], diag))
    for copy in slot_key_copies:
        copy.start()

    parts = ((0, ones), (main, tail), (0, 2 * LANES), (2 * LANES, LANES), (3 * LANES, LANES))

    def run(e, kind):
        at = pl.ds(*parts[kind])
        buf, land = (sum_buf, land_sum) if kind else (one_buf, land_one)
        return remote(buf.at[lax.rem(e, 2), at, :], land.at[0, at, cols(e)], run_send.at[kind, e],
                      run_recv.at[kind, e], peer)

    def fwd(e, kind):
        at = pl.ds(*parts[kind])
        land = land_sum if kind else land_one
        return remote(land.at[0, at, cols(e)], land.at[1, at, cols(e)], fwd_send.at[kind, e],
                      fwd_recv.at[kind, e], mate)

    kinds = range(len(parts))

    def reduce_runs(e):
        wait_near(e + 1, near_buf, near_sem)
        slot = lax.rem(e, 2)
        one_buf[slot] = jnp.dot(pick_ref[pl.ds(0, ones), :], near_buf[...],
                                preferred_element_type=f32).astype(bf16)
        sum_buf[slot] = jnp.dot(pick_ref[pl.ds(ones, sums), :], near_buf[...],
                                preferred_element_type=f32)
        for kind in kinds:
            run(e, kind).start()

    def next_near(e):
        @pl.when(e < run_chunks - 1)
        def _():
            near(e + 1).wait_recv()

        start_near(e + 1, near_buf, near_sem)

    def reduce_first(e):
        reduce_runs(e)
        next_near(e + 1)

    loop(2, reduce_first)

    near(0).wait_recv()
    start_near(0, rows_buf, load_sem)

    def forward_raw():
        raw.wait_recv()
        raw_fwd.start()

    places = [(mask_ref, 0), (mask_ref, rows), (mask_ref, 2 * rows), (out_ref, 0)]
    row_masks(keys_ref, lows, all_keys, places, forward_raw)

    def tiles_loop(body):
        loop(rows // tile, lambda i: body(block(i, tile)))

    def dot(at, start, n, buf, offset):
        return jnp.dot(mask_ref[at, pl.ds(start, n)], buf[pl.ds(offset, n), :],
                       preferred_element_type=f32)

    def raw_load(s):
        return local(land_raw.at[s], rows_buf.at[pl.ds((2 + s) * rows, rows), :], load_sem.at[2 + s])

    raw_load(0).start()
    raw_fwd.wait_recv()
    raw_load(1).start()
    wait_near(0, rows_buf, load_sem)
    raw_load(0).wait()
    raw_load(1).wait()

    def whole(at):
        acc = dot(at, 0, 3 * rows, rows_buf, 0)
        acc += jnp.dot(out_ref[at, :], rows_buf[pl.ds(3 * rows, rows), :], preferred_element_type=f32)
        out_ref[at, cols(0)] = acc.astype(bf16)

    tiles_loop(whole)
    start_near(1, rows_buf, load_sem)

    for copy in slot_key_copies:
        copy.wait()

    def slot_mask(b):
        own_k, low = expand(keys_ref, b), expand(lows, b)
        for s in range(2):
            for t in range((ones + main) // LANES):
                if t < ones // LANES:
                    column = ones_at + s * ones + t * LANES
                else:
                    column = sums_at + tile_of[s][t - ones // LANES] * LANES
                write_mask(mask_ref, block(b, LANES), own_k, low, slot_keys[1 + s, pl.ds(t, 1), :],
                           column)
        t = (ones + main) // LANES
        ends = [slot_keys[1 + s, pl.ds(t, 1), :] for s in range(2)]
        end_lane = lax.broadcasted_iota(jnp.int32, ends[0].shape, 1)
        ends = jnp.where(end_lane < tail, ends[0],
                         pltpu.roll(jnp.broadcast_to(ends[1], (8, LANES)), tail, 1)[0:1, :])
        ends = jnp.where(end_lane < 2 * tail, ends, -inf)
        write_mask(mask_ref, block(b, LANES), own_k, low, ends, tail_at)

    loop(key_rows, slot_mask)
    pad = LANES - 2 * tail
    for buf, end in ((rows_buf, tail_at), (mid_buf, tail_at - sums_at), (low_buf, tail_at - sums_at)):
        buf[pl.ds(end + 2 * tail, pad), :] = jnp.zeros((pad, COL_W), bf16)

    size = tail

    def split(kind, s):
        lo, n = parts[kind]
        if lo == main:
            offset = end_tile * LANES + s * tail - lo
        else:
            offset = tile_of[s][lo // LANES] * LANES - lo

        def step(i):
            at = lo + i * size
            v = sum_in[s, block(lo // size + i, size), :]
            high = jnp.clip(v, -BF16_MAX, BF16_MAX).astype(bf16)
            rest = v - high.astype(f32)
            mid = rest.astype(bf16)
            to = pl.multiple_of(at + offset, size)
            rows_buf[pl.ds(sums_at + to, size), :] = high
            mid_buf[pl.ds(to, size), :] = mid
            low_buf[pl.ds(to, size), :] = (rest - mid.astype(f32)).astype(bf16)

        loop(n // size, step)

    def run_load(e, kind, s):
        at = pl.ds(*parts[kind])
        if kind:
            src, dst = land_sum.at[s, at, cols(e)], sum_in.at[s, at, :]
        else:
            src, dst = land_one.at[s, :, cols(e)], rows_buf.at[pl.ds(ones_at + s * ones, ones), :]
        return local(src, dst, load_sem.at[2 + 2 * kind + s])

    def receive(e, kind):
        run(e, kind).wait_recv()
        fwd(e, kind).start()
        run_load(e, kind, 0).start()

    def arrive(e, kind):
        fwd(e, kind).wait_recv()
        run_load(e, kind, 1).start()

    def take(e, kind):
        for s in range(2):
            run_load(e, kind, s).wait()
            if kind:
                split(kind, s)

    def arrived(e):
        for kind in kinds:
            arrive(e, kind)
        wait_near(e + 1, rows_buf, load_sem)
        for kind in kinds:
            take(e, kind)

    def add_tile(e):
        def whole_runs(i):
            at = block(i, tile)
            acc = dot(at, 0, sums_at + run_cols, rows_buf, 0)
            acc += dot(at, sums_at, run_cols, mid_buf, 0)
            acc += dot(at, sums_at, run_cols, low_buf, 0)
            out_ref[at, cols(e + 1)] = acc.astype(bf16)

        return whole_runs

    flag_copy.wait()
    flags[2] = jnp.maximum(flags[0], flags[1])
    flag_all = small(9, flags.at[2], flags.at[3], (1 - batch, me))
    flag_all.start()

    last = run_chunks - 1

    def near_rows(at):
        acc_buf[at, :] = dot(at, 0, 2 * rows, last_buf, 0)

    def last_ones(s):
        return local(land_one.at[s, :, cols(last)], near_buf.at[pl.ds(s * ones, ones), :],
                     last_sem.at[2 + s])

    near(chunks - 1).wait_recv()
    start_near(chunks - 1, last_buf, last_sem)

    def steady(e):
        @pl.when(e == last - 3)
        def _():
            wait_near(chunks - 1, last_buf, last_sem)

        @pl.when(jnp.logical_and(e >= last - 3, e < last - 1))
        def _():
            near_rows(block(e - last + 3, tile))

        for kind in kinds:
            receive(e, kind)

        @pl.when(e < last - 1)
        def _():
            for kind in kinds:
                run(e, kind).wait_send()
            reduce_runs(e + 2)

        @pl.when(e < last - 2)
        def _():
            next_near(e + 3)

        arrived(e)
        add_chunk = add_tile(e)

        def step(i):
            add_chunk(i)

            @pl.when(jnp.logical_and(e == last - 1, i == 0))
            def _():
                for kind in range(2):
                    run(last, kind).wait_recv()
                    fwd(last, kind).start()
                last_ones(0).start()

        loop(rows // tile, step)

        @pl.when(e < last - 1)
        def _():
            start_near(e + 2, rows_buf, load_sem)

    loop(last, steady)
    receive(last, 2)
    fwd(last, 0).wait_recv()
    last_ones(1).start()
    run_load(last, 1, 0).start()
    arrive(last, 1)
    last_ones(0).wait()
    last_ones(1).wait()

    def add_sums(acc, at, first, n):
        for buf, offset in ((rows_buf, sums_at), (mid_buf, 0), (low_buf, 0)):
            acc += dot(at, sums_at + first * LANES, n * LANES, buf, offset + first * LANES)
        return acc

    def single_rows(at):
        acc_buf[at, :] += dot(at, ones_at, 2 * ones, near_buf, 0)

    def first_runs(at):
        acc_buf[at, :] = add_sums(acc_buf[at, :], at, 0, end_tile + 1)

    def second_runs(at):
        acc_buf[at, :] = add_sums(acc_buf[at, :], at, tile_of[0][2], 2)

    def last_runs(at):
        out_ref[at, cols(chunks - 1)] = add_sums(acc_buf[at, :], at, tile_of[0][3], 2).astype(bf16)

    tiles_loop(single_rows)
    take(last, 1)
    arrive(last, 2)
    take(last, 2)
    receive(last, 3)
    tiles_loop(first_runs)
    arrive(last, 3)
    take(last, 3)
    receive(last, 4)
    tiles_loop(second_runs)
    arrive(last, 4)
    take(last, 4)
    tiles_loop(last_runs)
    flag_all.wait()
    flag_ref[...] = jnp.maximum(flags[2], flags[3])
    raw.wait_send()
    raw_fwd.wait_send()
    loop(chunks, lambda c: near(c).wait_send())
    for kind in kinds:
        loop(run_chunks, lambda e: fwd(e, kind).wait_send())
        loop(run_chunks, lambda e: run(e, kind).wait_send(), run_chunks - 2)


def rows_kernel(keys_ref, x_ref, lows, all_keys, out_ref, land_ref, mask_ref, rows_buf, out_buf,
                send_sem, recv_sem, load_sem):
    rows, width = x_ref.shape
    chunks = width // COL_W
    tile = COL_W
    batch, _, _, mate, peer, diag = neighbours()
    mate, peer, diag = (batch, mate), (batch, peer), (batch, diag)
    greet((mate, peer, diag))

    def copy(kind, c):
        if kind < 2:
            src, dst, dev = x_ref.at[:, cols(c)], land_ref.at[kind, :, cols(c)], (mate, peer)[kind]
        else:
            src, dst, dev = land_ref.at[1, :, cols(c)], land_ref.at[2, :, cols(c)], mate
        return remote(src, dst, send_sem.at[kind, c], recv_sem.at[kind, c], dev)

    loop(chunks, lambda c: copy(1, c).start())
    loop(chunks, lambda c: copy(0, c).start())
    row_masks(keys_ref, lows, all_keys, [(mask_ref, q * rows) for q in range(4)])

    def chunk(c):
        copy(1, c).wait_recv()
        copy(2, c).start()
        copy(0, c).wait_recv()
        copy(2, c).wait_recv()
        loads = [local(x_ref.at[:, cols(c)], rows_buf.at[pl.ds(0, rows), :], load_sem.at[0])]
        for q in range(3):
            loads.append(local(land_ref.at[q, :, cols(c)], rows_buf.at[pl.ds((q + 1) * rows, rows), :],
                               load_sem.at[q + 1]))
        for load in loads:
            load.start()
        for load in loads:
            load.wait()

        def whole(i):
            out_buf[block(i, tile), :] = jnp.dot(mask_ref[block(i, tile), :], rows_buf[...],
                                                 preferred_element_type=f32).astype(bf16)

        loop(rows // tile, whole)
        store = local(out_buf, out_ref.at[:, cols(c)], load_sem.at[0])
        store.start()
        store.wait()

    loop(chunks, chunk)
    for kind in range(3):
        loop(chunks, lambda c: copy(kind, c).wait_send())


def solution(mesh):
    dma = pltpu.SemaphoreType.DMA
    any_spec = pl.BlockSpec(memory_space=pl.ANY)
    vmem_spec = pl.BlockSpec(memory_space=pltpu.VMEM)
    shape, vmem = jax.ShapeDtypeStruct, pltpu.VMEM

    def raw_exchange(keys, payload, lows, all_keys):
        rows, width = payload.shape
        chunks = width // COL_W
        out, _ = pl.pallas_call(
            rows_kernel,
            out_shape=(shape((rows, width), bf16), shape((3, rows, width), bf16)),
            in_specs=[vmem_spec, any_spec, vmem_spec, vmem_spec],
            out_specs=(any_spec, any_spec),
            scratch_shapes=[
                vmem((rows, 4 * rows), bf16), vmem((4 * rows, COL_W), bf16), vmem((rows, COL_W), bf16),
                dma((3, chunks)), dma((3, chunks)), dma((4,)),
            ],
            compiler_params=pltpu.CompilerParams(collective_id=1, has_side_effects=True,
                                                 vmem_limit_bytes=VMEM_LIMIT),
        )(keys, payload, lows, all_keys)
        return out

    def run_exchange(keys, segs, payload):
        rows, width = payload.shape
        ones, sums = rows // 4, rows * 33 // 128
        chunks = width // COL_W
        run_w = width - COL_W
        slot_rows = 2 * ones + LANES
        sum_rows = 2 * ones + LANES
        key_shape = keys.shape
        small, kinds = 12, 5
        return pl.pallas_call(
            runs_kernel,
            out_shape=(vmem((rows, width), bf16), vmem((8, LANES), f32), vmem(key_shape, f32),
                       vmem((4,) + key_shape, f32), shape((rows, width), bf16),
                       shape((2, rows, COL_W), bf16), shape((2, ones, run_w), bf16),
                       shape((2, sums, run_w), f32)),
            in_specs=[vmem_spec, vmem_spec, any_spec],
            out_specs=(vmem_spec,) * 4 + (any_spec,) * 4,
            scratch_shapes=[
                vmem((4,) + key_shape, jnp.int32), vmem((2,) + key_shape, f32),
                vmem((3,) + key_shape, f32), vmem((slot_rows, LANES), f32), vmem((4, 8, LANES), f32),
                vmem((rows, 3 * rows + LANES), bf16), vmem((2 * ones + COL_W // 4, 2 * rows), bf16),
                vmem((4 * rows, COL_W), bf16), vmem((sum_rows, COL_W), bf16),
                vmem((sum_rows, COL_W), bf16), vmem((2 * rows, COL_W), bf16), vmem((2 * rows, COL_W), bf16),
                vmem((2, ones, COL_W), bf16), vmem((2, sums, COL_W), f32),
                vmem((2, sums, COL_W), f32), vmem((rows, COL_W), f32),
                dma((small,)), dma((small,)), dma((2,)), dma((2,)), dma((chunks,)), dma((chunks,)),
                dma((kinds, chunks)), dma((kinds, chunks)), dma((kinds, chunks)), dma((kinds, chunks)),
                dma((small,)), dma((2,)), dma((4,)),
            ],
            compiler_params=pltpu.CompilerParams(collective_id=0, has_side_effects=True,
                                                 vmem_limit_bytes=VMEM_LIMIT),
        )(keys, segs, payload)[:4]

    def per_device(sort_keys, seg_ids, payload):
        key_shape = (payload.shape[0] // LANES, LANES)
        keys = sort_keys.reshape(key_shape)
        out, full, lows, all_keys = run_exchange(keys, seg_ids.reshape(key_shape), payload)
        return lax.cond(full[0, 0] > 0.0, raw_exchange, lambda *_: out, keys, payload, lows, all_keys)

    row_spec = P(('batch', 'group'))
    mat_spec = P(('batch', 'group'), None)
    return jax.shard_map(per_device, mesh=mesh, in_specs=(row_spec, row_spec, mat_spec),
                         out_specs=mat_spec, check_vma=False)
```

```python
import jax
import jax.numpy as jnp
from jax import lax
from jax.experimental import pallas as pl
from jax.experimental.pallas import tpu as pltpu
from jax.sharding import PartitionSpec as P

MESH = pl.DeviceIdType.MESH
LANES = 128
COL_W = 256
LOG_N = 13
BF16_MAX = 3.3895314e38
VMEM_LIMIT = 53200000
ROWS_LIMIT = 54500000
f32, bf16 = jnp.float32, jnp.bfloat16


def expand(ref, b, q=None):
    row = ref[pl.ds(b, 1), :] if q is None else ref[q, pl.ds(b, 1), :]
    return jnp.broadcast_to(row, (LANES, LANES)).T


def sort_index():
    sub = lax.broadcasted_iota(jnp.int32, (8, LANES), 0)
    lane = lax.broadcasted_iota(jnp.int32, (8, LANES), 1)
    return sub, lane


def bitonic(arrays):
    sub, lane = sort_index()
    arrays = [list(a) for a in arrays]

    def bit(k, v):
        if k < 3:
            return bool(v >> k & 1)
        if k < 6:
            return (sub >> (k - 3) & 1) == 1
        return (lane >> (k - 6) & 1) == 1

    for size in range(1, LOG_N + 1):
        for j in reversed(range(size)):
            if j < 3:
                for v in range(8):
                    if v >> j & 1:
                        continue
                    w = v | 1 << j
                    swap = arrays[0][v] > arrays[0][w]
                    if size < LOG_N:
                        down = bit(size, v)
                        if isinstance(down, bool):
                            swap = arrays[0][v] < arrays[0][w] if down else swap
                        else:
                            swap = jnp.logical_xor(swap, down)
                    for a in arrays:
                        a[v], a[w] = jnp.where(swap, a[w], a[v]), jnp.where(swap, a[v], a[w])
                continue
            axis, d, n = (0, 1 << (j - 3), 8) if j < 6 else (1, 1 << (j - 6), LANES)
            upper = bit(j, 0)
            for v in range(8):
                other = [jnp.where(upper, pltpu.roll(a[v], d, axis), pltpu.roll(a[v], n - d, axis))
                         for a in arrays]
                keep_max = upper
                if size < LOG_N:
                    down = bit(size, v)
                    if isinstance(down, bool):
                        keep_max = jnp.logical_not(upper) if down else upper
                    else:
                        keep_max = jnp.logical_xor(upper, down)
                take = jnp.logical_xor(other[0] < arrays[0][v], keep_max)
                for a, o in zip(arrays, other):
                    a[v] = jnp.where(take, o, a[v])
    return arrays


def shifted(values, step, fill):
    sub, lane = sort_index()
    if step == 1:
        edge, first = pltpu.roll(values[7], 1, 0), sub == 0
        edge = jnp.where(first, pltpu.roll(edge, 1, 1), edge)
        edge = jnp.where(jnp.logical_and(first, lane == 0), fill, edge)
        return [edge] + values[:7]
    edge, last = pltpu.roll(values[0], 7, 0), sub == 7
    edge = jnp.where(last, pltpu.roll(edge, LANES - 1, 1), edge)
    edge = jnp.where(jnp.logical_and(last, lane == LANES - 1), fill, edge)
    return values[1:] + [edge]


def running(values, op, start, back=False):
    sub, lane = sort_index()
    seq = values[::-1] if back else values
    inc = [seq[0]]
    for x in seq[1:]:
        inc.append(op(inc[-1], x))

    def moved(x, d, axis):
        n = 8 if axis == 0 else LANES
        at = sub if axis == 0 else lane
        if back:
            return jnp.where(at < n - d, pltpu.roll(x, n - d, axis), start)
        return jnp.where(at >= d, pltpu.roll(x, d, axis), start)

    t = inc[-1]
    for d in (1, 2, 4):
        t = op(t, moved(t, d, 0))
    row = t[0:1, :] if back else t[7:8, :]
    u = jnp.broadcast_to(row, (8, LANES))
    for d in (1, 2, 4, 8, 16, 32, 64):
        u = op(u, moved(u, d, 1))
    base = op(moved(u, 1, 1), moved(t, 1, 0))
    out = [op(base, x) for x in inc]
    return out[::-1] if back else out


def cols(c):
    return pl.ds(pl.multiple_of(c * COL_W, COL_W), COL_W)


def block(i, size):
    return pl.ds(pl.multiple_of(i * size, size), size)


def loop(n, body, first=0):
    def step(i, carry):
        body(i)
        return carry
    lax.fori_loop(first, n, step, 0)


def write_mask(mask_ref, at, own_k, low, k, column):
    inside = jnp.logical_and(k <= own_k, k > low)
    to = pl.ds(pl.multiple_of(column, LANES), LANES)
    mask_ref[at, to] = jnp.where(inside, 1.0, 0.0).astype(bf16)


def row_masks(keys_ref, lows, all_keys, places, between=None):
    key_rows = keys_ref.shape[0]
    unroll = 4

    def mask_block(b):
        own_k, low = expand(keys_ref, b), expand(lows, b)

        def fill(t):
            for q, (ref, first) in enumerate(places):
                for u in range(unroll):
                    row = t * unroll + u
                    write_mask(ref, block(b, LANES), own_k, low, all_keys[q, pl.ds(row, 1), :],
                               row * LANES + first)

        loop(key_rows // unroll, fill)

    if between is None:
        loop(key_rows, mask_block)
    else:
        loop(key_rows // 2, mask_block)
        between()
        loop(key_rows, mask_block, key_rows // 2)


def neighbours():
    batch, me = lax.axis_index('batch'), lax.axis_index('group')
    core = lax.rem(me, 2)
    return batch, me, core, me + 1 - 2 * core, lax.rem(me + 2, 4), 3 - me


def greet(devices):
    barrier = pltpu.get_barrier_semaphore()
    for dev in devices:
        pl.semaphore_signal(barrier, inc=1, device_id=dev, device_id_type=MESH)
    pl.semaphore_wait(barrier, len(devices))


def local(src, dst, sem):
    return pltpu.make_async_copy(src, dst, sem)


def remote(src, dst, ssem, rsem, dev):
    return pltpu.make_async_remote_copy(src, dst, ssem, rsem, device_id=dev, device_id_type=MESH)


def runs_kernel(keys_ref, segs_ref, x_ref, out_ref, flag_ref, lows, all_keys, acc_buf, end_mask, end_rows,
                land_mate, land_raw,
                land_one, land_sum, all_segs, slots, slot_keys, col_slot, flags, mask_ref, pick_ref,
                rows_buf, mid_buf, low_buf, near_buf, last_buf, one_buf, sum_buf, sum_in, small_send,
                small_recv, raw_send, raw_recv, mate_send, mate_recv, run_send, run_recv, fwd_send,
                fwd_recv, load_sem, near_sem, last_sem):
    rows, width = x_ref.shape
    key_rows = rows // LANES
    chunks = width // COL_W
    run_chunks = chunks - 1
    ones, sums = land_one.shape[1], land_sum.shape[1]
    main = ones
    tail = sums - main
    ones_at = 2 * rows
    sums_at = ones_at + 2 * ones
    end_tile = 4
    tile_of = ((0, 1, 5, 7), (2, 3, 6, 8))
    tail_at = sums_at + end_tile * LANES
    run_cols = 2 * main + LANES
    tile = 1024
    inf = jnp.inf
    batch, me, core, mate, peer, diag = neighbours()
    mate, peer, diag = (batch, mate), (batch, peer), (batch, diag)
    greet((mate, peer, diag, (1 - batch, me)))

    def small(n, src, dst, dev):
        return remote(src, dst, small_send.at[n], small_recv.at[n], dev)

    key_copies = []
    for q, dev in enumerate((mate, peer, diag)):
        key_copies.append(small(2 * q, keys_ref, all_keys.at[q + 1], dev))
        key_copies.append(small(2 * q + 1, segs_ref, all_segs.at[q + 1], dev))
    for copy in key_copies:
        copy.start()

    raw = remote(x_ref.at[:, cols(0)], land_raw.at[0], raw_send.at[0], raw_recv.at[0], peer)
    raw_fwd = remote(land_raw.at[0], land_raw.at[1], raw_send.at[1], raw_recv.at[1], mate)
    raw.start()

    def near(c):
        return remote(x_ref.at[:, cols(c)], land_mate.at[:, cols(c)], mate_send.at[c],
                      mate_recv.at[c], mate)

    loop(chunks, lambda c: near(c).start(), 1)
    near(0).start()
    all_keys[0] = keys_ref[...]
    all_segs[0] = segs_ref[...]
    for copy in key_copies:
        copy.wait()

    sub, lane = sort_index()
    key_list = [all_keys[v // 2, pl.ds(v % 2 * 8, 8), :] for v in range(8)]
    seg_list = [all_segs[v // 2, pl.ds(v % 2 * 8, 8), :] for v in range(8)]
    place = [(lane * 64 + sub * 8 + v).astype(f32) for v in range(8)]
    key_list, place_list, seg_list = bitonic([key_list, place, seg_list])

    zero, one = jnp.zeros((8, LANES), f32), jnp.ones((8, LANES), f32)
    both = jnp.logical_and

    def flag(c):
        return jnp.where(c, one, zero)

    first_seg = shifted(seg_list, 1, -1)
    before_key = shifted(key_list, 1, -inf)
    starts = [flag(x != y) for x, y in zip(seg_list, first_seg)]
    low_list = running([jnp.where(x > 0, k, -inf) for x, k in zip(starts, before_key)],
                       jnp.maximum, -inf)
    mine = [flag(p - 8.0 * jnp.floor(p * 0.125) < 4.0) for p in place_list]
    mine_before, mine_after = shifted(mine, 1, 0.0), shifted(mine, -1, 0.0)
    starts_after = shifted(starts, -1, 1.0)
    leader = [flag(both(both(m > 0, x == 0), y == 0))
              for m, x, y in zip(mine, mine_after, starts_after)]
    goes_on = [both(x > 0, y == 0) for x, y in zip(mine_after, starts_after)]
    begins = [jnp.logical_or(x == 0, y > 0) for x, y in zip(mine_before, starts)]
    weight = [jnp.where(x > 0, jnp.where(y, 1.0, 4096.0), 0.0) for x, y in zip(leader, begins)]
    counted = [x - y for x, y in zip(running(weight, jnp.add, 0.0), weight)]
    stop = [jnp.where(x > 0, 2.0 * p, jnp.where(both(m > 0, jnp.logical_not(g)), 2.0 * p + 1.0, 32768.0))
            for x, p, m, g in zip(leader, place, mine, goes_on)]
    stop = running(stop, jnp.minimum, 32768.0, back=True)
    needed = [both(m > 0, x - 2.0 * jnp.floor(x * 0.5) == 0.0) for m, x in zip(mine, stop)]

    def total(values):
        v = values[0]
        for x in values[1:]:
            v = v + x
        return jnp.sum(jnp.sum(v, axis=0, keepdims=True), axis=1, keepdims=True)

    n_single = total([flag(w == 1.0) for w in weight])
    n_longer = total([flag(w == 4096.0) for w in weight])
    spill = n_longer + jnp.maximum(n_single - 2.0 * ones, 0.0)
    flags[0] = jnp.broadcast_to(jnp.where(spill > 2.0 * sums, 1.0, 0.0), (8, LANES))

    float32_slots = float(rows)
    slot_list = []
    for w, c, m in zip(weight, counted, needed):
        before_longer = jnp.floor(c * (1.0 / 4096.0))
        before_single = c - 4096.0 * before_longer
        over = float32_slots + n_longer + before_single - 2.0 * ones
        slot = jnp.where(before_single < 2.0 * ones, before_single, over)
        slot = jnp.where(w == 1.0, slot, float32_slots + before_longer)
        slot_list.append(jnp.where(m, slot, -1.0))
    _, low_list, slot_list = bitonic([place_list, low_list, slot_list])
    for v in range(2):
        lows[pl.ds(v * 8, 8), :] = low_list[v]
    for v in range(4):
        slots[v // 2, pl.ds(v % 2 * 8, 8), :] = slot_list[v]
    flag_copy = small(6, flags.at[0], flags.at[1], peer)
    flag_copy.start()

    def near_loads(c, buf, sem):
        return (local(x_ref.at[:, cols(c)], buf.at[pl.ds(0, rows), :], sem.at[0]),
                local(land_mate.at[:, cols(c)], buf.at[pl.ds(rows, rows), :], sem.at[1]))

    def start_near(c, buf, sem):
        for copy in near_loads(c, buf, sem):
            copy.start()

    def wait_near(c, buf, sem):
        for copy in near_loads(c, buf, sem):
            copy.wait()

    near(1).wait_recv()
    start_near(1, near_buf, near_sem)

    size, unroll = 64, 4
    col_slot[...] = jnp.full(col_slot.shape, -inf, f32)

    def pick_block(b):
        base = jnp.where(b < ones // size, core * ones, rows + core * sums - ones) + b * size
        want = (lax.broadcasted_iota(jnp.int32, (size, LANES), 0) + base).astype(f32)

        def step(t, top):
            for q in range(2):
                for u in range(unroll):
                    row = t * unroll + u
                    hit = slots[q, pl.ds(row, 1), :] == want
                    pick_ref[block(b, size), block(q * key_rows + row, LANES)] = jnp.where(
                        hit, 1.0, 0.0).astype(bf16)
                    top = jnp.maximum(top, jnp.where(hit, all_keys[q, pl.ds(row, 1), :], -inf))
            return top

        top = lax.fori_loop(0, key_rows // unroll, step, jnp.full((size, LANES), -inf, f32))
        col_slot[block(b, size), :] = jnp.broadcast_to(jnp.max(top, axis=1, keepdims=True),
                                                       (size, LANES))

    loop(pick_ref.shape[0] // size, pick_block)

    for t in range(col_slot.shape[0] // LANES):
        slot_keys[0, pl.ds(t, 1), :] = col_slot[pl.ds(t * LANES, LANES), :].T[0:1, :]
    slot_key_copies = (small(7, slot_keys.at[0], slot_keys.at[1], peer),
                       small(8, slot_keys.at[0], slot_keys.at[2], diag))
    for copy in slot_key_copies:
        copy.start()

    parts = ((0, ones), (main, tail), (0, 2 * LANES), (2 * LANES, LANES), (3 * LANES, LANES))

    def run(e, kind):
        at = pl.ds(*parts[kind])
        buf, land = (sum_buf, land_sum) if kind else (one_buf, land_one)
        return remote(buf.at[lax.rem(e, 2), at, :], land.at[0, at, cols(e)], run_send.at[kind, e],
                      run_recv.at[kind, e], peer)

    def fwd(e, kind):
        at = pl.ds(*parts[kind])
        land = land_sum if kind else land_one
        return remote(land.at[0, at, cols(e)], land.at[1, at, cols(e)], fwd_send.at[kind, e],
                      fwd_recv.at[kind, e], mate)

    kinds = range(len(parts))

    def reduce_runs(e):
        wait_near(e + 1, near_buf, near_sem)
        slot = lax.rem(e, 2)
        one_buf[slot] = jnp.dot(pick_ref[pl.ds(0, ones), :], near_buf[...],
                                preferred_element_type=f32).astype(bf16)
        sum_buf[slot] = jnp.dot(pick_ref[pl.ds(ones, sums), :], near_buf[...],
                                preferred_element_type=f32)
        for kind in kinds:
            run(e, kind).start()

    def next_near(e):
        @pl.when(e < run_chunks - 1)
        def _():
            near(e + 1).wait_recv()

        start_near(e + 1, near_buf, near_sem)

    def reduce_first(e):
        reduce_runs(e)
        next_near(e + 1)

    loop(2, reduce_first)

    near(0).wait_recv()
    start_near(0, rows_buf, load_sem)

    def forward_raw():
        raw.wait_recv()
        raw_fwd.start()

    places = [(mask_ref, 0), (mask_ref, rows), (mask_ref, 2 * rows), (out_ref, 0)]
    row_masks(keys_ref, lows, all_keys, places, forward_raw)

    def tiles_loop(body):
        loop(rows // tile, lambda i: body(block(i, tile)))

    def dot(at, start, n, buf, offset):
        return jnp.dot(mask_ref[at, pl.ds(start, n)], buf[pl.ds(offset, n), :],
                       preferred_element_type=f32)

    def raw_load(s):
        return local(land_raw.at[s], rows_buf.at[pl.ds((2 + s) * rows, rows), :], load_sem.at[2 + s])

    raw_load(0).start()
    raw_fwd.wait_recv()
    raw_load(1).start()
    wait_near(0, rows_buf, load_sem)
    raw_load(0).wait()
    raw_load(1).wait()

    def whole(at):
        acc = dot(at, 0, 3 * rows, rows_buf, 0)
        acc += jnp.dot(out_ref[at, :], rows_buf[pl.ds(3 * rows, rows), :], preferred_element_type=f32)
        out_ref[at, cols(0)] = acc.astype(bf16)

    tiles_loop(whole)
    start_near(1, rows_buf, load_sem)

    for copy in slot_key_copies:
        copy.wait()

    def slot_mask(b):
        own_k, low = expand(keys_ref, b), expand(lows, b)
        for s in range(2):
            for t in range((ones + main) // LANES):
                if t < ones // LANES:
                    column = ones_at + s * ones + t * LANES
                else:
                    column = sums_at + tile_of[s][t - ones // LANES] * LANES
                key_row = slot_keys[1 + s, pl.ds(t, 1), :]
                write_mask(mask_ref, block(b, LANES), own_k, low, key_row, column)
                if column > tail_at:
                    write_mask(end_mask, block(b, LANES), own_k, low, key_row,
                               column - tail_at - LANES)
        t = (ones + main) // LANES
        ends = [slot_keys[1 + s, pl.ds(t, 1), :] for s in range(2)]
        end_lane = lax.broadcasted_iota(jnp.int32, ends[0].shape, 1)
        ends = jnp.where(end_lane < tail, ends[0],
                         pltpu.roll(jnp.broadcast_to(ends[1], (8, LANES)), tail, 1)[0:1, :])
        ends = jnp.where(end_lane < 2 * tail, ends, -inf)
        write_mask(mask_ref, block(b, LANES), own_k, low, ends, tail_at)

    loop(key_rows, slot_mask)
    pad = LANES - 2 * tail
    for buf, end in ((rows_buf, tail_at), (mid_buf, tail_at - sums_at), (low_buf, tail_at - sums_at)):
        buf[pl.ds(end + 2 * tail, pad), :] = jnp.zeros((pad, COL_W), bf16)

    size = tail

    def split(kind, s):
        lo, n = parts[kind]
        if lo == main:
            offset = end_tile * LANES + s * tail - lo
        else:
            offset = tile_of[s][lo // LANES] * LANES - lo

        def step(i):
            at = lo + i * size
            v = sum_in[s, block(lo // size + i, size), :]
            high = jnp.clip(v, -BF16_MAX, BF16_MAX).astype(bf16)
            rest = v - high.astype(f32)
            mid = rest.astype(bf16)
            to = pl.multiple_of(at + offset, size)
            rows_buf[pl.ds(sums_at + to, size), :] = high
            mid_buf[pl.ds(to, size), :] = mid
            low_buf[pl.ds(to, size), :] = (rest - mid.astype(f32)).astype(bf16)

        loop(n // size, step)

    def run_load(e, kind, s):
        at = pl.ds(*parts[kind])
        if kind:
            src, dst = land_sum.at[s, at, cols(e)], sum_in.at[s, at, :]
        else:
            src, dst = land_one.at[s, :, cols(e)], rows_buf.at[pl.ds(ones_at + s * ones, ones), :]
        return local(src, dst, load_sem.at[2 + 2 * kind + s])

    def receive(e, kind):
        run(e, kind).wait_recv()
        fwd(e, kind).start()
        run_load(e, kind, 0).start()

    def arrive(e, kind):
        fwd(e, kind).wait_recv()
        run_load(e, kind, 1).start()

    def take(e, kind):
        for s in range(2):
            run_load(e, kind, s).wait()
            if kind:
                split(kind, s)

    def arrived(e):
        for kind in kinds:
            arrive(e, kind)
        wait_near(e + 1, rows_buf, load_sem)
        for kind in kinds:
            take(e, kind)

    def add_tile(e):
        def whole_runs(i):
            at = block(i, tile)
            acc = dot(at, 0, sums_at + run_cols, rows_buf, 0)
            acc += dot(at, sums_at, run_cols, mid_buf, 0)
            acc += dot(at, sums_at, run_cols, low_buf, 0)
            out_ref[at, cols(e + 1)] = acc.astype(bf16)

        return whole_runs

    flag_copy.wait()
    flags[2] = jnp.maximum(flags[0], flags[1])
    flag_all = small(9, flags.at[2], flags.at[3], (1 - batch, me))
    flag_all.start()

    last = run_chunks - 1

    def near_rows(at):
        acc_buf[at, :] = dot(at, 0, 2 * rows, last_buf, 0)

    def last_ones(s):
        return local(land_one.at[s, :, cols(last)], near_buf.at[pl.ds(s * ones, ones), :],
                     last_sem.at[2 + s])

    near(chunks - 1).wait_recv()
    start_near(chunks - 1, last_buf, last_sem)

    def steady(e):
        @pl.when(e == last - 3)
        def _():
            wait_near(chunks - 1, last_buf, last_sem)

        @pl.when(jnp.logical_and(e >= last - 3, e < last - 1))
        def _():
            near_rows(block(e - last + 3, tile))

        for kind in kinds:
            receive(e, kind)

        @pl.when(e < last - 1)
        def _():
            for kind in kinds:
                run(e, kind).wait_send()
            reduce_runs(e + 2)

        @pl.when(e < last - 2)
        def _():
            next_near(e + 3)

        arrived(e)
        add_chunk = add_tile(e)

        def step(i):
            add_chunk(i)

            @pl.when(jnp.logical_and(e == last - 1, i == 0))
            def _():
                for kind in range(2):
                    run(last, kind).wait_recv()
                    fwd(last, kind).start()
                last_ones(0).start()

        loop(rows // tile, step)

        @pl.when(e < last - 1)
        def _():
            start_near(e + 2, rows_buf, load_sem)

    loop(last, steady)
    receive(last, 2)
    fwd(last, 0).wait_recv()
    last_ones(1).start()
    run_load(last, 1, 0).start()
    arrive(last, 1)
    last_ones(0).wait()
    last_ones(1).wait()

    def add_sums(acc, at, first, n):
        for buf, offset in ((rows_buf, sums_at), (mid_buf, 0), (low_buf, 0)):
            acc += dot(at, sums_at + first * LANES, n * LANES, buf, offset + first * LANES)
        return acc

    def single_rows(at):
        acc_buf[at, :] += dot(at, ones_at, 2 * ones, near_buf, 0)

    def first_runs(at):
        acc_buf[at, :] = add_sums(acc_buf[at, :], at, 0, end_tile + 1)

    def first_step(i):
        first_runs(block(i, tile))

        @pl.when(i == 0)
        def _():
            receive(last, 4)

    tiles_loop(single_rows)
    take(last, 1)
    arrive(last, 2)
    take(last, 2)
    receive(last, 3)
    loop(rows // tile, first_step)
    arrive(last, 3)
    take(last, 3)
    arrive(last, 4)
    take(last, 4)
    n = end_mask.shape[1]
    from_tile = tail_at + LANES
    for i, (buf, offset) in enumerate(((rows_buf, 0), (mid_buf, sums_at), (low_buf, sums_at))):
        end_rows[pl.ds(i * n, n), :] = buf[pl.ds(from_tile - offset, n), :]
    flag_all.wait()
    flag_ref[...] = jnp.maximum(flags[2], flags[3])
    raw.wait_send()
    raw_fwd.wait_send()
    loop(chunks, lambda c: near(c).wait_send())
    for kind in kinds:
        loop(run_chunks, lambda e: fwd(e, kind).wait_send())
        loop(run_chunks, lambda e: run(e, kind).wait_send(), run_chunks - 2)


def finish_kernel(done_ref, acc_ref, end_mask, end_rows, out_ref, last_buf, sem):
    rows, width = done_ref.shape
    n = end_mask.shape[1]
    done = pl.ds(0, width - COL_W)
    pieces = 4
    tile = rows // 2

    def store(i):
        at = pl.ds(i * (rows // pieces), rows // pieces)
        return local(done_ref.at[at, done], out_ref.at[at, done], sem.at[i])

    def last(i):
        at = pl.ds(i * tile, tile)
        return local(last_buf.at[at, :], out_ref.at[at, pl.ds(width - COL_W, COL_W)],
                     sem.at[pieces + i])

    for i in range(pieces):
        store(i).start()
    for t in range(2):
        at = pl.ds(t * tile, tile)
        acc = acc_ref[at, :]
        for i in range(3):
            acc += jnp.dot(end_mask[at, :], end_rows[pl.ds(i * n, n), :], preferred_element_type=f32)
        last_buf[at, :] = acc.astype(bf16)
        last(t).start()
    for i in range(pieces):
        store(i).wait()
    for t in range(2):
        last(t).wait()


def store_kernel(done_ref, out_ref, sem):
    store = local(done_ref, out_ref, sem.at[0])
    store.start()
    store.wait()


def rows_kernel(keys_ref, x_ref, lows, all_keys, out_ref, land_ref, mask_ref, rows_buf, send_sem,
                recv_sem, load_sem):
    rows, width = x_ref.shape
    chunks = width // COL_W
    tile = COL_W
    batch, _, _, mate, peer, diag = neighbours()
    mate, peer, diag = (batch, mate), (batch, peer), (batch, diag)
    greet((mate, peer, diag))

    def copy(kind, c):
        if kind < 2:
            src, dst, dev = x_ref.at[:, cols(c)], land_ref.at[kind, :, cols(c)], (mate, peer)[kind]
        else:
            src, dst, dev = land_ref.at[1, :, cols(c)], land_ref.at[2, :, cols(c)], mate
        return remote(src, dst, send_sem.at[kind, c], recv_sem.at[kind, c], dev)

    loop(chunks, lambda c: copy(1, c).start())
    loop(chunks, lambda c: copy(0, c).start())
    row_masks(keys_ref, lows, all_keys, [(mask_ref, q * rows) for q in range(4)])

    def chunk(c):
        copy(1, c).wait_recv()
        copy(2, c).start()
        copy(0, c).wait_recv()
        copy(2, c).wait_recv()
        loads = [local(x_ref.at[:, cols(c)], rows_buf.at[pl.ds(0, rows), :], load_sem.at[0])]
        for q in range(3):
            loads.append(local(land_ref.at[q, :, cols(c)], rows_buf.at[pl.ds((q + 1) * rows, rows), :],
                               load_sem.at[q + 1]))
        for load in loads:
            load.start()
        for load in loads:
            load.wait()

        def whole(i):
            out_ref[block(i, tile), cols(c)] = jnp.dot(mask_ref[block(i, tile), :], rows_buf[...],
                                                       preferred_element_type=f32).astype(bf16)

        loop(rows // tile, whole)

    loop(chunks, chunk)
    for kind in range(3):
        loop(chunks, lambda c: copy(kind, c).wait_send())


def solution(mesh):
    dma = pltpu.SemaphoreType.DMA
    any_spec = pl.BlockSpec(memory_space=pl.ANY)
    vmem_spec = pl.BlockSpec(memory_space=pltpu.VMEM)
    shape, vmem = jax.ShapeDtypeStruct, pltpu.VMEM

    def raw_exchange(keys, payload, lows, all_keys, *_):
        rows, width = payload.shape
        chunks = width // COL_W
        out, _ = pl.pallas_call(
            rows_kernel,
            out_shape=(vmem((rows, width), bf16), shape((3, rows, width), bf16)),
            in_specs=[vmem_spec, any_spec, vmem_spec, vmem_spec],
            out_specs=(vmem_spec, any_spec),
            scratch_shapes=[
                vmem((rows, 4 * rows), bf16), vmem((4 * rows, COL_W), bf16),
                dma((3, chunks)), dma((3, chunks)), dma((4,)),
            ],
            compiler_params=pltpu.CompilerParams(collective_id=1, has_side_effects=True,
                                                 vmem_limit_bytes=ROWS_LIMIT),
        )(keys, payload, lows, all_keys)
        return pl.pallas_call(
            store_kernel,
            out_shape=shape((rows, width), bf16),
            in_specs=[vmem_spec],
            out_specs=any_spec,
            scratch_shapes=[dma((1,))],
        )(out)

    def finish(keys, payload, lows, all_keys, done, acc, end_mask, end_rows):
        rows, width = payload.shape
        return pl.pallas_call(
            finish_kernel,
            out_shape=shape((rows, width), bf16),
            in_specs=[vmem_spec] * 4,
            out_specs=any_spec,
            scratch_shapes=[vmem((rows, COL_W), bf16), dma((6,))],
            compiler_params=pltpu.CompilerParams(vmem_limit_bytes=16000000),
        )(done, acc, end_mask, end_rows)

    def run_exchange(keys, segs, payload):
        rows, width = payload.shape
        ones, sums = rows // 4, rows * 33 // 128
        chunks = width // COL_W
        run_w = width - COL_W
        slot_rows = 2 * ones + LANES
        sum_rows = 2 * ones + LANES
        key_shape = keys.shape
        small, kinds = 12, 5
        return pl.pallas_call(
            runs_kernel,
            out_shape=(vmem((rows, width), bf16), vmem((8, LANES), f32), vmem(key_shape, f32),
                       vmem((4,) + key_shape, f32), vmem((rows, COL_W), f32),
                       vmem((rows, 4 * LANES), bf16), vmem((12 * LANES, COL_W), bf16),
                       shape((rows, width), bf16),
                       shape((2, rows, COL_W), bf16), shape((2, ones, run_w), bf16),
                       shape((2, sums, run_w), f32)),
            in_specs=[vmem_spec, vmem_spec, any_spec],
            out_specs=(vmem_spec,) * 7 + (any_spec,) * 4,
            scratch_shapes=[
                vmem((4,) + key_shape, jnp.int32), vmem((2,) + key_shape, f32),
                vmem((3,) + key_shape, f32), vmem((slot_rows, LANES), f32), vmem((4, 8, LANES), f32),
                vmem((rows, 3 * rows + LANES), bf16), vmem((2 * ones + COL_W // 4, 2 * rows), bf16),
                vmem((4 * rows, COL_W), bf16), vmem((sum_rows, COL_W), bf16),
                vmem((sum_rows, COL_W), bf16), vmem((2 * rows, COL_W), bf16), vmem((2 * rows, COL_W), bf16),
                vmem((2, ones, COL_W), bf16), vmem((2, sums, COL_W), f32),
                vmem((2, sums, COL_W), f32),
                dma((small,)), dma((small,)), dma((2,)), dma((2,)), dma((chunks,)), dma((chunks,)),
                dma((kinds, chunks)), dma((kinds, chunks)), dma((kinds, chunks)), dma((kinds, chunks)),
                dma((small,)), dma((2,)), dma((4,)),
            ],
            compiler_params=pltpu.CompilerParams(collective_id=0, has_side_effects=True,
                                                 vmem_limit_bytes=VMEM_LIMIT),
        )(keys, segs, payload)[:7]

    def per_device(sort_keys, seg_ids, payload):
        key_shape = (payload.shape[0] // LANES, LANES)
        keys = sort_keys.reshape(key_shape)
        done, full, lows, all_keys, *ends = run_exchange(keys, seg_ids.reshape(key_shape), payload)
        return lax.cond(full[0, 0] > 0.0, raw_exchange, finish, keys, payload, lows, all_keys, done,
                        *ends)

    row_spec = P(('batch', 'group'))
    mat_spec = P(('batch', 'group'), None)
    return jax.shard_map(per_device, mesh=mesh, in_specs=(row_spec, row_spec, mat_spec),
                         out_specs=mat_spec, check_vma=False)
```

```python
import jax
import jax.numpy as jnp
from jax import lax
from jax.experimental import pallas as pl
from jax.experimental.pallas import tpu as pltpu
from jax.sharding import PartitionSpec as P

MESH = pl.DeviceIdType.MESH
LANES = 128
COL_W = 256
LOG_N = 13
BF16_MAX = 3.3895314e38
VMEM_LIMIT = 53200000
ROWS_LIMIT = 54500000
f32, bf16 = jnp.float32, jnp.bfloat16


def expand(ref, b, q=None):
    row = ref[pl.ds(b, 1), :] if q is None else ref[q, pl.ds(b, 1), :]
    return jnp.broadcast_to(row, (LANES, LANES)).T


def sort_index():
    sub = lax.broadcasted_iota(jnp.int32, (8, LANES), 0)
    lane = lax.broadcasted_iota(jnp.int32, (8, LANES), 1)
    return sub, lane


def bitonic(arrays):
    sub, lane = sort_index()
    arrays = [list(a) for a in arrays]

    def bit(k, v):
        if k < 3:
            return bool(v >> k & 1)
        if k < 6:
            return (sub >> (k - 3) & 1) == 1
        return (lane >> (k - 6) & 1) == 1

    for size in range(1, LOG_N + 1):
        for j in reversed(range(size)):
            if j < 3:
                for v in range(8):
                    if v >> j & 1:
                        continue
                    w = v | 1 << j
                    swap = arrays[0][v] > arrays[0][w]
                    if size < LOG_N:
                        down = bit(size, v)
                        if isinstance(down, bool):
                            swap = arrays[0][v] < arrays[0][w] if down else swap
                        else:
                            swap = jnp.logical_xor(swap, down)
                    for a in arrays:
                        a[v], a[w] = jnp.where(swap, a[w], a[v]), jnp.where(swap, a[v], a[w])
                continue
            axis, d, n = (0, 1 << (j - 3), 8) if j < 6 else (1, 1 << (j - 6), LANES)
            upper = bit(j, 0)
            for v in range(8):
                other = [jnp.where(upper, pltpu.roll(a[v], d, axis), pltpu.roll(a[v], n - d, axis))
                         for a in arrays]
                keep_max = upper
                if size < LOG_N:
                    down = bit(size, v)
                    if isinstance(down, bool):
                        keep_max = jnp.logical_not(upper) if down else upper
                    else:
                        keep_max = jnp.logical_xor(upper, down)
                take = jnp.logical_xor(other[0] < arrays[0][v], keep_max)
                for a, o in zip(arrays, other):
                    a[v] = jnp.where(take, o, a[v])
    return arrays


def shifted(values, step, fill):
    sub, lane = sort_index()
    if step == 1:
        edge, first = pltpu.roll(values[7], 1, 0), sub == 0
        edge = jnp.where(first, pltpu.roll(edge, 1, 1), edge)
        edge = jnp.where(jnp.logical_and(first, lane == 0), fill, edge)
        return [edge] + values[:7]
    edge, last = pltpu.roll(values[0], 7, 0), sub == 7
    edge = jnp.where(last, pltpu.roll(edge, LANES - 1, 1), edge)
    edge = jnp.where(jnp.logical_and(last, lane == LANES - 1), fill, edge)
    return values[1:] + [edge]


def running(values, op, start, back=False):
    sub, lane = sort_index()
    seq = values[::-1] if back else values
    inc = [seq[0]]
    for x in seq[1:]:
        inc.append(op(inc[-1], x))

    def moved(x, d, axis):
        n = 8 if axis == 0 else LANES
        at = sub if axis == 0 else lane
        if back:
            return jnp.where(at < n - d, pltpu.roll(x, n - d, axis), start)
        return jnp.where(at >= d, pltpu.roll(x, d, axis), start)

    t = inc[-1]
    for d in (1, 2, 4):
        t = op(t, moved(t, d, 0))
    row = t[0:1, :] if back else t[7:8, :]
    u = jnp.broadcast_to(row, (8, LANES))
    for d in (1, 2, 4, 8, 16, 32, 64):
        u = op(u, moved(u, d, 1))
    base = op(moved(u, 1, 1), moved(t, 1, 0))
    out = [op(base, x) for x in inc]
    return out[::-1] if back else out


def cols(c):
    return pl.ds(pl.multiple_of(c * COL_W, COL_W), COL_W)


def block(i, size):
    return pl.ds(pl.multiple_of(i * size, size), size)


def loop(n, body, first=0):
    def step(i, carry):
        body(i)
        return carry
    lax.fori_loop(first, n, step, 0)


def write_mask(mask_ref, at, own_k, low, k, column):
    inside = jnp.logical_and(k <= own_k, k > low)
    to = pl.ds(pl.multiple_of(column, LANES), LANES)
    mask_ref[at, to] = jnp.where(inside, 1.0, 0.0).astype(bf16)


def row_masks(keys_ref, lows, all_keys, places, between=None):
    key_rows = keys_ref.shape[0]
    unroll = 4

    def mask_block(b):
        own_k, low = expand(keys_ref, b), expand(lows, b)

        def fill(t):
            for q, (ref, first) in enumerate(places):
                for u in range(unroll):
                    row = t * unroll + u
                    write_mask(ref, block(b, LANES), own_k, low, all_keys[q, pl.ds(row, 1), :],
                               row * LANES + first)

        loop(key_rows // unroll, fill)

    if between is None:
        loop(key_rows, mask_block)
    else:
        loop(key_rows // 2, mask_block)
        between()
        loop(key_rows, mask_block, key_rows // 2)


def neighbours():
    batch, me = lax.axis_index('batch'), lax.axis_index('group')
    core = lax.rem(me, 2)
    return batch, me, core, me + 1 - 2 * core, lax.rem(me + 2, 4), 3 - me


def greet(devices):
    barrier = pltpu.get_barrier_semaphore()
    for dev in devices:
        pl.semaphore_signal(barrier, inc=1, device_id=dev, device_id_type=MESH)
    pl.semaphore_wait(barrier, len(devices))


def local(src, dst, sem):
    return pltpu.make_async_copy(src, dst, sem)


def remote(src, dst, ssem, rsem, dev):
    return pltpu.make_async_remote_copy(src, dst, ssem, rsem, device_id=dev, device_id_type=MESH)


def runs_kernel(keys_ref, segs_ref, x_ref, out_ref, flag_ref, lows, all_keys, acc_buf, end_mask, end_rows,
                land_mate, land_raw,
                land_one, land_sum, all_segs, slots, slot_keys, col_slot, flags, mask_ref, pick_ref,
                rows_buf, mid_buf, low_buf, near_buf, last_buf, one_buf, sum_buf, sum_in, small_send,
                small_recv, raw_send, raw_recv, mate_send, mate_recv, run_send, run_recv, fwd_send,
                fwd_recv, load_sem, near_sem, last_sem):
    rows, width = x_ref.shape
    key_rows = rows // LANES
    chunks = width // COL_W
    run_chunks = chunks - 1
    ones, sums = land_one.shape[1], land_sum.shape[1]
    main = ones
    tail = sums - main
    ones_at = 2 * rows
    sums_at = ones_at + 2 * ones
    end_tile = 4
    tile_of = ((0, 1, 5, 7), (2, 3, 6, 8))
    tail_at = sums_at + end_tile * LANES
    run_cols = 2 * main + LANES
    tile = 1024
    inf = jnp.inf
    batch, me, core, mate, peer, diag = neighbours()
    mate, peer, diag = (batch, mate), (batch, peer), (batch, diag)
    greet((mate, peer, diag, (1 - batch, me)))

    def small(n, src, dst, dev):
        return remote(src, dst, small_send.at[n], small_recv.at[n], dev)

    key_copies = []
    for q, dev in enumerate((mate, peer, diag)):
        key_copies.append(small(2 * q, keys_ref, all_keys.at[q + 1], dev))
        key_copies.append(small(2 * q + 1, segs_ref, all_segs.at[q + 1], dev))
    for copy in key_copies:
        copy.start()

    raw = remote(x_ref.at[:, cols(0)], land_raw.at[0], raw_send.at[0], raw_recv.at[0], peer)
    raw_fwd = remote(land_raw.at[0], land_raw.at[1], raw_send.at[1], raw_recv.at[1], mate)
    raw.start()

    def near(c):
        return remote(x_ref.at[:, cols(c)], land_mate.at[:, cols(c)], mate_send.at[c],
                      mate_recv.at[c], mate)

    loop(chunks, lambda c: near(c).start(), 1)
    near(0).start()
    all_keys[0] = keys_ref[...]
    all_segs[0] = segs_ref[...]
    for copy in key_copies:
        copy.wait()

    sub, lane = sort_index()
    key_list = [all_keys[v // 2, pl.ds(v % 2 * 8, 8), :] for v in range(8)]
    seg_list = [all_segs[v // 2, pl.ds(v % 2 * 8, 8), :] for v in range(8)]
    place = [(lane * 64 + sub * 8 + v).astype(f32) for v in range(8)]
    key_list, place_list, seg_list = bitonic([key_list, place, seg_list])

    zero, one = jnp.zeros((8, LANES), f32), jnp.ones((8, LANES), f32)
    both = jnp.logical_and

    def flag(c):
        return jnp.where(c, one, zero)

    first_seg = shifted(seg_list, 1, -1)
    before_key = shifted(key_list, 1, -inf)
    starts = [flag(x != y) for x, y in zip(seg_list, first_seg)]
    low_list = running([jnp.where(x > 0, k, -inf) for x, k in zip(starts, before_key)],
                       jnp.maximum, -inf)
    mine = [flag(p - 8.0 * jnp.floor(p * 0.125) < 4.0) for p in place_list]
    mine_before, mine_after = shifted(mine, 1, 0.0), shifted(mine, -1, 0.0)
    starts_after = shifted(starts, -1, 1.0)
    leader = [flag(both(both(m > 0, x == 0), y == 0))
              for m, x, y in zip(mine, mine_after, starts_after)]
    goes_on = [both(x > 0, y == 0) for x, y in zip(mine_after, starts_after)]
    begins = [jnp.logical_or(x == 0, y > 0) for x, y in zip(mine_before, starts)]
    weight = [jnp.where(x > 0, jnp.where(y, 1.0, 4096.0), 0.0) for x, y in zip(leader, begins)]
    counted = [x - y for x, y in zip(running(weight, jnp.add, 0.0), weight)]
    stop = [jnp.where(x > 0, 2.0 * p, jnp.where(both(m > 0, jnp.logical_not(g)), 2.0 * p + 1.0, 32768.0))
            for x, p, m, g in zip(leader, place, mine, goes_on)]
    stop = running(stop, jnp.minimum, 32768.0, back=True)
    needed = [both(m > 0, x - 2.0 * jnp.floor(x * 0.5) == 0.0) for m, x in zip(mine, stop)]

    def total(values):
        v = values[0]
        for x in values[1:]:
            v = v + x
        return jnp.sum(jnp.sum(v, axis=0, keepdims=True), axis=1, keepdims=True)

    n_single = total([flag(w == 1.0) for w in weight])
    n_longer = total([flag(w == 4096.0) for w in weight])
    spill = n_longer + jnp.maximum(n_single - 2.0 * ones, 0.0)
    flags[0] = jnp.broadcast_to(jnp.where(spill > 2.0 * sums, 1.0, 0.0), (8, LANES))

    float32_slots = float(rows)
    slot_list = []
    for w, c, m in zip(weight, counted, needed):
        before_longer = jnp.floor(c * (1.0 / 4096.0))
        before_single = c - 4096.0 * before_longer
        over = float32_slots + n_longer + before_single - 2.0 * ones
        slot = jnp.where(before_single < 2.0 * ones, before_single, over)
        slot = jnp.where(w == 1.0, slot, float32_slots + before_longer)
        slot_list.append(jnp.where(m, slot, -1.0))
    _, low_list, slot_list = bitonic([place_list, low_list, slot_list])
    for v in range(2):
        lows[pl.ds(v * 8, 8), :] = low_list[v]
    for v in range(4):
        slots[v // 2, pl.ds(v % 2 * 8, 8), :] = slot_list[v]
    flag_copy = small(6, flags.at[0], flags.at[1], peer)
    flag_copy.start()

    def near_loads(c, buf, sem):
        return (local(x_ref.at[:, cols(c)], buf.at[pl.ds(0, rows), :], sem.at[0]),
                local(land_mate.at[:, cols(c)], buf.at[pl.ds(rows, rows), :], sem.at[1]))

    def start_near(c, buf, sem):
        for copy in near_loads(c, buf, sem):
            copy.start()

    def wait_near(c, buf, sem):
        for copy in near_loads(c, buf, sem):
            copy.wait()

    near(1).wait_recv()
    start_near(1, near_buf, near_sem)

    size, unroll = 64, 4
    col_slot[...] = jnp.full(col_slot.shape, -inf, f32)

    def pick_block(b):
        base = jnp.where(b < ones // size, core * ones, rows + core * sums - ones) + b * size
        want = (lax.broadcasted_iota(jnp.int32, (size, LANES), 0) + base).astype(f32)

        def step(t, top):
            for q in range(2):
                for u in range(unroll):
                    row = t * unroll + u
                    hit = slots[q, pl.ds(row, 1), :] == want
                    pick_ref[block(b, size), block(q * key_rows + row, LANES)] = jnp.where(
                        hit, 1.0, 0.0).astype(bf16)
                    top = jnp.maximum(top, jnp.where(hit, all_keys[q, pl.ds(row, 1), :], -inf))
            return top

        top = lax.fori_loop(0, key_rows // unroll, step, jnp.full((size, LANES), -inf, f32))
        col_slot[block(b, size), :] = jnp.broadcast_to(jnp.max(top, axis=1, keepdims=True),
                                                       (size, LANES))

    loop(pick_ref.shape[0] // size, pick_block)

    for t in range(col_slot.shape[0] // LANES):
        slot_keys[0, pl.ds(t, 1), :] = col_slot[pl.ds(t * LANES, LANES), :].T[0:1, :]
    slot_key_copies = (small(7, slot_keys.at[0], slot_keys.at[1], peer),
                       small(8, slot_keys.at[0], slot_keys.at[2], diag))
    for copy in slot_key_copies:
        copy.start()

    parts = ((0, ones), (main, tail), (0, 2 * LANES), (2 * LANES, LANES), (3 * LANES, LANES))

    def run(e, kind):
        at = pl.ds(*parts[kind])
        buf, land = (sum_buf, land_sum) if kind else (one_buf, land_one)
        return remote(buf.at[lax.rem(e, 2), at, :], land.at[0, at, cols(e)], run_send.at[kind, e],
                      run_recv.at[kind, e], peer)

    def fwd(e, kind):
        at = pl.ds(*parts[kind])
        land = land_sum if kind else land_one
        return remote(land.at[0, at, cols(e)], land.at[1, at, cols(e)], fwd_send.at[kind, e],
                      fwd_recv.at[kind, e], mate)

    kinds = range(len(parts))

    def reduce_runs(e):
        wait_near(e + 1, near_buf, near_sem)
        slot = lax.rem(e, 2)
        one_buf[slot] = jnp.dot(pick_ref[pl.ds(0, ones), :], near_buf[...],
                                preferred_element_type=f32).astype(bf16)
        sum_buf[slot] = jnp.dot(pick_ref[pl.ds(ones, sums), :], near_buf[...],
                                preferred_element_type=f32)
        for kind in kinds:
            run(e, kind).start()

    def next_near(e):
        @pl.when(e < run_chunks - 1)
        def _():
            near(e + 1).wait_recv()

        start_near(e + 1, near_buf, near_sem)

    def reduce_first(e):
        reduce_runs(e)
        next_near(e + 1)

    loop(2, reduce_first)

    near(0).wait_recv()
    start_near(0, rows_buf, load_sem)

    def forward_raw():
        raw.wait_recv()
        raw_fwd.start()

    places = [(mask_ref, 0), (mask_ref, rows), (mask_ref, 2 * rows), (out_ref, 0)]
    row_masks(keys_ref, lows, all_keys, places, forward_raw)

    def tiles_loop(body):
        loop(rows // tile, lambda i: body(block(i, tile)))

    def dot(at, start, n, buf, offset):
        return jnp.dot(mask_ref[at, pl.ds(start, n)], buf[pl.ds(offset, n), :],
                       preferred_element_type=f32)

    def raw_load(s):
        return local(land_raw.at[s], rows_buf.at[pl.ds((2 + s) * rows, rows), :], load_sem.at[2 + s])

    raw_load(0).start()
    raw_fwd.wait_recv()
    raw_load(1).start()
    wait_near(0, rows_buf, load_sem)
    raw_load(0).wait()
    raw_load(1).wait()

    def whole(at):
        acc = dot(at, 0, 3 * rows, rows_buf, 0)
        acc += jnp.dot(out_ref[at, :], rows_buf[pl.ds(3 * rows, rows), :], preferred_element_type=f32)
        out_ref[at, cols(0)] = acc.astype(bf16)

    tiles_loop(whole)
    start_near(1, rows_buf, load_sem)

    for copy in slot_key_copies:
        copy.wait()

    def slot_mask(b):
        own_k, low = expand(keys_ref, b), expand(lows, b)
        for s in range(2):
            for t in range((ones + main) // LANES):
                if t < ones // LANES:
                    column = ones_at + s * ones + t * LANES
                else:
                    column = sums_at + tile_of[s][t - ones // LANES] * LANES
                key_row = slot_keys[1 + s, pl.ds(t, 1), :]
                write_mask(mask_ref, block(b, LANES), own_k, low, key_row, column)
                if t == (ones + main) // LANES - 1:
                    write_mask(end_mask, block(b, LANES), own_k, low, key_row,
                               s * LANES)
        t = (ones + main) // LANES
        ends = [slot_keys[1 + s, pl.ds(t, 1), :] for s in range(2)]
        end_lane = lax.broadcasted_iota(jnp.int32, ends[0].shape, 1)
        ends = jnp.where(end_lane < tail, ends[0],
                         pltpu.roll(jnp.broadcast_to(ends[1], (8, LANES)), tail, 1)[0:1, :])
        ends = jnp.where(end_lane < 2 * tail, ends, -inf)
        write_mask(mask_ref, block(b, LANES), own_k, low, ends, tail_at)

    loop(key_rows, slot_mask)
    pad = LANES - 2 * tail
    for buf, end in ((rows_buf, tail_at), (mid_buf, tail_at - sums_at), (low_buf, tail_at - sums_at)):
        buf[pl.ds(end + 2 * tail, pad), :] = jnp.zeros((pad, COL_W), bf16)

    size = tail

    def split(kind, s):
        lo, n = parts[kind]
        if lo == main:
            offset = end_tile * LANES + s * tail - lo
        else:
            offset = tile_of[s][lo // LANES] * LANES - lo

        def step(i):
            at = lo + i * size
            v = sum_in[s, block(lo // size + i, size), :]
            high = jnp.clip(v, -BF16_MAX, BF16_MAX).astype(bf16)
            rest = v - high.astype(f32)
            mid = rest.astype(bf16)
            to = pl.multiple_of(at + offset, size)
            rows_buf[pl.ds(sums_at + to, size), :] = high
            mid_buf[pl.ds(to, size), :] = mid
            low_buf[pl.ds(to, size), :] = (rest - mid.astype(f32)).astype(bf16)

        loop(n // size, step)

    def run_load(e, kind, s):
        at = pl.ds(*parts[kind])
        if kind:
            src, dst = land_sum.at[s, at, cols(e)], sum_in.at[s, at, :]
        else:
            src, dst = land_one.at[s, :, cols(e)], rows_buf.at[pl.ds(ones_at + s * ones, ones), :]
        return local(src, dst, load_sem.at[2 + 2 * kind + s])

    def receive(e, kind):
        run(e, kind).wait_recv()
        fwd(e, kind).start()
        run_load(e, kind, 0).start()

    def arrive(e, kind):
        fwd(e, kind).wait_recv()
        run_load(e, kind, 1).start()

    def take(e, kind):
        for s in range(2):
            run_load(e, kind, s).wait()
            if kind:
                split(kind, s)

    def arrived(e):
        for kind in kinds:
            arrive(e, kind)
        wait_near(e + 1, rows_buf, load_sem)
        for kind in kinds:
            take(e, kind)

    def add_tile(e):
        def whole_runs(i):
            at = block(i, tile)
            acc = dot(at, 0, sums_at + run_cols, rows_buf, 0)
            acc += dot(at, sums_at, run_cols, mid_buf, 0)
            acc += dot(at, sums_at, run_cols, low_buf, 0)
            out_ref[at, cols(e + 1)] = acc.astype(bf16)

        return whole_runs

    flag_copy.wait()
    flags[2] = jnp.maximum(flags[0], flags[1])
    flag_all = small(9, flags.at[2], flags.at[3], (1 - batch, me))
    flag_all.start()

    last = run_chunks - 1

    def near_rows(at):
        acc_buf[at, :] = dot(at, 0, 2 * rows, last_buf, 0)

    def last_ones(s):
        return local(land_one.at[s, :, cols(last)], near_buf.at[pl.ds(s * ones, ones), :],
                     last_sem.at[2 + s])

    near(chunks - 1).wait_recv()
    start_near(chunks - 1, last_buf, last_sem)

    def steady(e):
        @pl.when(e == last - 3)
        def _():
            wait_near(chunks - 1, last_buf, last_sem)

        @pl.when(jnp.logical_and(e >= last - 3, e < last - 1))
        def _():
            near_rows(block(e - last + 3, tile))

        for kind in kinds:
            receive(e, kind)

        @pl.when(e < last - 1)
        def _():
            for kind in kinds:
                run(e, kind).wait_send()
            reduce_runs(e + 2)

        @pl.when(e < last - 2)
        def _():
            next_near(e + 3)

        arrived(e)
        add_chunk = add_tile(e)

        def step(i):
            add_chunk(i)

            @pl.when(jnp.logical_and(e == last - 1, i == 0))
            def _():
                for kind in range(2):
                    run(last, kind).wait_recv()
                    fwd(last, kind).start()
                last_ones(0).start()

        loop(rows // tile, step)

        @pl.when(e < last - 1)
        def _():
            start_near(e + 2, rows_buf, load_sem)

    loop(last, steady)
    receive(last, 2)
    fwd(last, 0).wait_recv()
    last_ones(1).start()
    run_load(last, 1, 0).start()
    arrive(last, 1)
    last_ones(0).wait()
    last_ones(1).wait()

    def add_sums(acc, at, first, n):
        for buf, offset in ((rows_buf, sums_at), (mid_buf, 0), (low_buf, 0)):
            acc += dot(at, sums_at + first * LANES, n * LANES, buf, offset + first * LANES)
        return acc

    def single_rows(at):
        acc_buf[at, :] += dot(at, ones_at, 2 * ones, near_buf, 0)

    def first_runs(at):
        acc_buf[at, :] = add_sums(acc_buf[at, :], at, 0, end_tile + 1)

    def second_runs(at):
        acc_buf[at, :] = add_sums(acc_buf[at, :], at, tile_of[0][2], 2)

    def first_step(i):
        first_runs(block(i, tile))

        @pl.when(i == 0)
        def _():
            receive(last, 4)
            arrive(last, 3)

    tiles_loop(single_rows)
    take(last, 1)
    arrive(last, 2)
    take(last, 2)
    receive(last, 3)
    loop(rows // tile, first_step)
    take(last, 3)
    tiles_loop(second_runs)
    arrive(last, 4)
    take(last, 4)
    n = end_mask.shape[1]
    from_tile = sums_at + tile_of[0][3] * LANES
    for i, (buf, offset) in enumerate(((rows_buf, 0), (mid_buf, sums_at), (low_buf, sums_at))):
        end_rows[pl.ds(i * n, n), :] = buf[pl.ds(from_tile - offset, n), :]
    flag_all.wait()
    flag_ref[...] = jnp.maximum(flags[2], flags[3])[0:1, 0:1]
    raw.wait_send()
    raw_fwd.wait_send()
    loop(chunks, lambda c: near(c).wait_send())
    for kind in kinds:
        loop(run_chunks, lambda e: fwd(e, kind).wait_send())
        loop(run_chunks, lambda e: run(e, kind).wait_send(), run_chunks - 2)


def finish_kernel(done_ref, acc_ref, end_mask, end_rows, out_ref, last_buf, sem):
    rows, width = done_ref.shape
    n = end_mask.shape[1]
    done = pl.ds(0, width - COL_W)
    pieces = 4
    tile = rows // 2

    def store(i):
        at = pl.ds(i * (rows // pieces), rows // pieces)
        return local(done_ref.at[at, done], out_ref.at[at, done], sem.at[i])

    def last(i):
        at = pl.ds(i * tile, tile)
        return local(last_buf.at[at, :], out_ref.at[at, pl.ds(width - COL_W, COL_W)],
                     sem.at[pieces + i])

    for i in range(pieces):
        store(i).start()
    for t in range(2):
        at = pl.ds(t * tile, tile)
        acc = acc_ref[at, :]
        for i in range(3):
            acc += jnp.dot(end_mask[at, :], end_rows[pl.ds(i * n, n), :], preferred_element_type=f32)
        last_buf[at, :] = acc.astype(bf16)
        last(t).start()
    for i in range(pieces):
        store(i).wait()
    for t in range(2):
        last(t).wait()


def store_kernel(done_ref, out_ref, sem):
    store = local(done_ref, out_ref, sem.at[0])
    store.start()
    store.wait()


def rows_kernel(keys_ref, x_ref, lows, all_keys, out_ref, land_ref, mask_ref, rows_buf, send_sem,
                recv_sem, load_sem):
    rows, width = x_ref.shape
    chunks = width // COL_W
    tile = COL_W
    batch, _, _, mate, peer, diag = neighbours()
    mate, peer, diag = (batch, mate), (batch, peer), (batch, diag)
    greet((mate, peer, diag))

    def copy(kind, c):
        if kind < 2:
            src, dst, dev = x_ref.at[:, cols(c)], land_ref.at[kind, :, cols(c)], (mate, peer)[kind]
        else:
            src, dst, dev = land_ref.at[1, :, cols(c)], land_ref.at[2, :, cols(c)], mate
        return remote(src, dst, send_sem.at[kind, c], recv_sem.at[kind, c], dev)

    loop(chunks, lambda c: copy(1, c).start())
    loop(chunks, lambda c: copy(0, c).start())
    row_masks(keys_ref, lows, all_keys, [(mask_ref, q * rows) for q in range(4)])

    def chunk(c):
        copy(1, c).wait_recv()
        copy(2, c).start()
        copy(0, c).wait_recv()
        copy(2, c).wait_recv()
        loads = [local(x_ref.at[:, cols(c)], rows_buf.at[pl.ds(0, rows), :], load_sem.at[0])]
        for q in range(3):
            loads.append(local(land_ref.at[q, :, cols(c)], rows_buf.at[pl.ds((q + 1) * rows, rows), :],
                               load_sem.at[q + 1]))
        for load in loads:
            load.start()
        for load in loads:
            load.wait()

        def whole(i):
            out_ref[block(i, tile), cols(c)] = jnp.dot(mask_ref[block(i, tile), :], rows_buf[...],
                                                       preferred_element_type=f32).astype(bf16)

        loop(rows // tile, whole)

    loop(chunks, chunk)
    for kind in range(3):
        loop(chunks, lambda c: copy(kind, c).wait_send())


def solution(mesh):
    dma = pltpu.SemaphoreType.DMA
    any_spec = pl.BlockSpec(memory_space=pl.ANY)
    vmem_spec = pl.BlockSpec(memory_space=pltpu.VMEM)
    shape, vmem = jax.ShapeDtypeStruct, pltpu.VMEM

    def raw_exchange(keys, payload, lows, all_keys, *_):
        rows, width = payload.shape
        chunks = width // COL_W
        out, _ = pl.pallas_call(
            rows_kernel,
            out_shape=(vmem((rows, width), bf16), shape((3, rows, width), bf16)),
            in_specs=[vmem_spec, any_spec, vmem_spec, vmem_spec],
            out_specs=(vmem_spec, any_spec),
            scratch_shapes=[
                vmem((rows, 4 * rows), bf16), vmem((4 * rows, COL_W), bf16),
                dma((3, chunks)), dma((3, chunks)), dma((4,)),
            ],
            compiler_params=pltpu.CompilerParams(collective_id=1, has_side_effects=True,
                                                 vmem_limit_bytes=ROWS_LIMIT),
        )(keys, payload, lows, all_keys)
        return pl.pallas_call(
            store_kernel,
            out_shape=shape((rows, width), bf16),
            in_specs=[vmem_spec],
            out_specs=any_spec,
            scratch_shapes=[dma((1,))],
        )(out)

    def finish(keys, payload, lows, all_keys, done, acc, end_mask, end_rows):
        rows, width = payload.shape
        return pl.pallas_call(
            finish_kernel,
            out_shape=shape((rows, width), bf16),
            in_specs=[vmem_spec] * 4,
            out_specs=any_spec,
            scratch_shapes=[vmem((rows, COL_W), bf16), dma((6,))],
            compiler_params=pltpu.CompilerParams(vmem_limit_bytes=16000000),
        )(done, acc, end_mask, end_rows)

    def run_exchange(keys, segs, payload):
        rows, width = payload.shape
        ones, sums = rows // 4, rows * 33 // 128
        chunks = width // COL_W
        run_w = width - COL_W
        slot_rows = 2 * ones + LANES
        sum_rows = 2 * ones + LANES
        key_shape = keys.shape
        small, kinds = 12, 5
        return pl.pallas_call(
            runs_kernel,
            out_shape=(vmem((rows, width), bf16), vmem((1, 1), f32), vmem(key_shape, f32),
                       vmem((4,) + key_shape, f32), vmem((rows, COL_W), f32),
                       vmem((rows, 2 * LANES), bf16), vmem((6 * LANES, COL_W), bf16),
                       shape((rows, width), bf16),
                       shape((2, rows, COL_W), bf16), shape((2, ones, run_w), bf16),
                       shape((2, sums, run_w), f32)),
            in_specs=[vmem_spec, vmem_spec, any_spec],
            out_specs=(vmem_spec,) * 7 + (any_spec,) * 4,
            scratch_shapes=[
                vmem((4,) + key_shape, jnp.int32), vmem((2,) + key_shape, f32),
                vmem((3,) + key_shape, f32), vmem((slot_rows, LANES), f32), vmem((4, 8, LANES), f32),
                vmem((rows, 3 * rows + LANES), bf16), vmem((2 * ones + COL_W // 4, 2 * rows), bf16),
                vmem((4 * rows, COL_W), bf16), vmem((sum_rows, COL_W), bf16),
                vmem((sum_rows, COL_W), bf16), vmem((2 * rows, COL_W), bf16), vmem((2 * rows, COL_W), bf16),
                vmem((2, ones, COL_W), bf16), vmem((2, sums, COL_W), f32),
                vmem((2, sums, COL_W), f32),
                dma((small,)), dma((small,)), dma((2,)), dma((2,)), dma((chunks,)), dma((chunks,)),
                dma((kinds, chunks)), dma((kinds, chunks)), dma((kinds, chunks)), dma((kinds, chunks)),
                dma((small,)), dma((2,)), dma((4,)),
            ],
            compiler_params=pltpu.CompilerParams(collective_id=0, has_side_effects=True,
                                                 vmem_limit_bytes=VMEM_LIMIT),
        )(keys, segs, payload)[:7]

    def per_device(sort_keys, seg_ids, payload):
        key_shape = (payload.shape[0] // LANES, LANES)
        keys = sort_keys.reshape(key_shape)
        done, full, lows, all_keys, *ends = run_exchange(keys, seg_ids.reshape(key_shape), payload)
        return lax.cond(full[0, 0] > 0.0, raw_exchange, finish, keys, payload, lows, all_keys, done,
                        *ends)

    row_spec = P(('batch', 'group'))
    mat_spec = P(('batch', 'group'), None)
    return jax.shard_map(per_device, mesh=mesh, in_specs=(row_spec, row_spec, mat_spec),
                         out_specs=mat_spec, check_vma=False)
```

```python
import jax
import jax.numpy as jnp
from jax import lax
from jax.experimental import pallas as pl
from jax.experimental.pallas import tpu as pltpu
from jax.sharding import PartitionSpec as P

MESH = pl.DeviceIdType.MESH
LANES = 128
COL_W = 256
LOG_N = 13
BF16_MAX = 3.3895314e38
VMEM_LIMIT = 53200000
ROWS_LIMIT = 54500000
f32, bf16 = jnp.float32, jnp.bfloat16


def expand(ref, b, q=None):
    row = ref[pl.ds(b, 1), :] if q is None else ref[q, pl.ds(b, 1), :]
    return jnp.broadcast_to(row, (LANES, LANES)).T


def sort_index():
    sub = lax.broadcasted_iota(jnp.int32, (8, LANES), 0)
    lane = lax.broadcasted_iota(jnp.int32, (8, LANES), 1)
    return sub, lane


def bitonic(arrays):
    sub, lane = sort_index()
    arrays = [list(a) for a in arrays]

    def bit(k, v):
        if k < 3:
            return bool(v >> k & 1)
        if k < 6:
            return (sub >> (k - 3) & 1) == 1
        return (lane >> (k - 6) & 1) == 1

    for size in range(1, LOG_N + 1):
        for j in reversed(range(size)):
            if j < 3:
                for v in range(8):
                    if v >> j & 1:
                        continue
                    w = v | 1 << j
                    swap = arrays[0][v] > arrays[0][w]
                    if size < LOG_N:
                        down = bit(size, v)
                        if isinstance(down, bool):
                            swap = arrays[0][v] < arrays[0][w] if down else swap
                        else:
                            swap = jnp.logical_xor(swap, down)
                    for a in arrays:
                        a[v], a[w] = jnp.where(swap, a[w], a[v]), jnp.where(swap, a[v], a[w])
                continue
            axis, d, n = (0, 1 << (j - 3), 8) if j < 6 else (1, 1 << (j - 6), LANES)
            upper = bit(j, 0)
            for v in range(8):
                other = [jnp.where(upper, pltpu.roll(a[v], d, axis), pltpu.roll(a[v], n - d, axis))
                         for a in arrays]
                keep_max = upper
                if size < LOG_N:
                    down = bit(size, v)
                    if isinstance(down, bool):
                        keep_max = jnp.logical_not(upper) if down else upper
                    else:
                        keep_max = jnp.logical_xor(upper, down)
                take = jnp.logical_xor(other[0] < arrays[0][v], keep_max)
                for a, o in zip(arrays, other):
                    a[v] = jnp.where(take, o, a[v])
    return arrays


def shifted(values, step, fill):
    sub, lane = sort_index()
    if step == 1:
        edge, first = pltpu.roll(values[7], 1, 0), sub == 0
        edge = jnp.where(first, pltpu.roll(edge, 1, 1), edge)
        edge = jnp.where(jnp.logical_and(first, lane == 0), fill, edge)
        return [edge] + values[:7]
    edge, last = pltpu.roll(values[0], 7, 0), sub == 7
    edge = jnp.where(last, pltpu.roll(edge, LANES - 1, 1), edge)
    edge = jnp.where(jnp.logical_and(last, lane == LANES - 1), fill, edge)
    return values[1:] + [edge]


def running(values, op, start, back=False):
    sub, lane = sort_index()
    seq = values[::-1] if back else values
    inc = [seq[0]]
    for x in seq[1:]:
        inc.append(op(inc[-1], x))

    def moved(x, d, axis):
        n = 8 if axis == 0 else LANES
        at = sub if axis == 0 else lane
        if back:
            return jnp.where(at < n - d, pltpu.roll(x, n - d, axis), start)
        return jnp.where(at >= d, pltpu.roll(x, d, axis), start)

    t = inc[-1]
    for d in (1, 2, 4):
        t = op(t, moved(t, d, 0))
    row = t[0:1, :] if back else t[7:8, :]
    u = jnp.broadcast_to(row, (8, LANES))
    for d in (1, 2, 4, 8, 16, 32, 64):
        u = op(u, moved(u, d, 1))
    base = op(moved(u, 1, 1), moved(t, 1, 0))
    out = [op(base, x) for x in inc]
    return out[::-1] if back else out


def cols(c):
    return pl.ds(pl.multiple_of(c * COL_W, COL_W), COL_W)


def block(i, size):
    return pl.ds(pl.multiple_of(i * size, size), size)


def loop(n, body, first=0):
    def step(i, carry):
        body(i)
        return carry
    lax.fori_loop(first, n, step, 0)


def write_mask(mask_ref, at, own_k, low, k, column):
    inside = jnp.logical_and(k <= own_k, k > low)
    to = pl.ds(pl.multiple_of(column, LANES), LANES)
    mask_ref[at, to] = jnp.where(inside, 1.0, 0.0).astype(bf16)


def row_masks(keys_ref, lows, all_keys, places, between=None):
    key_rows = keys_ref.shape[0]
    unroll = 4

    def mask_block(b):
        own_k, low = expand(keys_ref, b), expand(lows, b)

        def fill(t):
            for q, (ref, first) in enumerate(places):
                for u in range(unroll):
                    row = t * unroll + u
                    write_mask(ref, block(b, LANES), own_k, low, all_keys[q, pl.ds(row, 1), :],
                               row * LANES + first)

        loop(key_rows // unroll, fill)

    if between is None:
        loop(key_rows, mask_block)
    else:
        loop(key_rows // 2, mask_block)
        between()
        loop(key_rows, mask_block, key_rows // 2)


def neighbours():
    batch, me = lax.axis_index('batch'), lax.axis_index('group')
    core = lax.rem(me, 2)
    return batch, me, core, me + 1 - 2 * core, lax.rem(me + 2, 4), 3 - me


def greet(devices):
    barrier = pltpu.get_barrier_semaphore()
    for dev in devices:
        pl.semaphore_signal(barrier, inc=1, device_id=dev, device_id_type=MESH)
    pl.semaphore_wait(barrier, len(devices))


def local(src, dst, sem):
    return pltpu.make_async_copy(src, dst, sem)


def remote(src, dst, ssem, rsem, dev):
    return pltpu.make_async_remote_copy(src, dst, ssem, rsem, device_id=dev, device_id_type=MESH)


def runs_kernel(keys_ref, segs_ref, x_ref, out_ref, flag_ref, lows, all_keys, acc_buf, end_mask, end_rows,
                land_mate, land_raw,
                land_one, land_sum, all_segs, slots, slot_keys, col_slot, flags, mask_ref, pick_ref,
                rows_buf, mid_buf, low_buf, near_buf, last_buf, one_buf, sum_buf, sum_in, small_send,
                small_recv, raw_send, raw_recv, mate_send, mate_recv, run_send, run_recv, fwd_send,
                fwd_recv, load_sem, near_sem, last_sem):
    rows, width = x_ref.shape
    key_rows = rows // LANES
    chunks = width // COL_W
    run_chunks = chunks - 1
    ones, sums = land_one.shape[1], land_sum.shape[1]
    main = ones
    tail = sums - main
    ones_at = 2 * rows
    sums_at = ones_at + 2 * ones
    end_tile = 4
    tile_of = ((0, 1, 5, 7), (2, 3, 6, 8))
    tail_at = sums_at + end_tile * LANES
    run_cols = 2 * main + LANES
    tile = 1024
    inf = jnp.inf
    batch, me, core, mate, peer, diag = neighbours()
    mate, peer, diag = (batch, mate), (batch, peer), (batch, diag)
    greet((mate, peer, diag, (1 - batch, me)))

    def small(n, src, dst, dev):
        return remote(src, dst, small_send.at[n], small_recv.at[n], dev)

    key_copies = []
    for q, dev in enumerate((mate, peer, diag)):
        key_copies.append(small(2 * q, keys_ref, all_keys.at[q + 1], dev))
        key_copies.append(small(2 * q + 1, segs_ref, all_segs.at[q + 1], dev))
    for copy in key_copies:
        copy.start()

    raw = remote(x_ref.at[:, cols(0)], land_raw.at[0], raw_send.at[0], raw_recv.at[0], peer)
    raw_fwd = remote(land_raw.at[0], land_raw.at[1], raw_send.at[1], raw_recv.at[1], mate)
    raw.start()

    def near(c):
        return remote(x_ref.at[:, cols(c)], land_mate.at[:, cols(c)], mate_send.at[c],
                      mate_recv.at[c], mate)

    loop(chunks, lambda c: near(c).start(), 1)
    near(0).start()
    all_keys[0] = keys_ref[...]
    all_segs[0] = segs_ref[...]
    for copy in key_copies:
        copy.wait()

    sub, lane = sort_index()
    key_list = [all_keys[v // 2, pl.ds(v % 2 * 8, 8), :] for v in range(8)]
    seg_list = [all_segs[v // 2, pl.ds(v % 2 * 8, 8), :] for v in range(8)]
    place = [(lane * 64 + sub * 8 + v).astype(f32) for v in range(8)]
    key_list, place_list, seg_list = bitonic([key_list, place, seg_list])

    zero, one = jnp.zeros((8, LANES), f32), jnp.ones((8, LANES), f32)
    both = jnp.logical_and

    def flag(c):
        return jnp.where(c, one, zero)

    first_seg = shifted(seg_list, 1, -1)
    before_key = shifted(key_list, 1, -inf)
    starts = [flag(x != y) for x, y in zip(seg_list, first_seg)]
    low_list = running([jnp.where(x > 0, k, -inf) for x, k in zip(starts, before_key)],
                       jnp.maximum, -inf)
    mine = [flag(p - 8.0 * jnp.floor(p * 0.125) < 4.0) for p in place_list]
    mine_before, mine_after = shifted(mine, 1, 0.0), shifted(mine, -1, 0.0)
    starts_after = shifted(starts, -1, 1.0)
    leader = [flag(both(both(m > 0, x == 0), y == 0))
              for m, x, y in zip(mine, mine_after, starts_after)]
    goes_on = [both(x > 0, y == 0) for x, y in zip(mine_after, starts_after)]
    begins = [jnp.logical_or(x == 0, y > 0) for x, y in zip(mine_before, starts)]
    weight = [jnp.where(x > 0, jnp.where(y, 1.0, 4096.0), 0.0) for x, y in zip(leader, begins)]
    counted = [x - y for x, y in zip(running(weight, jnp.add, 0.0), weight)]
    stop = [jnp.where(x > 0, 2.0 * p, jnp.where(both(m > 0, jnp.logical_not(g)), 2.0 * p + 1.0, 32768.0))
            for x, p, m, g in zip(leader, place, mine, goes_on)]
    stop = running(stop, jnp.minimum, 32768.0, back=True)
    needed = [both(m > 0, x - 2.0 * jnp.floor(x * 0.5) == 0.0) for m, x in zip(mine, stop)]

    def total(values):
        v = values[0]
        for x in values[1:]:
            v = v + x
        return jnp.sum(jnp.sum(v, axis=0, keepdims=True), axis=1, keepdims=True)

    n_single = total([flag(w == 1.0) for w in weight])
    n_longer = total([flag(w == 4096.0) for w in weight])
    spill = n_longer + jnp.maximum(n_single - 2.0 * ones, 0.0)
    flags[0] = jnp.broadcast_to(jnp.where(spill > 2.0 * sums, 1.0, 0.0), (8, LANES))

    float32_slots = float(rows)
    slot_list = []
    for w, c, m in zip(weight, counted, needed):
        before_longer = jnp.floor(c * (1.0 / 4096.0))
        before_single = c - 4096.0 * before_longer
        over = float32_slots + n_longer + before_single - 2.0 * ones
        slot = jnp.where(before_single < 2.0 * ones, before_single, over)
        slot = jnp.where(w == 1.0, slot, float32_slots + before_longer)
        slot_list.append(jnp.where(m, slot, -1.0))
    _, low_list, slot_list = bitonic([place_list, low_list, slot_list])
    for v in range(2):
        lows[pl.ds(v * 8, 8), :] = low_list[v]
    for v in range(4):
        slots[v // 2, pl.ds(v % 2 * 8, 8), :] = slot_list[v]
    flag_copy = small(6, flags.at[0], flags.at[1], peer)
    flag_copy.start()

    def near_loads(c, buf, sem):
        return (local(x_ref.at[:, cols(c)], buf.at[pl.ds(0, rows), :], sem.at[0]),
                local(land_mate.at[:, cols(c)], buf.at[pl.ds(rows, rows), :], sem.at[1]))

    def start_near(c, buf, sem):
        for copy in near_loads(c, buf, sem):
            copy.start()

    def wait_near(c, buf, sem):
        for copy in near_loads(c, buf, sem):
            copy.wait()

    near(1).wait_recv()
    start_near(1, near_buf, near_sem)

    size, unroll = 64, 4
    col_slot[...] = jnp.full(col_slot.shape, -inf, f32)

    def pick_block(b):
        base = jnp.where(b < ones // size, core * ones, rows + core * sums - ones) + b * size
        want = (lax.broadcasted_iota(jnp.int32, (size, LANES), 0) + base).astype(f32)

        def step(t, top):
            for q in range(2):
                for u in range(unroll):
                    row = t * unroll + u
                    hit = slots[q, pl.ds(row, 1), :] == want
                    pick_ref[block(b, size), block(q * key_rows + row, LANES)] = jnp.where(
                        hit, 1.0, 0.0).astype(bf16)
                    top = jnp.maximum(top, jnp.where(hit, all_keys[q, pl.ds(row, 1), :], -inf))
            return top

        top = lax.fori_loop(0, key_rows // unroll, step, jnp.full((size, LANES), -inf, f32))
        col_slot[block(b, size), :] = jnp.broadcast_to(jnp.max(top, axis=1, keepdims=True),
                                                       (size, LANES))

    loop(pick_ref.shape[0] // size, pick_block)

    for t in range(col_slot.shape[0] // LANES):
        slot_keys[0, pl.ds(t, 1), :] = col_slot[pl.ds(t * LANES, LANES), :].T[0:1, :]
    slot_key_copies = (small(7, slot_keys.at[0], slot_keys.at[1], peer),
                       small(8, slot_keys.at[0], slot_keys.at[2], diag))
    for copy in slot_key_copies:
        copy.start()

    parts = ((0, ones), (main, tail), (0, 2 * LANES), (2 * LANES, LANES), (3 * LANES, LANES))

    def run(e, kind):
        at = pl.ds(*parts[kind])
        buf, land = (sum_buf, land_sum) if kind else (one_buf, land_one)
        return remote(buf.at[lax.rem(e, 2), at, :], land.at[0, at, cols(e)], run_send.at[kind, e],
                      run_recv.at[kind, e], peer)

    def fwd(e, kind):
        at = pl.ds(*parts[kind])
        land = land_sum if kind else land_one
        return remote(land.at[0, at, cols(e)], land.at[1, at, cols(e)], fwd_send.at[kind, e],
                      fwd_recv.at[kind, e], mate)

    kinds = range(len(parts))

    def reduce_runs(e):
        wait_near(e + 1, near_buf, near_sem)
        slot = lax.rem(e, 2)
        one_buf[slot] = jnp.dot(pick_ref[pl.ds(0, ones), :], near_buf[...],
                                preferred_element_type=f32).astype(bf16)
        sum_buf[slot] = jnp.dot(pick_ref[pl.ds(ones, sums), :], near_buf[...],
                                preferred_element_type=f32)
        for kind in kinds:
            run(e, kind).start()

    def next_near(e):
        @pl.when(e < run_chunks - 1)
        def _():
            near(e + 1).wait_recv()

        start_near(e + 1, near_buf, near_sem)

    def reduce_first(e):
        reduce_runs(e)
        next_near(e + 1)

    loop(2, reduce_first)

    near(0).wait_recv()
    start_near(0, rows_buf, load_sem)

    def forward_raw():
        raw.wait_recv()
        raw_fwd.start()

    places = [(mask_ref, 0), (mask_ref, rows), (mask_ref, 2 * rows), (out_ref, 0)]
    row_masks(keys_ref, lows, all_keys, places, forward_raw)

    def tiles_loop(body):
        loop(rows // tile, lambda i: body(block(i, tile)))

    def dot(at, start, n, buf, offset):
        return jnp.dot(mask_ref[at, pl.ds(start, n)], buf[pl.ds(offset, n), :],
                       preferred_element_type=f32)

    def raw_load(s):
        return local(land_raw.at[s], rows_buf.at[pl.ds((2 + s) * rows, rows), :], load_sem.at[2 + s])

    raw_load(0).start()
    raw_fwd.wait_recv()
    raw_load(1).start()
    wait_near(0, rows_buf, load_sem)
    raw_load(0).wait()
    raw_load(1).wait()

    def whole(at):
        acc = dot(at, 0, 3 * rows, rows_buf, 0)
        acc += jnp.dot(out_ref[at, :], rows_buf[pl.ds(3 * rows, rows), :], preferred_element_type=f32)
        out_ref[at, cols(0)] = acc.astype(bf16)

    tiles_loop(whole)
    start_near(1, rows_buf, load_sem)

    for copy in slot_key_copies:
        copy.wait()

    def slot_mask(b):
        own_k, low = expand(keys_ref, b), expand(lows, b)
        for s in range(2):
            for t in range((ones + main) // LANES):
                if t < ones // LANES:
                    column = ones_at + s * ones + t * LANES
                else:
                    column = sums_at + tile_of[s][t - ones // LANES] * LANES
                key_row = slot_keys[1 + s, pl.ds(t, 1), :]
                write_mask(mask_ref, block(b, LANES), own_k, low, key_row, column)
                if column > tail_at:
                    write_mask(end_mask, block(b, LANES), own_k, low, key_row,
                               column - tail_at - LANES)
        t = (ones + main) // LANES
        ends = [slot_keys[1 + s, pl.ds(t, 1), :] for s in range(2)]
        end_lane = lax.broadcasted_iota(jnp.int32, ends[0].shape, 1)
        ends = jnp.where(end_lane < tail, ends[0],
                         pltpu.roll(jnp.broadcast_to(ends[1], (8, LANES)), tail, 1)[0:1, :])
        ends = jnp.where(end_lane < 2 * tail, ends, -inf)
        write_mask(mask_ref, block(b, LANES), own_k, low, ends, tail_at)

    loop(key_rows, slot_mask)
    pad = LANES - 2 * tail
    for buf, end in ((rows_buf, tail_at), (mid_buf, tail_at - sums_at), (low_buf, tail_at - sums_at)):
        buf[pl.ds(end + 2 * tail, pad), :] = jnp.zeros((pad, COL_W), bf16)

    size = tail

    def split(kind, s):
        lo, n = parts[kind]
        if lo == main:
            offset = end_tile * LANES + s * tail - lo
        else:
            offset = tile_of[s][lo // LANES] * LANES - lo

        def step(i):
            at = lo + i * size
            v = sum_in[s, block(lo // size + i, size), :]
            high = jnp.clip(v, -BF16_MAX, BF16_MAX).astype(bf16)
            rest = v - high.astype(f32)
            mid = rest.astype(bf16)
            to = pl.multiple_of(at + offset, size)
            rows_buf[pl.ds(sums_at + to, size), :] = high
            mid_buf[pl.ds(to, size), :] = mid
            low_buf[pl.ds(to, size), :] = (rest - mid.astype(f32)).astype(bf16)

        loop(n // size, step)

    def run_load(e, kind, s):
        at = pl.ds(*parts[kind])
        if kind:
            src, dst = land_sum.at[s, at, cols(e)], sum_in.at[s, at, :]
        else:
            src, dst = land_one.at[s, :, cols(e)], rows_buf.at[pl.ds(ones_at + s * ones, ones), :]
        return local(src, dst, load_sem.at[2 + 2 * kind + s])

    def receive(e, kind):
        run(e, kind).wait_recv()
        fwd(e, kind).start()
        run_load(e, kind, 0).start()

    def arrive(e, kind):
        fwd(e, kind).wait_recv()
        run_load(e, kind, 1).start()

    def take(e, kind):
        for s in range(2):
            run_load(e, kind, s).wait()
            if kind:
                split(kind, s)

    def arrived(e):
        for kind in kinds:
            arrive(e, kind)
        wait_near(e + 1, rows_buf, load_sem)
        for kind in kinds:
            take(e, kind)

    def add_tile(e):
        def whole_runs(i):
            at = block(i, tile)
            acc = dot(at, 0, sums_at + run_cols, rows_buf, 0)
            acc += dot(at, sums_at, run_cols, mid_buf, 0)
            acc += dot(at, sums_at, run_cols, low_buf, 0)
            out_ref[at, cols(e + 1)] = acc.astype(bf16)

        return whole_runs

    flag_copy.wait()
    flags[2] = jnp.maximum(flags[0], flags[1])
    flag_all = small(9, flags.at[2], flags.at[3], (1 - batch, me))
    flag_all.start()

    last = run_chunks - 1

    def near_rows(at):
        acc_buf[at, :] = dot(at, 0, 2 * rows, last_buf, 0)

    def last_ones(s):
        return local(land_one.at[s, :, cols(last)], near_buf.at[pl.ds(s * ones, ones), :],
                     last_sem.at[2 + s])

    near(chunks - 1).wait_recv()
    start_near(chunks - 1, last_buf, last_sem)

    def steady(e):
        @pl.when(e == last - 3)
        def _():
            wait_near(chunks - 1, last_buf, last_sem)

        @pl.when(jnp.logical_and(e >= last - 3, e < last - 1))
        def _():
            near_rows(block(e - last + 3, tile))

        for kind in kinds:
            receive(e, kind)

        @pl.when(e < last - 1)
        def _():
            for kind in kinds:
                run(e, kind).wait_send()
            reduce_runs(e + 2)

        @pl.when(e < last - 2)
        def _():
            next_near(e + 3)

        arrived(e)
        add_chunk = add_tile(e)

        def step(i):
            add_chunk(i)

            @pl.when(jnp.logical_and(e == last - 1, i == 0))
            def _():
                for kind in range(2):
                    run(last, kind).wait_recv()
                    fwd(last, kind).start()
                last_ones(0).start()

        loop(rows // tile, step)

        @pl.when(e < last - 1)
        def _():
            start_near(e + 2, rows_buf, load_sem)

    loop(last, steady)
    receive(last, 2)
    fwd(last, 0).wait_recv()
    last_ones(1).start()
    run_load(last, 1, 0).start()
    arrive(last, 1)
    last_ones(0).wait()
    last_ones(1).wait()

    def add_sums(acc, at, first, n):
        for buf, offset in ((rows_buf, sums_at), (mid_buf, 0), (low_buf, 0)):
            acc += dot(at, sums_at + first * LANES, n * LANES, buf, offset + first * LANES)
        return acc

    def single_rows(at):
        acc_buf[at, :] += dot(at, ones_at, 2 * ones, near_buf, 0)

    def first_runs(at):
        acc_buf[at, :] = add_sums(acc_buf[at, :], at, 0, end_tile + 1)

    def first_step(i):
        first_runs(block(i, tile))

        @pl.when(i == 0)
        def _():
            receive(last, 4)
            arrive(last, 3)

    tiles_loop(single_rows)
    take(last, 1)
    arrive(last, 2)
    take(last, 2)
    receive(last, 3)
    loop(rows // tile, first_step)
    take(last, 3)
    arrive(last, 4)
    take(last, 4)
    n = end_mask.shape[1]
    from_tile = tail_at + LANES
    for i, (buf, offset) in enumerate(((rows_buf, 0), (mid_buf, sums_at), (low_buf, sums_at))):
        end_rows[pl.ds(i * n, n), :] = buf[pl.ds(from_tile - offset, n), :]
    flag_all.wait()
    flag_ref[...] = jnp.maximum(flags[2], flags[3])[0:1, 0:1]
    raw.wait_send()
    raw_fwd.wait_send()
    loop(chunks, lambda c: near(c).wait_send())
    for kind in kinds:
        loop(run_chunks, lambda e: fwd(e, kind).wait_send())
        loop(run_chunks, lambda e: run(e, kind).wait_send(), run_chunks - 2)


def finish_kernel(done_ref, acc_ref, end_mask, end_rows, out_ref, last_buf, sem):
    rows, width = done_ref.shape
    n = end_mask.shape[1]
    done = pl.ds(0, width - COL_W)
    pieces = 4
    tile = rows // 2

    def store(i):
        at = pl.ds(i * (rows // pieces), rows // pieces)
        return local(done_ref.at[at, done], out_ref.at[at, done], sem.at[i])

    def last(i):
        at = pl.ds(i * tile, tile)
        return local(last_buf.at[at, :], out_ref.at[at, pl.ds(width - COL_W, COL_W)],
                     sem.at[pieces + i])

    for i in range(pieces):
        store(i).start()
    for t in range(2):
        at = pl.ds(t * tile, tile)
        acc = acc_ref[at, :]
        for i in range(3):
            acc += jnp.dot(end_mask[at, :], end_rows[pl.ds(i * n, n), :], preferred_element_type=f32)
        last_buf[at, :] = acc.astype(bf16)
        last(t).start()
    for i in range(pieces):
        store(i).wait()
    for t in range(2):
        last(t).wait()


def store_kernel(done_ref, out_ref, sem):
    store = local(done_ref, out_ref, sem.at[0])
    store.start()
    store.wait()


def rows_kernel(keys_ref, x_ref, lows, all_keys, out_ref, land_ref, mask_ref, rows_buf, send_sem,
                recv_sem, load_sem):
    rows, width = x_ref.shape
    chunks = width // COL_W
    tile = COL_W
    batch, _, _, mate, peer, diag = neighbours()
    mate, peer, diag = (batch, mate), (batch, peer), (batch, diag)
    greet((mate, peer, diag))

    def copy(kind, c):
        if kind < 2:
            src, dst, dev = x_ref.at[:, cols(c)], land_ref.at[kind, :, cols(c)], (mate, peer)[kind]
        else:
            src, dst, dev = land_ref.at[1, :, cols(c)], land_ref.at[2, :, cols(c)], mate
        return remote(src, dst, send_sem.at[kind, c], recv_sem.at[kind, c], dev)

    loop(chunks, lambda c: copy(1, c).start())
    loop(chunks, lambda c: copy(0, c).start())
    row_masks(keys_ref, lows, all_keys, [(mask_ref, q * rows) for q in range(4)])

    def chunk(c):
        copy(1, c).wait_recv()
        copy(2, c).start()
        copy(0, c).wait_recv()
        copy(2, c).wait_recv()
        loads = [local(x_ref.at[:, cols(c)], rows_buf.at[pl.ds(0, rows), :], load_sem.at[0])]
        for q in range(3):
            loads.append(local(land_ref.at[q, :, cols(c)], rows_buf.at[pl.ds((q + 1) * rows, rows), :],
                               load_sem.at[q + 1]))
        for load in loads:
            load.start()
        for load in loads:
            load.wait()

        def whole(i):
            out_ref[block(i, tile), cols(c)] = jnp.dot(mask_ref[block(i, tile), :], rows_buf[...],
                                                       preferred_element_type=f32).astype(bf16)

        loop(rows // tile, whole)

    loop(chunks, chunk)
    for kind in range(3):
        loop(chunks, lambda c: copy(kind, c).wait_send())


def solution(mesh):
    dma = pltpu.SemaphoreType.DMA
    any_spec = pl.BlockSpec(memory_space=pl.ANY)
    vmem_spec = pl.BlockSpec(memory_space=pltpu.VMEM)
    shape, vmem = jax.ShapeDtypeStruct, pltpu.VMEM

    def raw_exchange(keys, payload, lows, all_keys, *_):
        rows, width = payload.shape
        chunks = width // COL_W
        out, _ = pl.pallas_call(
            rows_kernel,
            out_shape=(vmem((rows, width), bf16), shape((3, rows, width), bf16)),
            in_specs=[vmem_spec, any_spec, vmem_spec, vmem_spec],
            out_specs=(vmem_spec, any_spec),
            scratch_shapes=[
                vmem((rows, 4 * rows), bf16), vmem((4 * rows, COL_W), bf16),
                dma((3, chunks)), dma((3, chunks)), dma((4,)),
            ],
            compiler_params=pltpu.CompilerParams(collective_id=1, has_side_effects=True,
                                                 vmem_limit_bytes=ROWS_LIMIT),
        )(keys, payload, lows, all_keys)
        return pl.pallas_call(
            store_kernel,
            out_shape=shape((rows, width), bf16),
            in_specs=[vmem_spec],
            out_specs=any_spec,
            scratch_shapes=[dma((1,))],
        )(out)

    def finish(keys, payload, lows, all_keys, done, acc, end_mask, end_rows):
        rows, width = payload.shape
        return pl.pallas_call(
            finish_kernel,
            out_shape=shape((rows, width), bf16),
            in_specs=[vmem_spec] * 4,
            out_specs=any_spec,
            scratch_shapes=[vmem((rows, COL_W), bf16), dma((6,))],
            compiler_params=pltpu.CompilerParams(vmem_limit_bytes=16000000),
        )(done, acc, end_mask, end_rows)

    def run_exchange(keys, segs, payload):
        rows, width = payload.shape
        ones, sums = rows // 4, rows * 33 // 128
        chunks = width // COL_W
        run_w = width - COL_W
        slot_rows = 2 * ones + LANES
        sum_rows = 2 * ones + LANES
        key_shape = keys.shape
        small, kinds = 12, 5
        return pl.pallas_call(
            runs_kernel,
            out_shape=(vmem((rows, width), bf16), vmem((1, 1), f32), vmem(key_shape, f32),
                       vmem((4,) + key_shape, f32), vmem((rows, COL_W), f32),
                       vmem((rows, 4 * LANES), bf16), vmem((12 * LANES, COL_W), bf16),
                       shape((rows, width), bf16),
                       shape((2, rows, COL_W), bf16), shape((2, ones, run_w), bf16),
                       shape((2, sums, run_w), f32)),
            in_specs=[vmem_spec, vmem_spec, any_spec],
            out_specs=(vmem_spec,) * 7 + (any_spec,) * 4,
            scratch_shapes=[
                vmem((4,) + key_shape, jnp.int32), vmem((2,) + key_shape, f32),
                vmem((3,) + key_shape, f32), vmem((slot_rows, LANES), f32), vmem((4, 8, LANES), f32),
                vmem((rows, 3 * rows + LANES), bf16), vmem((2 * ones + COL_W // 4, 2 * rows), bf16),
                vmem((4 * rows, COL_W), bf16), vmem((sum_rows, COL_W), bf16),
                vmem((sum_rows, COL_W), bf16), vmem((2 * rows, COL_W), bf16), vmem((2 * rows, COL_W), bf16),
                vmem((2, ones, COL_W), bf16), vmem((2, sums, COL_W), f32),
                vmem((2, sums, COL_W), f32),
                dma((small,)), dma((small,)), dma((2,)), dma((2,)), dma((chunks,)), dma((chunks,)),
                dma((kinds, chunks)), dma((kinds, chunks)), dma((kinds, chunks)), dma((kinds, chunks)),
                dma((small,)), dma((2,)), dma((4,)),
            ],
            compiler_params=pltpu.CompilerParams(collective_id=0, has_side_effects=True,
                                                 vmem_limit_bytes=VMEM_LIMIT),
        )(keys, segs, payload)[:7]

    def per_device(sort_keys, seg_ids, payload):
        key_shape = (payload.shape[0] // LANES, LANES)
        keys = sort_keys.reshape(key_shape)
        done, full, lows, all_keys, *ends = run_exchange(keys, seg_ids.reshape(key_shape), payload)
        return lax.cond(full[0, 0] > 0.0, raw_exchange, finish, keys, payload, lows, all_keys, done,
                        *ends)

    row_spec = P(('batch', 'group'))
    mat_spec = P(('batch', 'group'), None)
    return jax.shard_map(per_device, mesh=mesh, in_specs=(row_spec, row_spec, mat_spec),
                         out_specs=mat_spec, check_vma=False)
```

```python
import jax
import jax.numpy as jnp
from jax import lax
from jax.experimental import pallas as pl
from jax.experimental.pallas import tpu as pltpu
from jax.sharding import PartitionSpec as P

MESH = pl.DeviceIdType.MESH
LANES = 128
COL_W = 256
LOG_N = 13
BF16_MAX = 3.3895314e38
VMEM_LIMIT = 53200000
ROWS_LIMIT = 54500000
f32, bf16 = jnp.float32, jnp.bfloat16


def expand(ref, b, q=None):
    row = ref[pl.ds(b, 1), :] if q is None else ref[q, pl.ds(b, 1), :]
    return jnp.broadcast_to(row, (LANES, LANES)).T


def sort_index():
    sub = lax.broadcasted_iota(jnp.int32, (8, LANES), 0)
    lane = lax.broadcasted_iota(jnp.int32, (8, LANES), 1)
    return sub, lane


def bitonic(arrays):
    sub, lane = sort_index()
    arrays = [list(a) for a in arrays]

    def bit(k, v):
        if k < 3:
            return bool(v >> k & 1)
        if k < 6:
            return (sub >> (k - 3) & 1) == 1
        return (lane >> (k - 6) & 1) == 1

    for size in range(1, LOG_N + 1):
        for j in reversed(range(size)):
            if j < 3:
                for v in range(8):
                    if v >> j & 1:
                        continue
                    w = v | 1 << j
                    swap = arrays[0][v] > arrays[0][w]
                    if size < LOG_N:
                        down = bit(size, v)
                        if isinstance(down, bool):
                            swap = arrays[0][v] < arrays[0][w] if down else swap
                        else:
                            swap = jnp.logical_xor(swap, down)
                    for a in arrays:
                        a[v], a[w] = jnp.where(swap, a[w], a[v]), jnp.where(swap, a[v], a[w])
                continue
            axis, d, n = (0, 1 << (j - 3), 8) if j < 6 else (1, 1 << (j - 6), LANES)
            upper = bit(j, 0)
            for v in range(8):
                other = [jnp.where(upper, pltpu.roll(a[v], d, axis), pltpu.roll(a[v], n - d, axis))
                         for a in arrays]
                keep_max = upper
                if size < LOG_N:
                    down = bit(size, v)
                    if isinstance(down, bool):
                        keep_max = jnp.logical_not(upper) if down else upper
                    else:
                        keep_max = jnp.logical_xor(upper, down)
                take = jnp.logical_xor(other[0] < arrays[0][v], keep_max)
                for a, o in zip(arrays, other):
                    a[v] = jnp.where(take, o, a[v])
    return arrays


def shifted(values, step, fill):
    sub, lane = sort_index()
    if step == 1:
        edge, first = pltpu.roll(values[7], 1, 0), sub == 0
        edge = jnp.where(first, pltpu.roll(edge, 1, 1), edge)
        edge = jnp.where(jnp.logical_and(first, lane == 0), fill, edge)
        return [edge] + values[:7]
    edge, last = pltpu.roll(values[0], 7, 0), sub == 7
    edge = jnp.where(last, pltpu.roll(edge, LANES - 1, 1), edge)
    edge = jnp.where(jnp.logical_and(last, lane == LANES - 1), fill, edge)
    return values[1:] + [edge]


def running(values, op, start, back=False):
    sub, lane = sort_index()
    seq = values[::-1] if back else values
    inc = [seq[0]]
    for x in seq[1:]:
        inc.append(op(inc[-1], x))

    def moved(x, d, axis):
        n = 8 if axis == 0 else LANES
        at = sub if axis == 0 else lane
        if back:
            return jnp.where(at < n - d, pltpu.roll(x, n - d, axis), start)
        return jnp.where(at >= d, pltpu.roll(x, d, axis), start)

    t = inc[-1]
    for d in (1, 2, 4):
        t = op(t, moved(t, d, 0))
    row = t[0:1, :] if back else t[7:8, :]
    u = jnp.broadcast_to(row, (8, LANES))
    for d in (1, 2, 4, 8, 16, 32, 64):
        u = op(u, moved(u, d, 1))
    base = op(moved(u, 1, 1), moved(t, 1, 0))
    out = [op(base, x) for x in inc]
    return out[::-1] if back else out


def cols(c):
    return pl.ds(pl.multiple_of(c * COL_W, COL_W), COL_W)


def block(i, size):
    return pl.ds(pl.multiple_of(i * size, size), size)


def loop(n, body, first=0):
    def step(i, carry):
        body(i)
        return carry
    lax.fori_loop(first, n, step, 0)


def write_mask(mask_ref, at, own_k, low, k, column):
    inside = jnp.logical_and(k <= own_k, k > low)
    to = pl.ds(pl.multiple_of(column, LANES), LANES)
    mask_ref[at, to] = jnp.where(inside, 1.0, 0.0).astype(bf16)


def row_masks(keys_ref, lows, all_keys, places, between=None):
    key_rows = keys_ref.shape[0]
    unroll = 4

    def mask_block(b):
        own_k, low = expand(keys_ref, b), expand(lows, b)

        def fill(t):
            for q, (ref, first) in enumerate(places):
                for u in range(unroll):
                    row = t * unroll + u
                    write_mask(ref, block(b, LANES), own_k, low, all_keys[q, pl.ds(row, 1), :],
                               row * LANES + first)

        loop(key_rows // unroll, fill)

    if between is None:
        loop(key_rows, mask_block)
    else:
        loop(key_rows // 2, mask_block)
        between()
        loop(key_rows, mask_block, key_rows // 2)


def neighbours():
    batch, me = lax.axis_index('batch'), lax.axis_index('group')
    core = lax.rem(me, 2)
    return batch, me, core, me + 1 - 2 * core, lax.rem(me + 2, 4), 3 - me


def greet(devices):
    barrier = pltpu.get_barrier_semaphore()
    for dev in devices:
        pl.semaphore_signal(barrier, inc=1, device_id=dev, device_id_type=MESH)
    pl.semaphore_wait(barrier, len(devices))


def local(src, dst, sem):
    return pltpu.make_async_copy(src, dst, sem)


def remote(src, dst, ssem, rsem, dev):
    return pltpu.make_async_remote_copy(src, dst, ssem, rsem, device_id=dev, device_id_type=MESH)


def runs_kernel(keys_ref, segs_ref, x_ref, out_ref, flag_ref, lows, all_keys, acc_buf, end_mask, end_rows,
                land_mate, land_raw,
                land_one, land_sum, all_segs, slots, slot_keys, col_slot, flags, mask_ref, pick_ref,
                rows_buf, mid_buf, low_buf, near_buf, last_buf, one_buf, sum_buf, sum_in, small_send,
                small_recv, raw_send, raw_recv, mate_send, mate_recv, run_send, run_recv, fwd_send,
                fwd_recv, load_sem, near_sem, last_sem):
    rows, width = x_ref.shape
    key_rows = rows // LANES
    chunks = width // COL_W
    run_chunks = chunks - 1
    ones, sums = land_one.shape[1], land_sum.shape[1]
    main = ones
    tail = sums - main
    ones_at = 2 * rows
    sums_at = ones_at + 2 * ones
    end_tile = 4
    tile_of = ((0, 1, 5, 7), (2, 3, 6, 8))
    tail_at = sums_at + end_tile * LANES
    run_cols = 2 * main + LANES
    tile = 1024
    inf = jnp.inf
    batch, me, core, mate, peer, diag = neighbours()
    mate, peer, diag = (batch, mate), (batch, peer), (batch, diag)
    greet((mate, peer, diag, (1 - batch, me)))

    def small(n, src, dst, dev):
        return remote(src, dst, small_send.at[n], small_recv.at[n], dev)

    key_copies = []
    for q, dev in enumerate((mate, peer, diag)):
        key_copies.append(small(2 * q, keys_ref, all_keys.at[q + 1], dev))
        key_copies.append(small(2 * q + 1, segs_ref, all_segs.at[q + 1], dev))
    for copy in key_copies:
        copy.start()

    raw = remote(x_ref.at[:, cols(0)], land_raw.at[0], raw_send.at[0], raw_recv.at[0], peer)
    raw_fwd = remote(land_raw.at[0], land_raw.at[1], raw_send.at[1], raw_recv.at[1], mate)
    raw.start()

    def near(c):
        return remote(x_ref.at[:, cols(c)], land_mate.at[:, cols(c)], mate_send.at[c],
                      mate_recv.at[c], mate)

    loop(chunks, lambda c: near(c).start(), 1)
    near(0).start()
    all_keys[0] = keys_ref[...]
    all_segs[0] = segs_ref[...]
    for copy in key_copies:
        copy.wait()

    sub, lane = sort_index()
    key_list = [all_keys[v // 2, pl.ds(v % 2 * 8, 8), :] for v in range(8)]
    seg_list = [all_segs[v // 2, pl.ds(v % 2 * 8, 8), :] for v in range(8)]
    place = [(lane * 64 + sub * 8 + v).astype(f32) for v in range(8)]
    key_list, place_list, seg_list = bitonic([key_list, place, seg_list])

    zero, one = jnp.zeros((8, LANES), f32), jnp.ones((8, LANES), f32)
    both = jnp.logical_and

    def flag(c):
        return jnp.where(c, one, zero)

    first_seg = shifted(seg_list, 1, -1)
    before_key = shifted(key_list, 1, -inf)
    starts = [flag(x != y) for x, y in zip(seg_list, first_seg)]
    low_list = running([jnp.where(x > 0, k, -inf) for x, k in zip(starts, before_key)],
                       jnp.maximum, -inf)
    mine = [flag(p - 8.0 * jnp.floor(p * 0.125) < 4.0) for p in place_list]
    mine_before, mine_after = shifted(mine, 1, 0.0), shifted(mine, -1, 0.0)
    starts_after = shifted(starts, -1, 1.0)
    leader = [flag(both(both(m > 0, x == 0), y == 0))
              for m, x, y in zip(mine, mine_after, starts_after)]
    goes_on = [both(x > 0, y == 0) for x, y in zip(mine_after, starts_after)]
    begins = [jnp.logical_or(x == 0, y > 0) for x, y in zip(mine_before, starts)]
    weight = [jnp.where(x > 0, jnp.where(y, 1.0, 4096.0), 0.0) for x, y in zip(leader, begins)]
    counted = [x - y for x, y in zip(running(weight, jnp.add, 0.0), weight)]
    stop = [jnp.where(x > 0, 2.0 * p, jnp.where(both(m > 0, jnp.logical_not(g)), 2.0 * p + 1.0, 32768.0))
            for x, p, m, g in zip(leader, place, mine, goes_on)]
    stop = running(stop, jnp.minimum, 32768.0, back=True)
    needed = [both(m > 0, x - 2.0 * jnp.floor(x * 0.5) == 0.0) for m, x in zip(mine, stop)]

    def total(values):
        v = values[0]
        for x in values[1:]:
            v = v + x
        return jnp.sum(jnp.sum(v, axis=0, keepdims=True), axis=1, keepdims=True)

    n_single = total([flag(w == 1.0) for w in weight])
    n_longer = total([flag(w == 4096.0) for w in weight])
    spill = n_longer + jnp.maximum(n_single - 2.0 * ones, 0.0)
    flags[0] = jnp.broadcast_to(jnp.where(spill > 2.0 * sums, 1.0, 0.0), (8, LANES))

    float32_slots = float(rows)
    slot_list = []
    for w, c, m in zip(weight, counted, needed):
        before_longer = jnp.floor(c * (1.0 / 4096.0))
        before_single = c - 4096.0 * before_longer
        over = float32_slots + n_longer + before_single - 2.0 * ones
        slot = jnp.where(before_single < 2.0 * ones, before_single, over)
        slot = jnp.where(w == 1.0, slot, float32_slots + before_longer)
        slot_list.append(jnp.where(m, slot, -1.0))
    _, low_list, slot_list = bitonic([place_list, low_list, slot_list])
    for v in range(2):
        lows[pl.ds(v * 8, 8), :] = low_list[v]
    for v in range(4):
        slots[v // 2, pl.ds(v % 2 * 8, 8), :] = slot_list[v]
    flag_copy = small(6, flags.at[0], flags.at[1], peer)
    flag_copy.start()

    def near_loads(c, buf, sem):
        return (local(x_ref.at[:, cols(c)], buf.at[pl.ds(0, rows), :], sem.at[0]),
                local(land_mate.at[:, cols(c)], buf.at[pl.ds(rows, rows), :], sem.at[1]))

    def start_near(c, buf, sem):
        for copy in near_loads(c, buf, sem):
            copy.start()

    def wait_near(c, buf, sem):
        for copy in near_loads(c, buf, sem):
            copy.wait()

    near(1).wait_recv()
    start_near(1, near_buf, near_sem)

    size, unroll = 64, 4
    col_slot[...] = jnp.full(col_slot.shape, -inf, f32)

    def pick_block(b):
        base = jnp.where(b < ones // size, core * ones, rows + core * sums - ones) + b * size
        want = (lax.broadcasted_iota(jnp.int32, (size, LANES), 0) + base).astype(f32)

        def step(t, top):
            for q in range(2):
                for u in range(unroll):
                    row = t * unroll + u
                    hit = slots[q, pl.ds(row, 1), :] == want
                    pick_ref[block(b, size), block(q * key_rows + row, LANES)] = jnp.where(
                        hit, 1.0, 0.0).astype(bf16)
                    top = jnp.maximum(top, jnp.where(hit, all_keys[q, pl.ds(row, 1), :], -inf))
            return top

        top = lax.fori_loop(0, key_rows // unroll, step, jnp.full((size, LANES), -inf, f32))
        col_slot[block(b, size), :] = jnp.broadcast_to(jnp.max(top, axis=1, keepdims=True),
                                                       (size, LANES))

    loop(pick_ref.shape[0] // size, pick_block)

    for t in range(col_slot.shape[0] // LANES):
        slot_keys[0, pl.ds(t, 1), :] = col_slot[pl.ds(t * LANES, LANES), :].T[0:1, :]
    slot_key_copies = (small(7, slot_keys.at[0], slot_keys.at[1], peer),
                       small(8, slot_keys.at[0], slot_keys.at[2], diag))
    for copy in slot_key_copies:
        copy.start()

    parts = ((0, ones), (main, tail), (0, 2 * LANES), (2 * LANES, LANES), (3 * LANES, LANES))

    def run(e, kind):
        at = pl.ds(*parts[kind])
        buf, land = (sum_buf, land_sum) if kind else (one_buf, land_one)
        return remote(buf.at[lax.rem(e, 2), at, :], land.at[0, at, cols(e)], run_send.at[kind, e],
                      run_recv.at[kind, e], peer)

    def fwd(e, kind):
        at = pl.ds(*parts[kind])
        land = land_sum if kind else land_one
        return remote(land.at[0, at, cols(e)], land.at[1, at, cols(e)], fwd_send.at[kind, e],
                      fwd_recv.at[kind, e], mate)

    kinds = range(len(parts))

    def reduce_runs(e):
        wait_near(e + 1, near_buf, near_sem)
        slot = lax.rem(e, 2)
        one_buf[slot] = jnp.dot(pick_ref[pl.ds(0, ones), :], near_buf[...],
                                preferred_element_type=f32).astype(bf16)
        sum_buf[slot] = jnp.dot(pick_ref[pl.ds(ones, sums), :], near_buf[...],
                                preferred_element_type=f32)
        for kind in kinds:
            run(e, kind).start()

    def next_near(e):
        @pl.when(e < run_chunks - 1)
        def _():
            near(e + 1).wait_recv()

        start_near(e + 1, near_buf, near_sem)

    def reduce_first(e):
        reduce_runs(e)
        next_near(e + 1)

    loop(2, reduce_first)

    near(0).wait_recv()
    start_near(0, rows_buf, load_sem)

    def forward_raw():
        raw.wait_recv()
        raw_fwd.start()

    places = [(mask_ref, 0), (mask_ref, rows), (mask_ref, 2 * rows), (out_ref, 0)]
    row_masks(keys_ref, lows, all_keys, places, forward_raw)

    def tiles_loop(body):
        loop(rows // tile, lambda i: body(block(i, tile)))

    def dot(at, start, n, buf, offset):
        return jnp.dot(mask_ref[at, pl.ds(start, n)], buf[pl.ds(offset, n), :],
                       preferred_element_type=f32)

    def raw_load(s):
        return local(land_raw.at[s], rows_buf.at[pl.ds((2 + s) * rows, rows), :], load_sem.at[2 + s])

    raw_load(0).start()
    raw_fwd.wait_recv()
    raw_load(1).start()
    wait_near(0, rows_buf, load_sem)
    raw_load(0).wait()
    raw_load(1).wait()

    def whole(at):
        acc = dot(at, 0, 3 * rows, rows_buf, 0)
        acc += jnp.dot(out_ref[at, :], rows_buf[pl.ds(3 * rows, rows), :], preferred_element_type=f32)
        out_ref[at, cols(0)] = acc.astype(bf16)

    tiles_loop(whole)
    start_near(1, rows_buf, load_sem)

    for copy in slot_key_copies:
        copy.wait()

    def slot_mask(b):
        own_k, low = expand(keys_ref, b), expand(lows, b)
        for s in range(2):
            for t in range((ones + main) // LANES):
                if t < ones // LANES:
                    column = ones_at + s * ones + t * LANES
                else:
                    column = sums_at + tile_of[s][t - ones // LANES] * LANES
                key_row = slot_keys[1 + s, pl.ds(t, 1), :]
                write_mask(mask_ref, block(b, LANES), own_k, low, key_row, column)
                if column > tail_at:
                    write_mask(end_mask, block(b, LANES), own_k, low, key_row,
                               column - tail_at - LANES)
        t = (ones + main) // LANES
        ends = [slot_keys[1 + s, pl.ds(t, 1), :] for s in range(2)]
        end_lane = lax.broadcasted_iota(jnp.int32, ends[0].shape, 1)
        ends = jnp.where(end_lane < tail, ends[0],
                         pltpu.roll(jnp.broadcast_to(ends[1], (8, LANES)), tail, 1)[0:1, :])
        ends = jnp.where(end_lane < 2 * tail, ends, -inf)
        write_mask(mask_ref, block(b, LANES), own_k, low, ends, tail_at)

    loop(key_rows, slot_mask)
    pad = LANES - 2 * tail
    for buf, end in ((rows_buf, tail_at), (mid_buf, tail_at - sums_at), (low_buf, tail_at - sums_at)):
        buf[pl.ds(end + 2 * tail, pad), :] = jnp.zeros((pad, COL_W), bf16)

    size = tail

    def split(kind, s):
        lo, n = parts[kind]
        if lo == main:
            offset = end_tile * LANES + s * tail - lo
        else:
            offset = tile_of[s][lo // LANES] * LANES - lo

        def step(i):
            at = lo + i * size
            v = sum_in[s, block(lo // size + i, size), :]
            high = jnp.clip(v, -BF16_MAX, BF16_MAX).astype(bf16)
            rest = v - high.astype(f32)
            mid = rest.astype(bf16)
            to = pl.multiple_of(at + offset, size)
            rows_buf[pl.ds(sums_at + to, size), :] = high
            mid_buf[pl.ds(to, size), :] = mid
            low_buf[pl.ds(to, size), :] = (rest - mid.astype(f32)).astype(bf16)

        loop(n // size, step)

    def run_load(e, kind, s):
        at = pl.ds(*parts[kind])
        if kind:
            src, dst = land_sum.at[s, at, cols(e)], sum_in.at[s, at, :]
        else:
            src, dst = land_one.at[s, :, cols(e)], rows_buf.at[pl.ds(ones_at + s * ones, ones), :]
        return local(src, dst, load_sem.at[2 + 2 * kind + s])

    def receive(e, kind):
        run(e, kind).wait_recv()
        fwd(e, kind).start()
        run_load(e, kind, 0).start()

    def arrive(e, kind):
        fwd(e, kind).wait_recv()
        run_load(e, kind, 1).start()

    def take(e, kind):
        for s in range(2):
            run_load(e, kind, s).wait()
            if kind:
                split(kind, s)

    def arrived(e):
        for kind in kinds:
            arrive(e, kind)
        wait_near(e + 1, rows_buf, load_sem)
        for kind in kinds:
            take(e, kind)

    def add_tile(e):
        def whole_runs(i):
            at = block(i, tile)
            acc = dot(at, 0, sums_at + run_cols, rows_buf, 0)
            acc += dot(at, sums_at, run_cols, mid_buf, 0)
            acc += dot(at, sums_at, run_cols, low_buf, 0)
            out_ref[at, cols(e + 1)] = acc.astype(bf16)

        return whole_runs

    flag_copy.wait()
    flags[2] = jnp.maximum(flags[0], flags[1])
    flag_all = small(9, flags.at[2], flags.at[3], (1 - batch, me))
    flag_all.start()

    last = run_chunks - 1

    def near_rows(at):
        acc_buf[at, :] = dot(at, 0, 2 * rows, last_buf, 0)

    def last_ones(s):
        return local(land_one.at[s, :, cols(last)], near_buf.at[pl.ds(s * ones, ones), :],
                     last_sem.at[2 + s])

    near(chunks - 1).wait_recv()
    start_near(chunks - 1, last_buf, last_sem)

    def steady(e):
        @pl.when(e == last - 3)
        def _():
            wait_near(chunks - 1, last_buf, last_sem)

        @pl.when(jnp.logical_and(e >= last - 3, e < last - 1))
        def _():
            near_rows(block(e - last + 3, tile))

        for kind in kinds:
            receive(e, kind)

        @pl.when(e < last - 1)
        def _():
            for kind in kinds:
                run(e, kind).wait_send()
            reduce_runs(e + 2)

        @pl.when(e < last - 2)
        def _():
            next_near(e + 3)

        arrived(e)
        add_chunk = add_tile(e)

        def step(i):
            add_chunk(i)

            @pl.when(jnp.logical_and(e == last - 1, i == 0))
            def _():
                for kind in range(2):
                    run(last, kind).wait_recv()
                    fwd(last, kind).start()
                last_ones(0).start()

        loop(rows // tile, step)

        @pl.when(e < last - 1)
        def _():
            start_near(e + 2, rows_buf, load_sem)

    loop(last, steady)
    receive(last, 2)
    fwd(last, 0).wait_recv()
    last_ones(1).start()
    run_load(last, 1, 0).start()
    arrive(last, 1)
    last_ones(0).wait()
    last_ones(1).wait()

    def add_sums(acc, at, first, n):
        for buf, offset in ((rows_buf, sums_at), (mid_buf, 0), (low_buf, 0)):
            acc += dot(at, sums_at + first * LANES, n * LANES, buf, offset + first * LANES)
        return acc

    def single_rows(at):
        acc_buf[at, :] += dot(at, ones_at, 2 * ones, near_buf, 0)

    def first_runs(at):
        acc_buf[at, :] = add_sums(acc_buf[at, :], at, 0, end_tile + 1)

    def first_step(i):
        first_runs(block(i, tile))

        @pl.when(i == 0)
        def _():
            receive(last, 4)
            arrive(last, 3)

    tiles_loop(single_rows)
    take(last, 1)
    arrive(last, 2)
    take(last, 2)
    receive(last, 3)
    loop(rows // tile, first_step)
    take(last, 3)
    arrive(last, 4)
    take(last, 4)
    n = end_mask.shape[1]
    from_tile = tail_at + LANES
    for i, (buf, offset) in enumerate(((rows_buf, 0), (mid_buf, sums_at), (low_buf, sums_at))):
        end_rows[pl.ds(i * n, n), :] = buf[pl.ds(from_tile - offset, n), :]
    flag_all.wait()
    flag_ref[...] = jnp.maximum(flags[2], flags[3])[0:1, 0:1]
    raw.wait_send()
    raw_fwd.wait_send()
    loop(chunks, lambda c: near(c).wait_send())
    for kind in kinds:
        loop(run_chunks, lambda e: fwd(e, kind).wait_send())
        loop(run_chunks, lambda e: run(e, kind).wait_send(), run_chunks - 2)


def finish_kernel(done_ref, acc_ref, end_mask, end_rows, out_ref, last_buf, sem):
    rows, width = done_ref.shape
    n = end_mask.shape[1]
    done = pl.ds(0, width - COL_W)
    pieces = 16
    tile = rows // 2

    def store(i):
        at = pl.ds(i * (rows // pieces), rows // pieces)
        return local(done_ref.at[at, done], out_ref.at[at, done], sem.at[i])

    def last(i):
        at = pl.ds(i * tile, tile)
        return local(last_buf.at[at, :], out_ref.at[at, pl.ds(width - COL_W, COL_W)],
                     sem.at[pieces + i])

    for i in range(pieces):
        store(i).start()
    for t in range(2):
        at = pl.ds(t * tile, tile)
        acc = acc_ref[at, :]
        for i in range(3):
            acc += jnp.dot(end_mask[at, :], end_rows[pl.ds(i * n, n), :], preferred_element_type=f32)
        last_buf[at, :] = acc.astype(bf16)
        last(t).start()
    for i in range(pieces):
        store(i).wait()
    for t in range(2):
        last(t).wait()


def store_kernel(done_ref, out_ref, sem):
    store = local(done_ref, out_ref, sem.at[0])
    store.start()
    store.wait()


def rows_kernel(keys_ref, x_ref, lows, all_keys, out_ref, land_ref, mask_ref, rows_buf, send_sem,
                recv_sem, load_sem):
    rows, width = x_ref.shape
    chunks = width // COL_W
    tile = COL_W
    batch, _, _, mate, peer, diag = neighbours()
    mate, peer, diag = (batch, mate), (batch, peer), (batch, diag)
    greet((mate, peer, diag))

    def copy(kind, c):
        if kind < 2:
            src, dst, dev = x_ref.at[:, cols(c)], land_ref.at[kind, :, cols(c)], (mate, peer)[kind]
        else:
            src, dst, dev = land_ref.at[1, :, cols(c)], land_ref.at[2, :, cols(c)], mate
        return remote(src, dst, send_sem.at[kind, c], recv_sem.at[kind, c], dev)

    loop(chunks, lambda c: copy(1, c).start())
    loop(chunks, lambda c: copy(0, c).start())
    row_masks(keys_ref, lows, all_keys, [(mask_ref, q * rows) for q in range(4)])

    def chunk(c):
        copy(1, c).wait_recv()
        copy(2, c).start()
        copy(0, c).wait_recv()
        copy(2, c).wait_recv()
        loads = [local(x_ref.at[:, cols(c)], rows_buf.at[pl.ds(0, rows), :], load_sem.at[0])]
        for q in range(3):
            loads.append(local(land_ref.at[q, :, cols(c)], rows_buf.at[pl.ds((q + 1) * rows, rows), :],
                               load_sem.at[q + 1]))
        for load in loads:
            load.start()
        for load in loads:
            load.wait()

        def whole(i):
            out_ref[block(i, tile), cols(c)] = jnp.dot(mask_ref[block(i, tile), :], rows_buf[...],
                                                       preferred_element_type=f32).astype(bf16)

        loop(rows // tile, whole)

    loop(chunks, chunk)
    for kind in range(3):
        loop(chunks, lambda c: copy(kind, c).wait_send())


def solution(mesh):
    dma = pltpu.SemaphoreType.DMA
    any_spec = pl.BlockSpec(memory_space=pl.ANY)
    vmem_spec = pl.BlockSpec(memory_space=pltpu.VMEM)
    shape, vmem = jax.ShapeDtypeStruct, pltpu.VMEM

    def raw_exchange(keys, payload, lows, all_keys, *_):
        rows, width = payload.shape
        chunks = width // COL_W
        out, _ = pl.pallas_call(
            rows_kernel,
            out_shape=(vmem((rows, width), bf16), shape((3, rows, width), bf16)),
            in_specs=[vmem_spec, any_spec, vmem_spec, vmem_spec],
            out_specs=(vmem_spec, any_spec),
            scratch_shapes=[
                vmem((rows, 4 * rows), bf16), vmem((4 * rows, COL_W), bf16),
                dma((3, chunks)), dma((3, chunks)), dma((4,)),
            ],
            compiler_params=pltpu.CompilerParams(collective_id=1, has_side_effects=True,
                                                 vmem_limit_bytes=ROWS_LIMIT),
        )(keys, payload, lows, all_keys)
        return pl.pallas_call(
            store_kernel,
            out_shape=shape((rows, width), bf16),
            in_specs=[vmem_spec],
            out_specs=any_spec,
            scratch_shapes=[dma((1,))],
        )(out)

    def finish(keys, payload, lows, all_keys, done, acc, end_mask, end_rows):
        rows, width = payload.shape
        return pl.pallas_call(
            finish_kernel,
            out_shape=shape((rows, width), bf16),
            in_specs=[vmem_spec] * 4,
            out_specs=any_spec,
            scratch_shapes=[vmem((rows, COL_W), bf16), dma((18,))],
            compiler_params=pltpu.CompilerParams(vmem_limit_bytes=16000000),
        )(done, acc, end_mask, end_rows)

    def run_exchange(keys, segs, payload):
        rows, width = payload.shape
        ones, sums = rows // 4, rows * 33 // 128
        chunks = width // COL_W
        run_w = width - COL_W
        slot_rows = 2 * ones + LANES
        sum_rows = 2 * ones + LANES
        key_shape = keys.shape
        small, kinds = 12, 5
        return pl.pallas_call(
            runs_kernel,
            out_shape=(vmem((rows, width), bf16), vmem((1, 1), f32), vmem(key_shape, f32),
                       vmem((4,) + key_shape, f32), vmem((rows, COL_W), f32),
                       vmem((rows, 4 * LANES), bf16), vmem((12 * LANES, COL_W), bf16),
                       shape((rows, width), bf16),
                       shape((2, rows, COL_W), bf16), shape((2, ones, run_w), bf16),
                       shape((2, sums, run_w), f32)),
            in_specs=[vmem_spec, vmem_spec, any_spec],
            out_specs=(vmem_spec,) * 7 + (any_spec,) * 4,
            scratch_shapes=[
                vmem((4,) + key_shape, jnp.int32), vmem((2,) + key_shape, f32),
                vmem((3,) + key_shape, f32), vmem((slot_rows, LANES), f32), vmem((4, 8, LANES), f32),
                vmem((rows, 3 * rows + LANES), bf16), vmem((2 * ones + COL_W // 4, 2 * rows), bf16),
                vmem((4 * rows, COL_W), bf16), vmem((sum_rows, COL_W), bf16),
                vmem((sum_rows, COL_W), bf16), vmem((2 * rows, COL_W), bf16), vmem((2 * rows, COL_W), bf16),
                vmem((2, ones, COL_W), bf16), vmem((2, sums, COL_W), f32),
                vmem((2, sums, COL_W), f32),
                dma((small,)), dma((small,)), dma((2,)), dma((2,)), dma((chunks,)), dma((chunks,)),
                dma((kinds, chunks)), dma((kinds, chunks)), dma((kinds, chunks)), dma((kinds, chunks)),
                dma((small,)), dma((2,)), dma((4,)),
            ],
            compiler_params=pltpu.CompilerParams(collective_id=0, has_side_effects=True,
                                                 vmem_limit_bytes=VMEM_LIMIT),
        )(keys, segs, payload)[:7]

    def per_device(sort_keys, seg_ids, payload):
        key_shape = (payload.shape[0] // LANES, LANES)
        keys = sort_keys.reshape(key_shape)
        done, full, lows, all_keys, *ends = run_exchange(keys, seg_ids.reshape(key_shape), payload)
        return lax.cond(full[0, 0] > 0.0, raw_exchange, finish, keys, payload, lows, all_keys, done,
                        *ends)

    row_spec = P(('batch', 'group'))
    mat_spec = P(('batch', 'group'), None)
    return jax.shard_map(per_device, mesh=mesh, in_specs=(row_spec, row_spec, mat_spec),
                         out_specs=mat_spec, check_vma=False)
```
